32 devices in a mesh: gx: 4 (over y, core), gy: 2 (over x), gz: 4 (over z).
Axes of the slice: x: 2, y: 2, z: 4, core: 2. Of those that a mesh axis runs over, the one named last changes fastest.
Arguments:
- noisy_image: float32 [32, 64, 512], P('gz', 'gy', 'gx'), may hold values from -6 to 6
- fidelity: float32 [32, 64, 512], P('gz', 'gy', 'gx'), may hold values from 0.5 to 8
- primal_u: float32 [32, 64, 512], P('gz', 'gy', 'gx'), may hold values from -6 to 6
- primal_v: float32 [3, 32, 64, 512], P(None, 'gz', 'gy', 'gx'), may hold values from -2 to 2
- dual_p: float32 [3, 32, 64, 512], P(None, 'gz', 'gy', 'gx'), may hold values from -2.5 to 2.5
- dual_q: float32 [6, 32, 64, 512], P(None, 'gz', 'gy', 'gx'), may hold values from -2.5 to 2.5
Outputs:
- denoised: float32 [32, 64, 512], P('gz', 'gy', 'gx')
- vector_field: float32 [3, 32, 64, 512], P(None, 'gz', 'gy', 'gx')
- grad_dual: float32 [3, 32, 64, 512], P(None, 'gz', 'gy', 'gx')
- sym_dual: float32 [6, 32, 64, 512], P(None, 'gz', 'gy', 'gx')
The draws below stay inside these ranges and needn't reach their ends.
All inputs are finite; a program needn't handle non-finite values.
Results may differ from the reference program's by a relative error of at most 0.0001.
Values sent between devices are 32-bit elements; how exact they have to be, the bound alone decides.
A program may use at most 64 MiB of HBM per device.

```python
import math
import jax
import jax.numpy as jnp
from jax import lax

ITERS = 3
NX = 512
NY = 64
NZ = 32


def shard_levels(stream_key, shape, split, smallest, largest):
    def one(dim, shards_of):
        draws = jax.random.uniform(jax.random.fold_in(jax.random.fold_in(stream_key, 6), dim), (shards_of,), jnp.float32, smallest / len(split), largest / len(split))
        return jnp.repeat(jnp.exp(draws), shape[dim] // shards_of).reshape((-1,) + (1,) * (len(shape) - dim - 1))

    loudness = one(*split[0])
    for cut in split[1:]:
        loudness = loudness * one(*cut)
    return loudness


def bell_draw(own_key, shape, spread, limit, shards=(), kind=jnp.bfloat16):
    drawn = jax.random.normal(own_key, shape, jnp.float32) * spread
    if len(shards) > 0:
        drawn = shard_levels(own_key, shape, shards, -0.22, 0.18) * drawn
    return jnp.clip(drawn, min=-limit, max=limit).astype(kind)


def setup_inputs(seed: int = 0) -> dict:
    streams_of = jax.random.split(jax.random.key(seed), 7)
    noisy_image = bell_draw(streams_of[0], (NZ, NY, NX), 1.0, 6.0, ((0, 4), (1, 2), (2, 4)), jnp.float32)
    fidelity = jnp.clip(jnp.exp(math.log(8.0) - 2.7725887 * jax.random.uniform(streams_of[1], (NZ, NY, NX), jnp.float32) ** shard_levels(streams_of[1], (NZ, NY, NX), ((0, 4), (1, 2), (2, 4)), -0.2, 0.2)), 0.5, 8.0)
    primal_u = bell_draw(streams_of[2], (NZ, NY, NX), 1.0, 6.0, ((0, 4), (1, 2), (2, 4)), jnp.float32)
    primal_v = bell_draw(streams_of[3], (3, NZ, NY, NX), 0.3, 2.0, ((1, 4), (2, 2), (3, 4)), jnp.float32)
    dual_p = bell_draw(streams_of[4], (3, NZ, NY, NX), 0.4, 2.5, ((1, 4), (2, 2), (3, 4)), jnp.float32)
    dual_q = bell_draw(streams_of[5], (6, NZ, NY, NX), 0.4, 2.5, ((1, 4), (2, 2), (3, 4)), jnp.float32)
    return {"noisy_image": noisy_image, "fidelity": fidelity, "primal_u": primal_u, "primal_v": primal_v, "dual_p": dual_p, "dual_q": dual_q}


first_alpha = 0.5
second_alpha = 1.0
dual_step = 0.2
primal_step = 0.2
index_pairs = ((0, 0), (1, 1), (2, 2), (0, 1), (0, 2), (1, 2))

def pair_index(left_axis, right_axis):
    for position, entry_pair in enumerate(index_pairs):
        if entry_pair == (left_axis, right_axis) or entry_pair == (right_axis, left_axis):
            return position
    return 0

def shift_next(values, axis_dim):
    extent = values.shape[axis_dim]
    tail_part = lax.slice_in_dim(values, 1, extent, axis=axis_dim)
    zeros_shape = list(values.shape)
    zeros_shape[axis_dim] = 1
    return jnp.concatenate([tail_part, jnp.zeros(zeros_shape, values.dtype)], axis=axis_dim)

def shift_prev(values, axis_dim):
    extent = values.shape[axis_dim]
    head_part = lax.slice_in_dim(values, 0, extent - 1, axis=axis_dim)
    zeros_shape = list(values.shape)
    zeros_shape[axis_dim] = 1
    return jnp.concatenate([jnp.zeros(zeros_shape, values.dtype), head_part], axis=axis_dim)

def edge_masks(extents):
    lower_masks = []
    upper_masks = []
    for component in range(3):
        extent = extents[2 - component]
        places = lax.iota(jnp.int32, extent)
        shape_list = [1, 1, 1, 1]
        shape_list[3 - component] = extent
        upper_masks.append((places < extent - 1).astype(jnp.float32).reshape(shape_list))
        lower_masks.append((places > 0).astype(jnp.float32).reshape(shape_list))
    return (lower_masks, upper_masks)

def q_rows(stacked, column):
    return jnp.stack([stacked[pair_index(row_axis, column)] for row_axis in range(3)], axis=0)

def project(stacked, weights, bound):
    magnitude = jnp.sqrt(lax.optimization_barrier(jnp.sum(weights * stacked * stacked, axis=0, keepdims=True)))
    return stacked / jnp.maximum(1.0, magnitude / bound)

def dual_update(bar_u, bar_v, grad_dual, sym_dual, next_u, prev_v, lower_masks, upper_masks):
    grads = jnp.concatenate([upper_masks[component] * (next_u[component] - bar_u) for component in range(3)], axis=0)
    trial_p = grad_dual + dual_step * (grads - bar_v)
    new_p = project(trial_p, jnp.ones((3, 1, 1, 1), jnp.float32), first_alpha)
    derivs = [lower_masks[component] * (bar_v - prev_v[component]) for component in range(3)]
    sym_parts = []
    for left_axis, right_axis in index_pairs:
        sym_parts.append(0.5 * (derivs[right_axis][left_axis] + derivs[left_axis][right_axis]))
    trial_q = sym_dual + dual_step * jnp.stack(sym_parts, axis=0)
    weights = jnp.array([1.0, 1.0, 1.0, 2.0, 2.0, 2.0], jnp.float32).reshape((6, 1, 1, 1))
    new_q = project(trial_q, weights, second_alpha)
    return (new_p, new_q)

def primal_update(image_u, vector_v, grad_dual, sym_dual, noisy, weight_map, prev_p, next_q, lower_masks, upper_masks):
    divergence = jnp.zeros_like(image_u)
    second_div = jnp.zeros_like(vector_v)
    for component in range(3):
        divergence = divergence + upper_masks[component] * grad_dual[component:component + 1] - prev_p[component]
        second_div = second_div + next_q[component] - lower_masks[component] * q_rows(sym_dual, component)
    new_u = (image_u + primal_step * divergence + primal_step * weight_map * noisy) / (1.0 + primal_step * weight_map)
    new_v = vector_v + primal_step * (grad_dual + second_div)
    return (new_u, new_v)

def reference(noisy_image, fidelity, primal_u, primal_v, dual_p, dual_q):
    noisy = noisy_image[None]
    weight_map = fidelity[None]
    image_u = primal_u[None]
    vector_v = primal_v
    grad_dual = dual_p
    sym_dual = dual_q
    lower_masks, upper_masks = edge_masks(noisy_image.shape)
    bar_u = image_u
    bar_v = vector_v
    for step_index in range(ITERS):
        next_u = [shift_next(bar_u, 3 - component) for component in range(3)]
        prev_v = [shift_prev(bar_v, 3 - component) for component in range(3)]
        grad_dual, sym_dual = dual_update(bar_u, bar_v, grad_dual, sym_dual, next_u, prev_v, lower_masks, upper_masks)
        prev_p = [shift_prev(grad_dual[component:component + 1], 3 - component) for component in range(3)]
        next_q = [shift_next(q_rows(sym_dual, component), 3 - component) for component in range(3)]
        new_u, new_v = primal_update(image_u, vector_v, grad_dual, sym_dual, noisy, weight_map, prev_p, next_q, lower_masks, upper_masks)
        bar_u = 2.0 * new_u - image_u
        bar_v = 2.0 * new_v - vector_v
        image_u = new_u
        vector_v = new_v
    return (image_u[0], vector_v, grad_dual, sym_dual)
```

```python
import jax
import jax.numpy as jnp
from jax import lax
from jax.experimental import pallas as pl
from jax.experimental.pallas import tpu as pltpu
from jax.sharding import PartitionSpec as P

ITERS = 3
AXES = ("gx", "gy", "gz")
ALPHA1, ALPHA0, SIGMA, TAU = 0.5, 1.0, 0.2, 0.2
XX, YY, ZZ, XY, XZ, YZ = range(6)
PARTS = ((XX, XY, XZ), (XY, YY, YZ), (XZ, YZ, ZZ))
MESH = pl.DeviceIdType.MESH
Z_UP, Z_DOWN, X_UP, X_DOWN, Y_UP, Y_DOWN, XY_A, XY_B, XZ_A, XZ_B, YZ_A, YZ_B = range(12)
WAYS = (
    (0, 0, 1), (0, 0, -1), (1, 0, 0), (-1, 0, 0), (0, 1, 0), (0, -1, 0),
    (1, -1, 0), (-1, 1, 0), (1, 0, -1), (-1, 0, 1), (0, 1, -1), (0, -1, 1),
)


def kernel(
    noisy_in, fid_in, u_in, v_in, p_in, q_in,
    u_out, v_out, p_out, q_out,
    bar, gain, offset, face,
    z_lo, z_hi, x_lo, x_hi, y_lo, y_hi, d_a, d_b, d_c, d_d, d_e, d_g,
    zp, zq, yp, yq, xs_own, xp, xq, cv, cp,
    load_sem, send_sem, recv_sem, first_send, first_recv,
):
    zs, ys, xs = u_in.shape
    blocks = ys // 8
    pairs = zs * blocks
    half_lanes = 2 * pairs
    place = [lax.axis_index(a) for a in AXES]
    count = [lax.axis_size(a) for a in AXES]
    below = [place[i] > 0 for i in range(3)]
    above = [place[i] < count[i] - 1 for i in range(3)]

    def exists(way):
        there = None
        for i, by in enumerate(way):
            if by:
                one = above[i] if by > 0 else below[i]
                there = one if there is None else jnp.logical_and(there, one)
        return there

    def target(way):
        return {AXES[i]: place[i] + by for i, by in enumerate(way) if by}

    goes = [exists(way) for way in WAYS]
    comes = [exists(tuple(-by for by in way)) for way in WAYS]
    peers = sum(there.astype(jnp.int32) for there in goes)

    barrier = pltpu.get_barrier_semaphore()
    for way, there in zip(WAYS, goes):
        @pl.when(there)
        def _():
            pl.semaphore_signal(barrier, inc=1, device_id=target(way), device_id_type=MESH)

    u_face, xf, top_face = pl.ds(0, 4), pl.ds(4, 2), pl.ds(6, 4)
    loads = [
        pltpu.make_async_copy(u_in, bar.at[0], load_sem.at[0]),
        pltpu.make_async_copy(v_in, bar.at[pl.ds(1, 3)], load_sem.at[1]),
        pltpu.make_async_copy(u_in.at[:, 0], face.at[0], load_sem.at[2]),
        pltpu.make_async_copy(v_in.at[:, :, 0], face.at[pl.ds(1, 3)], load_sem.at[3]),
        pltpu.make_async_copy(u_in.at[:, ys - 1], face.at[6], load_sem.at[4]),
        pltpu.make_async_copy(v_in.at[:, :, ys - 1], face.at[pl.ds(7, 3)], load_sem.at[5]),
        pltpu.make_async_copy(p_in, p_out, load_sem.at[6]),
        pltpu.make_async_copy(q_in, q_out, load_sem.at[7]),
        pltpu.make_async_copy(noisy_in, offset, load_sem.at[8]),
        pltpu.make_async_copy(fid_in, gain, load_sem.at[9]),
        pltpu.make_async_copy(u_in, u_out, load_sem.at[10]),
        pltpu.make_async_copy(v_in, v_out, load_sem.at[11]),
    ]
    for load in loads:
        load.start()

    def clear(there, *refs):
        @pl.when(jnp.logical_not(there))
        def _():
            for ref in refs:
                ref[...] = jnp.zeros(ref.shape, jnp.float32)

    clear(below[0], x_lo, xp)
    clear(above[0], x_hi, xq)
    clear(below[1], y_lo, yp)
    clear(above[1], y_hi, yq)
    clear(below[2], z_lo, zp)
    clear(above[2], z_hi, zq)
    for way, ref in zip(WAYS[6:], (d_a, d_b, d_c, d_d, d_e, d_g)):
        clear(exists(tuple(-by for by in way)), ref)

    lane = lax.broadcasted_iota(jnp.int32, (8, xs), 1)
    sub = lax.broadcasted_iota(jnp.int32, (8, xs), 0)
    pair = lane >> 1
    odd = (lane & 1) == 1
    first_lane, last_lane = lane == 0, lane == xs - 1
    first_row, last_row = sub == 0, sub == 7
    of_block = pair & (blocks - 1)
    first_block, last_block = of_block == 0, of_block == blocks - 1
    first_z, last_z = pair < blocks, jnp.logical_and(pair >= pairs - blocks, pair < pairs)

    def factor(flag):
        return jnp.where(flag, jnp.float32(1), jnp.float32(0))

    up_x = jnp.where(last_lane, factor(above[0]), 1.0)
    lo_x = jnp.where(first_lane, factor(below[0]), 1.0)
    up_y_last = jnp.where(last_row, factor(above[1]), 1.0)
    lo_y_first = jnp.where(first_row, factor(below[1]), 1.0)

    def rows(b, by=0):
        return pl.ds(8 * b + by, 8)

    def turn_lanes(value, by):
        return value if isinstance(by, int) and by % xs == 0 else pltpu.roll(value, by % xs if isinstance(by, int) else by, 1)

    def turn_rows(value, by):
        return pltpu.roll(value, by % 8, 0)

    def flush(later):
        for ref, at, value in later:
            ref[at + (slice(None),)] = value
        later.clear()

    def up_z(z):
        return factor(jnp.logical_or(z < zs - 1, above[2]))

    def lo_z(z):
        return factor(jnp.logical_or(z > 0, below[2]))

    def up_y(b, value):
        return up_y_last * value if b == blocks - 1 else value

    def lo_y(b, value):
        return lo_y_first * value if b == 0 else value

    def next_x(value):
        return jnp.where(last_lane, 0.0, pltpu.roll(value, xs - 1, 1))

    def prev_x(value):
        return jnp.where(first_lane, 0.0, pltpu.roll(value, 1, 1))

    def next_y(ref, k, z, b, value):
        if b < blocks - 1:
            return ref[k, z, rows(b, 1), :]
        return jnp.where(last_row, 0.0, pltpu.roll(value, 7, 0))

    def prev_y(ref, k, z, b, value):
        if b > 0:
            return ref[k, z, rows(b, -1), :]
        return jnp.where(first_row, 0.0, pltpu.roll(value, 1, 0))

    def next_z(ref, k, z, b):
        if isinstance(z, int):
            return ref[k, z + 1, rows(b), :] if z < zs - 1 else jnp.zeros((8, xs), jnp.float32)
        return factor(z < zs - 1) * ref[k, jnp.minimum(z + 1, zs - 1), rows(b), :]

    def prev_z(ref, k, z, b):
        if isinstance(z, int):
            return ref[k, z - 1, rows(b), :] if z > 0 else jnp.zeros((8, xs), jnp.float32)
        return factor(z > 0) * ref[k, jnp.maximum(z - 1, 0), rows(b), :]

    def shrink_p(t):
        size = t[0] * t[0] + t[1] * t[1] + t[2] * t[2]
        scale = jnp.minimum(1.0, ALPHA1 * lax.rsqrt(size))
        return [scale * part for part in t]

    def shrink_q(s):
        size = (s[XX] * s[XX] + s[YY] * s[YY] + s[ZZ] * s[ZZ]) + 2.0 * (
            s[XY] * s[XY] + s[XZ] * s[XZ] + s[YZ] * s[YZ]
        )
        scale = jnp.minimum(1.0, ALPHA0 * lax.rsqrt(size))
        return [scale * part for part in s]

    half = 0.5 * SIGMA

    def grow_q(q, dx, dy, dz):
        return [
            q[XX] + SIGMA * dx[0], q[YY] + SIGMA * dy[1], q[ZZ] + SIGMA * dz[2],
            q[XY] + half * (dy[0] + dx[1]), q[XZ] + half * (dz[0] + dx[2]),
            q[YZ] + half * (dz[1] + dy[2]),
        ]

    def keep(flag, value):
        return jnp.where(flag, value, 0.0)

    def pack(packed, value, base, j):
        return jnp.where(pair == base + j, pltpu.roll(value, 2 * (base + j) + 1, 1), packed)

    def pack_bar(packed, values, z, b):
        j = z * blocks + b
        packed[0] = pack(packed[0], values[0], 0, j)
        packed[0] = pack(packed[0], values[1], pairs, j)
        packed[1] = pack(packed[1], values[2], 0, j)
        packed[1] = pack(packed[1], values[3], pairs, j)

    def message(src, dst, way, send, recv):
        return pltpu.make_async_remote_copy(
            src_ref=src, dst_ref=dst, send_sem=send, recv_sem=recv,
            device_id=target(WAYS[way]), device_id_type=MESH,
        )

    exchanges = []
    for s in range(ITERS):
        ends = (
            (bar.at[:, zs - 1], z_lo.at[s]),
            (bar.at[:, 0], z_hi.at[s]),
            (face.at[xf], x_lo.at[s]),
            (face.at[xf], x_hi.at[s]),
            (face.at[top_face], y_lo.at[s]),
            (face.at[u_face], y_hi.at[s]),
            (face.at[pl.ds(0, 6)], d_a.at[s]),
            (face.at[pl.ds(4, 6)], d_b.at[s]),
            (face.at[xf], d_c.at[s]),
            (face.at[xf], d_d.at[s]),
            (face.at[top_face, pl.ds(0, 1)], d_e.at[s, :, pl.ds(0, 1)]),
            (face.at[u_face, pl.ds(zs - 1, 1)], d_g.at[s, :, pl.ds(zs - 1, 1)]),
        )
        exchanges.append([
            (message(src, dst, k, send_sem.at[s, k], recv_sem.at[s, k]), goes[k], comes[k])
            for k, (src, dst) in enumerate(ends)
        ])
    duals = [
        (message(src, dst, way, first_send.at[k], first_recv.at[k]), goes[way], comes[way])
        for k, (src, dst, way) in enumerate((
            (p_in.at[:, zs - 1], zp, Z_UP),
            (q_in.at[:, 0], zq, Z_DOWN),
            (p_in.at[:, :, ys - 1], yp, Y_UP),
            (q_in.at[:, :, 0], yq, Y_DOWN),
            (xs_own, xp, X_UP),
            (xs_own, xq, X_DOWN),
        ))
    ]

    def start(moves):
        for copy, there, _ in moves:
            @pl.when(there)
            def _():
                copy.start()

    def sent(moves):
        for copy, there, _ in moves:
            @pl.when(there)
            def _():
                copy.wait_send()

    def got(moves):
        for copy, _, there in moves:
            @pl.when(there)
            def _():
                copy.wait_recv()

    empty = jnp.zeros((8, xs), jnp.float32)

    def each(low, high, body, carry):
        def turn(j, carry):
            one = list(carry)
            body(low + 2 * j, one)
            body(low + 2 * j + 1, one)
            return tuple(one)

        return lax.fori_loop(0, (high - low) // 2, turn, tuple(carry))

    def dual_inside(z, _):
        later = []
        z_up, z_lo_ = up_z(z), lo_z(z)
        for b in range(blocks):
            r = rows(b)
            u = bar[0, z, r, :]
            v = [bar[1 + k, z, r, :] for k in range(3)]
            slopes = (
                next_x(u) - up_x * u,
                next_y(bar, 0, z, b, u) - up_y(b, u),
                next_z(bar, 0, z, b) - z_up * u,
            )
            for k in range(3):
                later.append((p_out, (k, z, r), p_out[k, z, r, :] + SIGMA * (slopes[k] - v[k])))
            dx = [lo_x * v[k] - prev_x(v[k]) for k in range(3)]
            dy = [lo_y(b, v[k]) - prev_y(bar, 1 + k, z, b, v[k]) for k in range(3)]
            dz = [z_lo_ * v[k] - prev_z(bar, 1 + k, z, b) for k in range(3)]
            for k, new in enumerate(grow_q([q_out[k, z, r, :] for k in range(6)], dx, dy, dz)):
                later.append((q_out, (k, z, r), new))
        flush(later)

    def line_up(s):
        cv[0] = jnp.where(odd, turn_lanes(x_hi[s, 0], half_lanes - 2), x_lo[s, 0])
        cv[1] = turn_lanes(x_lo[s, 1], half_lanes)
        cv[2] = x_lo[s, 1]

    def dual(z, s):
        later = []
        for b in range(blocks):
            r = rows(b)
            by = half_lanes - 2 * (z * blocks + b)
            from_x = [turn_lanes(cv[k], by) for k in range(3)]
            t = [p_out[k, z, r, :] for k in range(3)]
            t[0] = t[0] + SIGMA * jnp.where(last_lane, from_x[0], 0.0)
            if b == blocks - 1:
                t[1] = t[1] + SIGMA * jnp.where(last_row, y_hi[s, 0, pl.ds(z, 1), :], 0.0)
            if isinstance(z, int) and z == zs - 1:
                t[2] = t[2] + SIGMA * z_hi[s, 0, r, :]
            for k, new in enumerate(shrink_p(t)):
                later.append((p_out, (k, z, r), new))
            hx = [jnp.where(first_lane, part, 0.0) for part in from_x]
            q = [q_out[k, z, r, :] for k in range(6)]
            q[XX] = q[XX] - SIGMA * hx[0]
            q[XY] = q[XY] - half * hx[1]
            q[XZ] = q[XZ] - half * hx[2]
            if b == 0:
                hy = [jnp.where(first_row, y_lo[s, 1 + k, pl.ds(z, 1), :], 0.0) for k in range(3)]
                q[YY] = q[YY] - SIGMA * hy[1]
                q[XY] = q[XY] - half * hy[0]
                q[YZ] = q[YZ] - half * hy[2]
            if isinstance(z, int) and z == 0:
                hz = [z_lo[s, 1 + k, r, :] for k in range(3)]
                q[ZZ] = q[ZZ] - SIGMA * hz[2]
                q[XZ] = q[XZ] - half * hz[0]
                q[YZ] = q[YZ] - half * hz[1]
            for k, new in enumerate(shrink_q(q)):
                later.append((q_out, (k, z, r), new))
        flush(later)

    def halo_x(s):
        own = [face[4], face[5]]
        up_yc = jnp.where(jnp.logical_and(last_row, last_block), factor(above[1]), 1.0)
        lo_yc = jnp.where(jnp.logical_and(first_row, first_block), factor(below[1]), 1.0)
        up_zc = jnp.where(last_z, factor(above[2]), 1.0)
        lo_zc = jnp.where(first_z, factor(below[2]), 1.0)
        got0, got1 = x_lo[s, 0], x_lo[s, 1]
        u = got0
        v = [turn_lanes(got0, half_lanes), got1, turn_lanes(got1, half_lanes)]
        moved = turn_rows(u, -1)
        edge_y = turn_lanes(turn_rows(d_a[s, 4], -1), 2 * (blocks - 1))
        ahead_y = jnp.where(last_row, jnp.where(last_block, edge_y, turn_lanes(moved, -2)), moved)
        ahead_z = jnp.where(
            last_z, turn_lanes(d_c[s, 0], half_lanes - 2 * blocks), turn_lanes(u, -2 * blocks)
        )
        slopes = (turn_lanes(own[0], -1) - u, ahead_y - up_yc * u, ahead_z - up_zc * u)
        p = shrink_p([xp[k] + SIGMA * (slopes[k] - v[k]) for k in range(3)])
        p = [keep(below[0], part) for part in p]

        got0, got1 = x_hi[s, 0], x_hi[s, 1]
        v = [turn_lanes(got0, half_lanes), got1, turn_lanes(got1, half_lanes)]
        mine = [turn_lanes(own[0], half_lanes + 1), turn_lanes(own[1], 1), turn_lanes(own[1], half_lanes + 1)]
        where = ((0, half_lanes), (1, 0), (1, half_lanes))
        dx, dy, dz = [], [], []
        for k, (h, base) in enumerate(where):
            dx.append(v[k] - mine[k])
            moved = turn_rows(v[k], 1)
            edge_y = turn_lanes(turn_rows(d_b[s, h], 1), -base - 2 * (blocks - 1))
            behind_y = jnp.where(first_row, jnp.where(first_block, edge_y, turn_lanes(moved, 2)), moved)
            dy.append(lo_yc * v[k] - behind_y)
            edge_z = turn_lanes(d_d[s, h], -base - 2 * blocks * (zs - 1))
            dz.append(lo_zc * v[k] - jnp.where(first_z, edge_z, turn_lanes(v[k], 2 * blocks)))
        q = shrink_q(grow_q([xq[k] for k in range(6)], dx, dy, dz))
        q = [keep(above[0], part) for part in q]
        for k in range(3):
            xp[k] = p[k]
        for k in range(6):
            xq[k] = q[k]
        cp[0] = jnp.where(odd, turn_lanes(q[XX], half_lanes - 2), turn_lanes(p[0], half_lanes))
        cp[1] = turn_lanes(q[XY], half_lanes - 2)
        cp[2] = turn_lanes(q[XZ], half_lanes - 2)

    def halo_y(s):
        up_zr = jnp.where(last_row, factor(above[2]), 1.0)
        lo_zr = jnp.where(first_row, factor(below[2]), 1.0)
        u = y_lo[s, 0]
        slopes = (
            turn_lanes(jnp.where(first_lane, d_b[s, 2], u), -1) - up_x * u,
            face[0] - u,
            jnp.where(last_row, d_e[s, 0, pl.ds(0, 1), :], turn_rows(u, -1)) - up_zr * u,
        )
        p = shrink_p([yp[k] + SIGMA * (slopes[k] - y_lo[s, 1 + k]) for k in range(3)])
        v = [y_hi[s, 1 + k] for k in range(3)]
        dx = [lo_x * v[k] - turn_lanes(jnp.where(last_lane, d_a[s, 1 + k], v[k]), 1) for k in range(3)]
        dy = [v[k] - face[7 + k] for k in range(3)]
        dz = [
            lo_zr * v[k] - jnp.where(first_row, d_g[s, 1 + k, pl.ds(zs - 1, 1), :], turn_rows(v[k], 1))
            for k in range(3)
        ]
        q = shrink_q(grow_q([yq[k] for k in range(6)], dx, dy, dz))
        for k in range(3):
            yp[k] = keep(below[1], p[k])
        for k in range(6):
            yq[k] = keep(above[1], q[k])

    def halo_z(s):
        later = []
        for b in range(blocks):
            r = rows(b)
            u = z_lo[s, 0, r, :]
            edge_x = turn_lanes(d_d[s, 0], xs - 2 - 2 * (blocks * (zs - 1) + b))
            if b < blocks - 1:
                ahead_y = z_lo[s, 0, rows(b, 1), :]
            else:
                ahead_y = jnp.where(last_row, d_g[s, 0, pl.ds(zs - 1, 1), :], turn_rows(u, -1))
            slopes = (
                jnp.where(last_lane, edge_x, turn_lanes(u, -1)) - up_x * u,
                ahead_y - up_y(b, u),
                bar[0, 0, r, :] - u,
            )
            p = shrink_p([zp[k, r, :] + SIGMA * (slopes[k] - z_lo[s, 1 + k, r, :]) for k in range(3)])
            for k in range(3):
                later.append((zp, (k, r), keep(below[2], p[k])))

            v = [z_hi[s, 1 + k, r, :] for k in range(3)]
            where = ((0, half_lanes), (1, 0), (1, half_lanes))
            dx, dy, dz = [], [], []
            for k, (h, base) in enumerate(where):
                edge_x = turn_lanes(d_c[s, h], -base - 2 * b)
                dx.append(lo_x * v[k] - jnp.where(first_lane, edge_x, turn_lanes(v[k], 1)))
                if b > 0:
                    behind_y = z_hi[s, 1 + k, rows(b, -1), :]
                else:
                    behind_y = jnp.where(first_row, d_e[s, 1 + k, pl.ds(0, 1), :], turn_rows(v[k], 1))
                dy.append(lo_y(b, v[k]) - behind_y)
                dz.append(v[k] - bar[1 + k, zs - 1, r, :])
            q = shrink_q(grow_q([zq[k, r, :] for k in range(6)], dx, dy, dz))
            for k in range(6):
                later.append((zq, (k, r), keep(above[2], q[k])))
        flush(later)

    def primal(z, packed, last):
        later = []
        z_up, z_lo_ = up_z(z), lo_z(z)
        at_start = isinstance(z, int) and z == 0
        at_end = isinstance(z, int) and z == zs - 1
        for b in range(blocks):
            r = rows(b)
            by = half_lanes - 2 * (z * blocks + b)
            from_x = [turn_lanes(cp[k], by) for k in range(3)]
            p = [p_out[k, z, r, :] for k in range(3)]
            before_x = jnp.where(first_lane, from_x[0], pltpu.roll(p[0], 1, 1))
            if b > 0:
                before_y = p_out[1, z, rows(b, -1), :]
            else:
                before_y = jnp.where(first_row, yp[1, pl.ds(z, 1), :], pltpu.roll(p[1], 1, 0))
            before_z = zp[2, r, :] if at_start else p_out[2, z - 1, r, :]
            div = (up_x * p[0] - before_x) + (up_y(b, p[1]) - before_y) + (z_up * p[2] - before_z)
            old = u_out[z, r, :]
            new = (old + TAU * div) * gain[z, r, :] + offset[z, r, :]
            later.append((u_out, (z, r), new))
            ahead = [2.0 * new - old]
            q = [q_out[k, z, r, :] for k in range(6)]
            for k, (ax, ay, az) in enumerate(PARTS):
                after_x = jnp.where(last_lane, from_x[k], pltpu.roll(q[ax], xs - 1, 1))
                if b < blocks - 1:
                    after_y = q_out[ay, z, rows(b, 1), :]
                else:
                    after_y = jnp.where(last_row, yq[ay, pl.ds(z, 1), :], pltpu.roll(q[ay], 7, 0))
                after_z = zq[az, r, :] if at_end else q_out[az, z + 1, r, :]
                div2 = (
                    (after_x - lo_x * q[ax]) + (after_y - lo_y(b, q[ay])) + (after_z - z_lo_ * q[az])
                )
                old = v_out[k, z, r, :]
                new = old + TAU * (p[k] + div2)
                later.append((v_out, (k, z, r), new))
                ahead.append(2.0 * new - old)
            if not last:
                for k in range(4):
                    later.append((bar, (k, z, r), ahead[k]))
                    if b == 0:
                        later.append((face, (k, pl.ds(z, 1)), ahead[k][0:1, :]))
                    if b == blocks - 1:
                        later.append((face, (6 + k, pl.ds(z, 1)), ahead[k][7:8, :]))
                pack_bar(packed, ahead, z, b)
        flush(later)

    for load in loads[:2]:
        load.wait()
    pl.semaphore_wait(barrier, peers)
    start(exchanges[0][:2])
    start(duals[:4])
    for load in loads[2:6]:
        load.wait()
    start(exchanges[0][4:6])

    def first_faces(z, packed):
        for b in range(blocks):
            pack_bar(packed, [bar[k, z, rows(b), :] for k in range(4)], z, b)

    packed = each(0, zs, first_faces, (empty, empty))
    face[4] = packed[0]
    face[5] = packed[1]
    start(exchanges[0][2:4])
    start(exchanges[0][6:])

    for load in loads[6:8]:
        load.wait()

    def dual_faces(z, packed):
        for b in range(blocks):
            for k in range(6):
                value = q_out[k, z, rows(b), :]
                if k < 3:
                    value = jnp.where(last_lane, p_out[k, z, rows(b), :], value)
                packed[k] = pack(packed[k], value, 0, z * blocks + b)

    for k, value in enumerate(each(0, zs, dual_faces, (empty,) * 6)):
        xs_own[k] = value
    start(duals[4:])

    for load in loads[8:]:
        load.wait()

    def prepare(z, carry):
        weight = TAU * gain[z]
        inverse = 1.0 / (1.0 + weight)
        gain[z] = inverse
        offset[z] = weight * offset[z] * inverse
        return carry

    lax.fori_loop(0, zs, prepare, 0)

    def two_faces(body, carry):
        for z in (0, zs - 1):
            body(z, carry)

    for s in range(ITERS):
        last = s == ITERS - 1
        moves = exchanges[s]
        each(0, zs, dual_inside, ())
        got(moves[2:6])
        line_up(s)
        each(1, zs - 1, lambda z, _: dual(z, s), ())
        got(moves[6:])
        if s == 0:
            got(duals[2:])
        halo_x(s)
        halo_y(s)
        sent(moves[2:])
        packed = list(each(2, zs - 2, lambda z, packed: primal(z, packed, last), (empty, empty)))
        got(moves[:2])
        sent(moves[:2])
        if s == 0:
            got(duals[:2])
            sent(duals)
        halo_z(s)
        for z in (0, zs - 1):
            dual(z, s)
        for z in (0, zs - 1):
            primal(z, packed, last)
        if not last:
            start(exchanges[s + 1][:2])
        for z in (1, zs - 2):
            primal(z, packed, last)
        if not last:
            face[4] = packed[0]
            face[5] = packed[1]
            start(exchanges[s + 1][2:])


def copy_out(u_in, v_in, p_in, q_in, u_out, v_out, p_out, q_out, sems):
    pairs = ((q_in, q_out), (p_in, p_out), (v_in, v_out), (u_in, u_out))
    copies = [pltpu.make_async_copy(a, b, sems.at[i]) for i, (a, b) in enumerate(pairs)]
    for copy in copies:
        copy.start()
    for copy in copies:
        copy.wait()


def per_device(noisy_image, fidelity, primal_u, primal_v, dual_p, dual_q):
    zs, ys, xs = primal_u.shape
    blocks = ys // 8
    assert zs == 8 and ys % 8 == 0 and blocks & (blocks - 1) == 0 and 4 * zs * blocks == xs == 128
    f32 = jnp.float32

    def vmem(*shape):
        return pltpu.VMEM(shape, f32)

    results = pl.pallas_call(
        kernel,
        out_shape=tuple(pltpu.VMEM(a.shape, f32) for a in (primal_u, primal_v, dual_p, dual_q)),
        in_specs=[pl.BlockSpec(memory_space=pl.ANY)] * 6,
        out_specs=tuple([pl.BlockSpec(memory_space=pltpu.VMEM)] * 4),
        scratch_shapes=[
            vmem(4, zs, ys, xs),
            vmem(zs, ys, xs),
            vmem(zs, ys, xs),
            vmem(10, 8, xs),
            vmem(ITERS, 4, ys, xs),
            vmem(ITERS, 4, ys, xs),
            vmem(ITERS, 2, 8, xs),
            vmem(ITERS, 2, 8, xs),
            vmem(ITERS, 4, 8, xs),
            vmem(ITERS, 4, 8, xs),
            vmem(ITERS, 6, 8, xs),
            vmem(ITERS, 6, 8, xs),
            vmem(ITERS, 2, 8, xs),
            vmem(ITERS, 2, 8, xs),
            vmem(ITERS, 4, 8, xs),
            vmem(ITERS, 4, 8, xs),
            vmem(3, ys, xs),
            vmem(6, ys, xs),
            vmem(3, 8, xs),
            vmem(6, 8, xs),
            vmem(6, 8, xs),
            vmem(6, 8, xs),
            vmem(6, 8, xs),
            vmem(3, 8, xs),
            vmem(3, 8, xs),
            pltpu.SemaphoreType.DMA((12,)),
            pltpu.SemaphoreType.DMA((ITERS, 12)),
            pltpu.SemaphoreType.DMA((ITERS, 12)),
            pltpu.SemaphoreType.DMA((6,)),
            pltpu.SemaphoreType.DMA((6,)),
        ],
        compiler_params=pltpu.CompilerParams(collective_id=0, has_side_effects=True),
        name="tgv",
    )(noisy_image, fidelity, primal_u, primal_v, dual_p, dual_q)
    return pl.pallas_call(
        copy_out,
        out_shape=tuple(jax.ShapeDtypeStruct(a.shape, f32) for a in results),
        in_specs=[pl.BlockSpec(memory_space=pltpu.VMEM)] * 4,
        out_specs=tuple([pl.BlockSpec(memory_space=pl.ANY)] * 4),
        scratch_shapes=[pltpu.SemaphoreType.DMA((4,))],
        name="out",
    )(*[pltpu.with_memory_space_constraint(r, pltpu.VMEM) for r in results])


def solution(mesh):
    scalar, stack = P("gz", "gy", "gx"), P(None, "gz", "gy", "gx")
    return jax.shard_map(
        per_device,
        mesh=mesh,
        in_specs=(scalar, scalar, scalar, stack, stack, stack),
        out_specs=(scalar, stack, stack, stack),
        check_vma=False,
    )
```

```python
import jax
import jax.numpy as jnp
from jax import lax
from jax.experimental import pallas as pl
from jax.experimental.pallas import tpu as pltpu
from jax.sharding import PartitionSpec as P

ITERS = 3
AXES = ("gx", "gy", "gz")
ALPHA1, ALPHA0, SIGMA, TAU = 0.5, 1.0, 0.2, 0.2
XX, YY, ZZ, XY, XZ, YZ = range(6)
PARTS = ((XX, XY, XZ), (XY, YY, YZ), (XZ, YZ, ZZ))
MESH = pl.DeviceIdType.MESH
Z_UP, Z_DOWN, X_UP, X_DOWN, Y_UP, Y_DOWN, XY_A, XY_B, XZ_A, XZ_B, YZ_A, YZ_B = range(12)
WAYS = (
    (0, 0, 1), (0, 0, -1), (1, 0, 0), (-1, 0, 0), (0, 1, 0), (0, -1, 0),
    (1, -1, 0), (-1, 1, 0), (1, 0, -1), (-1, 0, 1), (0, 1, -1), (0, -1, 1),
)


def kernel(
    noisy_in, fid_in, u_in, v_in, p_in, q_in,
    u_out, v_out, p_out, q_out,
    bar, gain, offset, face,
    z_lo, z_hi, x_lo, x_hi, y_lo, y_hi, d_a, d_b, d_c, d_d, d_e, d_g,
    zp, zq, yp, yq, xs_own, xp, xq, cv, cp,
    load_sem, send_sem, recv_sem, first_send, first_recv,
):
    zs, ys, xs = u_in.shape
    blocks = ys // 8
    pairs = zs * blocks
    half_lanes = 2 * pairs
    place = [lax.axis_index(a) for a in AXES]
    count = [lax.axis_size(a) for a in AXES]
    below = [place[i] > 0 for i in range(3)]
    above = [place[i] < count[i] - 1 for i in range(3)]

    def exists(way):
        there = None
        for i, by in enumerate(way):
            if by:
                one = above[i] if by > 0 else below[i]
                there = one if there is None else jnp.logical_and(there, one)
        return there

    def target(way):
        return {AXES[i]: place[i] + by for i, by in enumerate(way) if by}

    goes = [exists(way) for way in WAYS]
    comes = [exists(tuple(-by for by in way)) for way in WAYS]
    peers = sum(there.astype(jnp.int32) for there in goes)

    u_face, xf, top_face = pl.ds(0, 4), pl.ds(4, 2), pl.ds(6, 4)
    loads = [
        pltpu.make_async_copy(u_in, bar.at[0], load_sem.at[0]),
        pltpu.make_async_copy(v_in, bar.at[pl.ds(1, 3)], load_sem.at[1]),
        pltpu.make_async_copy(u_in.at[:, 0], face.at[0], load_sem.at[2]),
        pltpu.make_async_copy(v_in.at[:, :, 0], face.at[pl.ds(1, 3)], load_sem.at[3]),
        pltpu.make_async_copy(u_in.at[:, ys - 1], face.at[6], load_sem.at[4]),
        pltpu.make_async_copy(v_in.at[:, :, ys - 1], face.at[pl.ds(7, 3)], load_sem.at[5]),
        pltpu.make_async_copy(p_in, p_out, load_sem.at[6]),
        pltpu.make_async_copy(q_in, q_out, load_sem.at[7]),
        pltpu.make_async_copy(noisy_in, offset, load_sem.at[8]),
        pltpu.make_async_copy(fid_in, gain, load_sem.at[9]),
        pltpu.make_async_copy(u_in, u_out, load_sem.at[10]),
        pltpu.make_async_copy(v_in, v_out, load_sem.at[11]),
    ]
    for load in loads[:8]:
        load.start()
    barrier = pltpu.get_barrier_semaphore()
    for way, there in zip(WAYS, goes):
        @pl.when(there)
        def _():
            pl.semaphore_signal(barrier, inc=1, device_id=target(way), device_id_type=MESH)
    for load in loads[8:]:
        load.start()

    def clear(there, *refs):
        @pl.when(jnp.logical_not(there))
        def _():
            for ref in refs:
                ref[...] = jnp.zeros(ref.shape, jnp.float32)

    clear(below[0], x_lo, xp)
    clear(above[0], x_hi, xq)
    clear(below[1], y_lo, yp)
    clear(above[1], y_hi, yq)
    clear(below[2], z_lo, zp)
    clear(above[2], z_hi, zq)
    for way, ref in zip(WAYS[6:], (d_a, d_b, d_c, d_d, d_e, d_g)):
        clear(exists(tuple(-by for by in way)), ref)

    lane = lax.broadcasted_iota(jnp.int32, (8, xs), 1)
    sub = lax.broadcasted_iota(jnp.int32, (8, xs), 0)
    pair = lane >> 1
    odd = (lane & 1) == 1
    first_lane, last_lane = lane == 0, lane == xs - 1
    first_row, last_row = sub == 0, sub == 7
    of_block = pair & (blocks - 1)
    first_block, last_block = of_block == 0, of_block == blocks - 1
    first_z, last_z = pair < blocks, jnp.logical_and(pair >= pairs - blocks, pair < pairs)

    def factor(flag):
        return jnp.where(flag, jnp.float32(1), jnp.float32(0))

    up_x = jnp.where(last_lane, factor(above[0]), 1.0)
    lo_x = jnp.where(first_lane, factor(below[0]), 1.0)
    up_y_last = jnp.where(last_row, factor(above[1]), 1.0)
    lo_y_first = jnp.where(first_row, factor(below[1]), 1.0)

    def rows(b, by=0):
        return pl.ds(8 * b + by, 8)

    def turn_lanes(value, by):
        return value if isinstance(by, int) and by % xs == 0 else pltpu.roll(value, by % xs if isinstance(by, int) else by, 1)

    def turn_rows(value, by):
        return pltpu.roll(value, by % 8, 0)

    def flush(later):
        for ref, at, value in later:
            ref[at + (slice(None),)] = value
        later.clear()

    def up_z(z):
        return factor(jnp.logical_or(z < zs - 1, above[2]))

    def lo_z(z):
        return factor(jnp.logical_or(z > 0, below[2]))

    def up_y(b, value):
        return up_y_last * value if b == blocks - 1 else value

    def lo_y(b, value):
        return lo_y_first * value if b == 0 else value

    def next_x(value):
        return jnp.where(last_lane, 0.0, pltpu.roll(value, xs - 1, 1))

    def prev_x(value):
        return jnp.where(first_lane, 0.0, pltpu.roll(value, 1, 1))

    def next_y(ref, k, z, b, value):
        if b < blocks - 1:
            return ref[k, z, rows(b, 1), :]
        return jnp.where(last_row, 0.0, pltpu.roll(value, 7, 0))

    def prev_y(ref, k, z, b, value):
        if b > 0:
            return ref[k, z, rows(b, -1), :]
        return jnp.where(first_row, 0.0, pltpu.roll(value, 1, 0))

    def next_z(ref, k, z, b):
        if isinstance(z, int):
            return ref[k, z + 1, rows(b), :] if z < zs - 1 else jnp.zeros((8, xs), jnp.float32)
        return factor(z < zs - 1) * ref[k, jnp.minimum(z + 1, zs - 1), rows(b), :]

    def prev_z(ref, k, z, b):
        if isinstance(z, int):
            return ref[k, z - 1, rows(b), :] if z > 0 else jnp.zeros((8, xs), jnp.float32)
        return factor(z > 0) * ref[k, jnp.maximum(z - 1, 0), rows(b), :]

    def shrink_p(t):
        size = t[0] * t[0] + t[1] * t[1] + t[2] * t[2]
        scale = jnp.minimum(1.0, ALPHA1 * lax.rsqrt(size))
        return [scale * part for part in t]

    def shrink_q(s):
        size = (s[XX] * s[XX] + s[YY] * s[YY] + s[ZZ] * s[ZZ]) + 2.0 * (
            s[XY] * s[XY] + s[XZ] * s[XZ] + s[YZ] * s[YZ]
        )
        scale = jnp.minimum(1.0, ALPHA0 * lax.rsqrt(size))
        return [scale * part for part in s]

    half = 0.5 * SIGMA

    def grow_q(q, dx, dy, dz):
        return [
            q[XX] + SIGMA * dx[0], q[YY] + SIGMA * dy[1], q[ZZ] + SIGMA * dz[2],
            q[XY] + half * (dy[0] + dx[1]), q[XZ] + half * (dz[0] + dx[2]),
            q[YZ] + half * (dz[1] + dy[2]),
        ]

    def keep(flag, value):
        return jnp.where(flag, value, 0.0)

    def pack(packed, value, base, j):
        return jnp.where(pair == base + j, pltpu.roll(value, 2 * (base + j) + 1, 1), packed)

    def pack_bar(packed, values, z, b):
        j = z * blocks + b
        packed[0] = pack(packed[0], values[0], 0, j)
        packed[0] = pack(packed[0], values[1], pairs, j)
        packed[1] = pack(packed[1], values[2], 0, j)
        packed[1] = pack(packed[1], values[3], pairs, j)

    def message(src, dst, way, send, recv):
        return pltpu.make_async_remote_copy(
            src_ref=src, dst_ref=dst, send_sem=send, recv_sem=recv,
            device_id=target(WAYS[way]), device_id_type=MESH,
        )

    exchanges = []
    for s in range(ITERS):
        z_up_part = pl.ds(1, 3) if s == 0 else pl.ds(0, 4)
        z_down_part = pl.ds(0, 1) if s == 0 else pl.ds(0, 4)
        ends = (
            (bar.at[z_up_part, zs - 1], z_lo.at[s, z_up_part]),
            (bar.at[z_down_part, 0], z_hi.at[s, z_down_part]),
            (face.at[xf], x_lo.at[s]),
            (face.at[xf], x_hi.at[s]),
            (face.at[top_face], y_lo.at[s]),
            (face.at[u_face], y_hi.at[s]),
            (face.at[xf, pl.ds(0, 1)], d_a.at[s, :, pl.ds(0, 1)]),
            (face.at[xf, pl.ds(7, 1)], d_b.at[s, :, pl.ds(7, 1)]),
            (face.at[xf], d_c.at[s]),
            (face.at[xf], d_d.at[s]),
            (face.at[top_face, pl.ds(0, 1)], d_e.at[s, :, pl.ds(0, 1)]),
            (face.at[u_face, pl.ds(zs - 1, 1)], d_g.at[s, :, pl.ds(zs - 1, 1)]),
        )
        exchanges.append([
            (message(src, dst, k, send_sem.at[s, k], recv_sem.at[s, k]), goes[k], comes[k])
            for k, (src, dst) in enumerate(ends)
        ])
    duals = [
        (message(src, dst, way, first_send.at[k], first_recv.at[k]), goes[way], comes[way])
        for k, (src, dst, way) in enumerate((
            (p_out.at[:, zs - 1], zp, Z_UP),
            (q_out.at[:, 0], zq, Z_DOWN),
            (p_in.at[:, :, ys - 1], yp, Y_UP),
            (q_in.at[:, :, 0], yq, Y_DOWN),
            (xs_own, xp, X_UP),
            (xs_own, xq, X_DOWN),
        ))
    ]

    def start(moves):
        for copy, there, _ in moves:
            @pl.when(there)
            def _():
                copy.start()

    def sent(moves):
        for copy, there, _ in moves:
            @pl.when(there)
            def _():
                copy.wait_send()

    def got(moves):
        for copy, _, there in moves:
            @pl.when(there)
            def _():
                copy.wait_recv()

    empty = jnp.zeros((8, xs), jnp.float32)

    def each(low, high, body, carry):
        def turn(j, carry):
            one = list(carry)
            body(low + 2 * j, one)
            body(low + 2 * j + 1, one)
            return tuple(one)

        return lax.fori_loop(0, (high - low) // 2, turn, tuple(carry))

    def dual_inside(z, _):
        later = []
        z_up, z_lo_ = up_z(z), lo_z(z)
        for b in range(blocks):
            r = rows(b)
            u = bar[0, z, r, :]
            v = [bar[1 + k, z, r, :] for k in range(3)]
            slopes = (
                next_x(u) - up_x * u,
                next_y(bar, 0, z, b, u) - up_y(b, u),
                next_z(bar, 0, z, b) - z_up * u,
            )
            for k in range(3):
                later.append((p_out, (k, z, r), p_out[k, z, r, :] + SIGMA * (slopes[k] - v[k])))
            dx = [lo_x * v[k] - prev_x(v[k]) for k in range(3)]
            dy = [lo_y(b, v[k]) - prev_y(bar, 1 + k, z, b, v[k]) for k in range(3)]
            dz = [z_lo_ * v[k] - prev_z(bar, 1 + k, z, b) for k in range(3)]
            for k, new in enumerate(grow_q([q_out[k, z, r, :] for k in range(6)], dx, dy, dz)):
                later.append((q_out, (k, z, r), new))
        flush(later)

    def line_up(s):
        cv[0] = jnp.where(odd, turn_lanes(x_hi[s, 0], half_lanes - 2), x_lo[s, 0])
        cv[1] = turn_lanes(x_lo[s, 1], half_lanes)
        cv[2] = x_lo[s, 1]

    def dual(z, s, for_p=True, for_q=True):
        later = []
        for b in range(blocks):
            r = rows(b)
            by = half_lanes - 2 * (z * blocks + b)
            from_x = [turn_lanes(cv[k], by) for k in range(3 if for_q else 1)]
            if for_p:
                t = [p_out[k, z, r, :] for k in range(3)]
                t[0] = t[0] + SIGMA * jnp.where(last_lane, from_x[0], 0.0)
                if b == blocks - 1:
                    t[1] = t[1] + SIGMA * jnp.where(last_row, y_hi[s, 0, pl.ds(z, 1), :], 0.0)
                if isinstance(z, int) and z == zs - 1:
                    t[2] = t[2] + SIGMA * z_hi[s, 0, r, :]
                for k, new in enumerate(shrink_p(t)):
                    later.append((p_out, (k, z, r), new))
            if not for_q:
                continue
            hx = [jnp.where(first_lane, part, 0.0) for part in from_x]
            q = [q_out[k, z, r, :] for k in range(6)]
            q[XX] = q[XX] - SIGMA * hx[0]
            q[XY] = q[XY] - half * hx[1]
            q[XZ] = q[XZ] - half * hx[2]
            if b == 0:
                hy = [jnp.where(first_row, y_lo[s, 1 + k, pl.ds(z, 1), :], 0.0) for k in range(3)]
                q[YY] = q[YY] - SIGMA * hy[1]
                q[XY] = q[XY] - half * hy[0]
                q[YZ] = q[YZ] - half * hy[2]
            if isinstance(z, int) and z == 0:
                hz = [z_lo[s, 1 + k, r, :] for k in range(3)]
                q[ZZ] = q[ZZ] - SIGMA * hz[2]
                q[XZ] = q[XZ] - half * hz[0]
                q[YZ] = q[YZ] - half * hz[1]
            for k, new in enumerate(shrink_q(q)):
                later.append((q_out, (k, z, r), new))
        flush(later)

    def spread(row):
        return jnp.broadcast_to(row, (8, xs))

    def column(row, lane_of_first):
        mine = lane == lane_of_first + 2 * blocks * sub
        return jnp.sum(jnp.where(mine, spread(row), 0.0), axis=1, keepdims=True)

    where = ((0, half_lanes), (1, 0), (1, half_lanes))

    def halo_x(s):
        own = [face[4], face[5]]
        up_yc = jnp.where(jnp.logical_and(last_row, last_block), factor(above[1]), 1.0)
        lo_yc = jnp.where(jnp.logical_and(first_row, first_block), factor(below[1]), 1.0)
        up_zc = jnp.where(last_z, factor(above[2]), 1.0)
        lo_zc = jnp.where(first_z, factor(below[2]), 1.0)
        got0, got1 = x_lo[s, 0], x_lo[s, 1]
        u = got0
        v = [turn_lanes(got0, half_lanes), got1, turn_lanes(got1, half_lanes)]
        moved = turn_rows(u, -1)
        edge_y = turn_lanes(spread(d_a[s, 0, pl.ds(0, 1), :]), 2 * (blocks - 1))
        ahead_y = jnp.where(last_row, jnp.where(last_block, edge_y, turn_lanes(moved, -2)), moved)
        ahead_z = jnp.where(
            last_z, turn_lanes(d_c[s, 0], half_lanes - 2 * blocks), turn_lanes(u, -2 * blocks)
        )
        slopes = (turn_lanes(own[0], -1) - u, ahead_y - up_yc * u, ahead_z - up_zc * u)
        p = shrink_p([xp[k] + SIGMA * (slopes[k] - v[k]) for k in range(3)])
        p = [keep(below[0], part) for part in p]

        got0, got1 = x_hi[s, 0], x_hi[s, 1]
        v = [turn_lanes(got0, half_lanes), got1, turn_lanes(got1, half_lanes)]
        mine = [turn_lanes(own[0], half_lanes + 1), turn_lanes(own[1], 1), turn_lanes(own[1], half_lanes + 1)]
        dx, dy, dz = [], [], []
        for k, (h, base) in enumerate(where):
            dx.append(v[k] - mine[k])
            moved = turn_rows(v[k], 1)
            edge_y = turn_lanes(spread(d_b[s, h, pl.ds(7, 1), :]), -base - 2 * (blocks - 1))
            behind_y = jnp.where(first_row, jnp.where(first_block, edge_y, turn_lanes(moved, 2)), moved)
            dy.append(lo_yc * v[k] - behind_y)
            edge_z = turn_lanes(d_d[s, h], -base - 2 * blocks * (zs - 1))
            dz.append(lo_zc * v[k] - jnp.where(first_z, edge_z, turn_lanes(v[k], 2 * blocks)))
        q = shrink_q(grow_q([xq[k] for k in range(6)], dx, dy, dz))
        q = [keep(above[0], part) for part in q]
        for k in range(3):
            xp[k] = p[k]
        for k in range(6):
            xq[k] = q[k]
        cp[0] = jnp.where(odd, turn_lanes(q[XX], half_lanes - 2), turn_lanes(p[0], half_lanes))
        cp[1] = turn_lanes(q[XY], half_lanes - 2)
        cp[2] = turn_lanes(q[XZ], half_lanes - 2)

    def halo_y(s):
        up_zr = jnp.where(last_row, factor(above[2]), 1.0)
        lo_zr = jnp.where(first_row, factor(below[2]), 1.0)
        u = y_lo[s, 0]
        slopes = (
            jnp.where(last_lane, column(d_b[s, 0, pl.ds(7, 1), :], 2 * blocks - 1), turn_lanes(u, -1)) - up_x * u,
            face[0] - u,
            jnp.where(last_row, d_e[s, 0, pl.ds(0, 1), :], turn_rows(u, -1)) - up_zr * u,
        )
        p = shrink_p([yp[k] + SIGMA * (slopes[k] - y_lo[s, 1 + k]) for k in range(3)])
        v = [y_hi[s, 1 + k] for k in range(3)]
        dx = [
            lo_x * v[k] - jnp.where(first_lane, column(d_a[s, h, pl.ds(0, 1), :], base), turn_lanes(v[k], 1))
            for k, (h, base) in enumerate(where)
        ]
        dy = [v[k] - face[7 + k] for k in range(3)]
        dz = [
            lo_zr * v[k] - jnp.where(first_row, d_g[s, 1 + k, pl.ds(zs - 1, 1), :], turn_rows(v[k], 1))
            for k in range(3)
        ]
        q = shrink_q(grow_q([yq[k] for k in range(6)], dx, dy, dz))
        for k in range(3):
            yp[k] = keep(below[1], p[k])
        for k in range(6):
            yq[k] = keep(above[1], q[k])

    def halo_z_first():
        later = []
        for b in range(blocks):
            r = rows(b)
            t = [zp[k, r, :] for k in range(3)]
            edge_x = turn_lanes(d_d[0, 0], xs - 2 - 2 * (blocks * (zs - 1) + b))
            t[0] = t[0] + SIGMA * jnp.where(last_lane, edge_x, 0.0)
            if b == blocks - 1:
                t[1] = t[1] + SIGMA * jnp.where(last_row, d_g[0, 0, pl.ds(zs - 1, 1), :], 0.0)
            t[2] = t[2] + SIGMA * bar[0, 0, r, :]
            for k, new in enumerate(shrink_p(t)):
                later.append((zp, (k, r), keep(below[2], new)))

            hx = [
                jnp.where(first_lane, turn_lanes(d_c[0, h], -base - 2 * b), 0.0) for h, base in where
            ]
            hz = [bar[1 + k, zs - 1, r, :] for k in range(3)]
            q = [zq[k, r, :] for k in range(6)]
            q[XX] = q[XX] - SIGMA * hx[0]
            q[ZZ] = q[ZZ] - SIGMA * hz[2]
            q[XY] = q[XY] - half * hx[1]
            q[XZ] = q[XZ] - half * (hx[2] + hz[0])
            q[YZ] = q[YZ] - half * hz[1]
            if b == 0:
                hy = [jnp.where(first_row, d_e[0, 1 + k, pl.ds(0, 1), :], 0.0) for k in range(3)]
                q[YY] = q[YY] - SIGMA * hy[1]
                q[XY] = q[XY] - half * hy[0]
                q[YZ] = q[YZ] - half * hy[2]
            for k, new in enumerate(shrink_q(q)):
                later.append((zq, (k, r), keep(above[2], new)))
        flush(later)

    def halo_z(s):
        later = []
        for b in range(blocks):
            r = rows(b)
            u = z_lo[s, 0, r, :]
            edge_x = turn_lanes(d_d[s, 0], xs - 2 - 2 * (blocks * (zs - 1) + b))
            if b < blocks - 1:
                ahead_y = z_lo[s, 0, rows(b, 1), :]
            else:
                ahead_y = jnp.where(last_row, d_g[s, 0, pl.ds(zs - 1, 1), :], turn_rows(u, -1))
            slopes = (
                jnp.where(last_lane, edge_x, turn_lanes(u, -1)) - up_x * u,
                ahead_y - up_y(b, u),
                bar[0, 0, r, :] - u,
            )
            p = shrink_p([zp[k, r, :] + SIGMA * (slopes[k] - z_lo[s, 1 + k, r, :]) for k in range(3)])
            for k in range(3):
                later.append((zp, (k, r), keep(below[2], p[k])))

            v = [z_hi[s, 1 + k, r, :] for k in range(3)]
            dx, dy, dz = [], [], []
            for k, (h, base) in enumerate(where):
                edge_x = turn_lanes(d_c[s, h], -base - 2 * b)
                dx.append(lo_x * v[k] - jnp.where(first_lane, edge_x, turn_lanes(v[k], 1)))
                if b > 0:
                    behind_y = z_hi[s, 1 + k, rows(b, -1), :]
                else:
                    behind_y = jnp.where(first_row, d_e[s, 1 + k, pl.ds(0, 1), :], turn_rows(v[k], 1))
                dy.append(lo_y(b, v[k]) - behind_y)
                dz.append(v[k] - bar[1 + k, zs - 1, r, :])
            q = shrink_q(grow_q([zq[k, r, :] for k in range(6)], dx, dy, dz))
            for k in range(6):
                later.append((zq, (k, r), keep(above[2], q[k])))
        flush(later)

    def primal(z, packed, last):
        later = []
        z_up, z_lo_ = up_z(z), lo_z(z)
        at_start = isinstance(z, int) and z == 0
        at_end = isinstance(z, int) and z == zs - 1
        for b in range(blocks):
            r = rows(b)
            by = half_lanes - 2 * (z * blocks + b)
            from_x = [turn_lanes(cp[k], by) for k in range(3)]
            p = [p_out[k, z, r, :] for k in range(3)]
            before_x = jnp.where(first_lane, from_x[0], pltpu.roll(p[0], 1, 1))
            if b > 0:
                before_y = p_out[1, z, rows(b, -1), :]
            else:
                before_y = jnp.where(first_row, yp[1, pl.ds(z, 1), :], pltpu.roll(p[1], 1, 0))
            before_z = zp[2, r, :] if at_start else p_out[2, z - 1, r, :]
            div = (up_x * p[0] - before_x) + (up_y(b, p[1]) - before_y) + (z_up * p[2] - before_z)
            old = u_out[z, r, :]
            new = (old + TAU * div) * gain[z, r, :] + offset[z, r, :]
            later.append((u_out, (z, r), new))
            ahead = [2.0 * new - old]
            q = [q_out[k, z, r, :] for k in range(6)]
            for k, (ax, ay, az) in enumerate(PARTS):
                after_x = jnp.where(last_lane, from_x[k], pltpu.roll(q[ax], xs - 1, 1))
                if b < blocks - 1:
                    after_y = q_out[ay, z, rows(b, 1), :]
                else:
                    after_y = jnp.where(last_row, yq[ay, pl.ds(z, 1), :], pltpu.roll(q[ay], 7, 0))
                after_z = zq[az, r, :] if at_end else q_out[az, z + 1, r, :]
                div2 = (
                    (after_x - lo_x * q[ax]) + (after_y - lo_y(b, q[ay])) + (after_z - z_lo_ * q[az])
                )
                old = v_out[k, z, r, :]
                new = old + TAU * (p[k] + div2)
                later.append((v_out, (k, z, r), new))
                ahead.append(2.0 * new - old)
            if not last:
                for k in range(4):
                    later.append((bar, (k, z, r), ahead[k]))
                    if b == 0:
                        later.append((face, (k, pl.ds(z, 1)), ahead[k][0:1, :]))
                    if b == blocks - 1:
                        later.append((face, (6 + k, pl.ds(z, 1)), ahead[k][7:8, :]))
                pack_bar(packed, ahead, z, b)
        flush(later)

    def pack_dual(packed, z):
        for b in range(blocks):
            for k in range(6):
                value = q_out[k, z, rows(b), :]
                if k < 3:
                    value = jnp.where(last_lane, p_out[k, z, rows(b), :], value)
                packed[k] = pack(packed[k], value, 0, z * blocks + b)

    def prepare(z, carry):
        weight = TAU * gain[z]
        inverse = 1.0 / (1.0 + weight)
        gain[z] = inverse
        offset[z] = weight * offset[z] * inverse
        return carry

    ends, middle = (0, zs - 1), range(1, zs - 1)
    with jax.named_scope("load_uv"):
        for load in loads[:2]:
            load.wait()
    with jax.named_scope("barrier"):
        pl.semaphore_wait(barrier, peers)
    with jax.named_scope("send_z0"):
        start(exchanges[0][:2])
        start(duals[2:4])
    with jax.named_scope("load_face"):
        for load in loads[2:6]:
            load.wait()
        start(exchanges[0][4:6])
    with jax.named_scope("pack_uv"):
        packed = [empty, empty]
        for z in range(zs):
            for b in range(blocks):
                pack_bar(packed, [bar[k, z, rows(b), :] for k in range(4)], z, b)
        face[4] = packed[0]
        face[5] = packed[1]
        start(exchanges[0][6:])
        start(exchanges[0][2:4])
    with jax.named_scope("load_pq"):
        for load in loads[6:8]:
            load.wait()
    with jax.named_scope("pack_pq"):
        packed = [empty] * 6
        for z in ends:
            pack_dual(packed, z)
        for z in ends:
            dual_inside(z, None)
        start(duals[:2])
    with jax.named_scope("pack_pq_rest"):
        for z in middle:
            pack_dual(packed, z)
        for k in range(6):
            xs_own[k] = packed[k]
        start(duals[4:])
    with jax.named_scope("inside0"):
        each(1, zs - 1, dual_inside, ())
    with jax.named_scope("prepare"):
        for load in loads[8:]:
            load.wait()
        lax.fori_loop(0, zs, prepare, 0)

    for s in range(ITERS):
        last = s == ITERS - 1
        moves = exchanges[s]
        if s > 0:
            with jax.named_scope(f"inside{s}"):
                each(0, zs, dual_inside, ())
        with jax.named_scope(f"wait_xy{s}"):
            got(moves[2:6])
            line_up(s)
        with jax.named_scope(f"dual_mid{s}"):
            dual(0, s, for_q=False)
            for z in middle:
                dual(z, s)
            dual(zs - 1, s, for_p=False)
        with jax.named_scope(f"wait_diag{s}"):
            got(moves[6:])
        if s == 0:
            with jax.named_scope(f"wait_pq{s}"):
                got(duals[2:])
        with jax.named_scope(f"halo_xy{s}"):
            halo_x(s)
            halo_y(s)
        with jax.named_scope(f"wait_sent{s}"):
            sent(moves[2:])
        with jax.named_scope(f"primal_mid{s}"):
            packed = [empty, empty]
            for z in middle:
                primal(z, packed, last)
        with jax.named_scope(f"wait_z{s}"):
            got(moves[:2])
            sent(moves[:2])
        if s == 0:
            with jax.named_scope(f"wait_zpq{s}"):
                got(duals[:2])
                sent(duals)
        with jax.named_scope(f"ends{s}"):
            if s == 0:
                halo_z_first()
            else:
                halo_z(s)
            dual(0, s, for_p=False)
            dual(zs - 1, s, for_q=False)
            for z in ends:
                primal(z, packed, last)
        if not last:
            with jax.named_scope(f"send{s}"):
                face[4] = packed[0]
                face[5] = packed[1]
                start(exchanges[s + 1][6:])
                start(exchanges[s + 1][2:6])
                start(exchanges[s + 1][:2])


def copy_out(u_in, v_in, p_in, q_in, u_out, v_out, p_out, q_out, sems):
    pairs = ((q_in, q_out), (p_in, p_out), (v_in, v_out), (u_in, u_out))
    copies = [pltpu.make_async_copy(a, b, sems.at[i]) for i, (a, b) in enumerate(pairs)]
    for copy in copies:
        copy.start()
    for copy in copies:
        copy.wait()


def per_device(noisy_image, fidelity, primal_u, primal_v, dual_p, dual_q):
    zs, ys, xs = primal_u.shape
    blocks = ys // 8
    assert zs == 8 and ys % 8 == 0 and blocks & (blocks - 1) == 0 and 4 * zs * blocks == xs == 128
    f32 = jnp.float32

    def vmem(*shape):
        return pltpu.VMEM(shape, f32)

    results = pl.pallas_call(
        kernel,
        out_shape=tuple(pltpu.VMEM(a.shape, f32) for a in (primal_u, primal_v, dual_p, dual_q)),
        in_specs=[pl.BlockSpec(memory_space=pl.ANY)] * 6,
        out_specs=tuple([pl.BlockSpec(memory_space=pltpu.VMEM)] * 4),
        scratch_shapes=[
            vmem(4, zs, ys, xs),
            vmem(zs, ys, xs),
            vmem(zs, ys, xs),
            vmem(10, 8, xs),
            vmem(ITERS, 4, ys, xs),
            vmem(ITERS, 4, ys, xs),
            vmem(ITERS, 2, 8, xs),
            vmem(ITERS, 2, 8, xs),
            vmem(ITERS, 4, 8, xs),
            vmem(ITERS, 4, 8, xs),
            vmem(ITERS, 2, 8, xs),
            vmem(ITERS, 2, 8, xs),
            vmem(ITERS, 2, 8, xs),
            vmem(ITERS, 2, 8, xs),
            vmem(ITERS, 4, 8, xs),
            vmem(ITERS, 4, 8, xs),
            vmem(3, ys, xs),
            vmem(6, ys, xs),
            vmem(3, 8, xs),
            vmem(6, 8, xs),
            vmem(6, 8, xs),
            vmem(6, 8, xs),
            vmem(6, 8, xs),
            vmem(3, 8, xs),
            vmem(3, 8, xs),
            pltpu.SemaphoreType.DMA((12,)),
            pltpu.SemaphoreType.DMA((ITERS, 12)),
            pltpu.SemaphoreType.DMA((ITERS, 12)),
            pltpu.SemaphoreType.DMA((6,)),
            pltpu.SemaphoreType.DMA((6,)),
        ],
        compiler_params=pltpu.CompilerParams(collective_id=0, has_side_effects=True),
        name="tgv",
    )(noisy_image, fidelity, primal_u, primal_v, dual_p, dual_q)
    return pl.pallas_call(
        copy_out,
        out_shape=tuple(jax.ShapeDtypeStruct(a.shape, f32) for a in results),
        in_specs=[pl.BlockSpec(memory_space=pltpu.VMEM)] * 4,
        out_specs=tuple([pl.BlockSpec(memory_space=pl.ANY)] * 4),
        scratch_shapes=[pltpu.SemaphoreType.DMA((4,))],
        name="out",
    )(*[pltpu.with_memory_space_constraint(r, pltpu.VMEM) for r in results])


def solution(mesh):
    scalar, stack = P("gz", "gy", "gx"), P(None, "gz", "gy", "gx")
    return jax.shard_map(
        per_device,
        mesh=mesh,
        in_specs=(scalar, scalar, scalar, stack, stack, stack),
        out_specs=(scalar, stack, stack, stack),
        check_vma=False,
    )
```

```python
import jax
import jax.numpy as jnp
from jax import lax
from jax.experimental import pallas as pl
from jax.experimental.pallas import tpu as pltpu
from jax.sharding import PartitionSpec as P

ITERS = 3
AXES = ("gx", "gy", "gz")
ALPHA1, ALPHA0, SIGMA, TAU = 0.5, 1.0, 0.2, 0.2
XX, YY, ZZ, XY, XZ, YZ = range(6)
PARTS = ((XX, XY, XZ), (XY, YY, YZ), (XZ, YZ, ZZ))
MESH = pl.DeviceIdType.MESH
Z_UP, Z_DOWN, X_UP, X_DOWN, Y_UP, Y_DOWN, XY_A, XY_B, XZ_A, XZ_B, YZ_A, YZ_B = range(12)
WAYS = (
    (0, 0, 1), (0, 0, -1), (1, 0, 0), (-1, 0, 0), (0, 1, 0), (0, -1, 0),
    (1, -1, 0), (-1, 1, 0), (1, 0, -1), (-1, 0, 1), (0, 1, -1), (0, -1, 1),
)


def kernel(
    noisy_in, fid_in, u_in, v_in, p_in, q_in,
    u_out, v_out, p_out, q_out,
    bar, gain, offset, face,
    z_lo, z_hi, x_lo, x_hi, y_lo, y_hi, d_a, d_b, d_c, d_d, d_e, d_g,
    zp, zq, yp, yq, xs_own, xp, xq, cv, cp, xe, part_p, part_q,
    load_sem, send_sem, recv_sem, first_send, first_recv,
):
    zs, ys, xs = u_in.shape
    blocks = ys // 8
    pairs = zs * blocks
    half_lanes = 2 * pairs
    place = [lax.axis_index(a) for a in AXES]
    count = [lax.axis_size(a) for a in AXES]
    below = [place[i] > 0 for i in range(3)]
    above = [place[i] < count[i] - 1 for i in range(3)]

    def exists(way):
        there = None
        for i, by in enumerate(way):
            if by:
                one = above[i] if by > 0 else below[i]
                there = one if there is None else jnp.logical_and(there, one)
        return there

    def target(way):
        return {AXES[i]: place[i] + by for i, by in enumerate(way) if by}

    goes = [exists(way) for way in WAYS]
    comes = [exists(tuple(-by for by in way)) for way in WAYS]
    peers = sum(there.astype(jnp.int32) for there in goes)

    u_face, xf, top_face = pl.ds(0, 4), pl.ds(4, 2), pl.ds(6, 4)
    loads = [
        pltpu.make_async_copy(u_in, bar.at[0], load_sem.at[0]),
        pltpu.make_async_copy(v_in, bar.at[pl.ds(1, 3)], load_sem.at[1]),
        pltpu.make_async_copy(u_in.at[:, 0], face.at[0], load_sem.at[2]),
        pltpu.make_async_copy(v_in.at[:, :, 0], face.at[pl.ds(1, 3)], load_sem.at[3]),
        pltpu.make_async_copy(u_in.at[:, ys - 1], face.at[6], load_sem.at[4]),
        pltpu.make_async_copy(v_in.at[:, :, ys - 1], face.at[pl.ds(7, 3)], load_sem.at[5]),
        pltpu.make_async_copy(p_in, p_out, load_sem.at[6]),
        pltpu.make_async_copy(q_in, q_out, load_sem.at[7]),
        pltpu.make_async_copy(noisy_in, offset, load_sem.at[8]),
        pltpu.make_async_copy(fid_in, gain, load_sem.at[9]),
        pltpu.make_async_copy(u_in, u_out, load_sem.at[10]),
        pltpu.make_async_copy(v_in, v_out, load_sem.at[11]),
    ]
    for load in loads[:8]:
        load.start()
    barrier = pltpu.get_barrier_semaphore()
    for way, there in zip(WAYS, goes):
        @pl.when(there)
        def _():
            pl.semaphore_signal(barrier, inc=1, device_id=target(way), device_id_type=MESH)
    for load in loads[8:]:
        load.start()

    def clear(there, *refs):
        @pl.when(jnp.logical_not(there))
        def _():
            for ref in refs:
                ref[...] = jnp.zeros(ref.shape, jnp.float32)

    clear(below[0], x_lo, xp)
    clear(above[0], x_hi, xq)
    clear(below[1], y_lo, yp)
    clear(above[1], y_hi, yq)
    clear(below[2], z_lo, zp)
    clear(above[2], z_hi, zq)
    for way, ref in zip(WAYS[6:], (d_a, d_b, d_c, d_d, d_e, d_g)):
        clear(exists(tuple(-by for by in way)), ref)

    lane = lax.broadcasted_iota(jnp.int32, (8, xs), 1)
    sub = lax.broadcasted_iota(jnp.int32, (8, xs), 0)
    pair = lane >> 1
    odd = (lane & 1) == 1
    first_lane, last_lane = lane == 0, lane == xs - 1
    first_row, last_row = sub == 0, sub == 7
    p_pair, q_pair = (lane - half_lanes) >> 1, (lane + 1 - half_lanes) >> 1

    def factor(flag):
        return jnp.where(flag, jnp.float32(1), jnp.float32(0))

    up_x = jnp.where(last_lane, factor(above[0]), 1.0)
    lo_x = jnp.where(first_lane, factor(below[0]), 1.0)
    up_y_last = jnp.where(last_row, factor(above[1]), 1.0)
    lo_y_first = jnp.where(first_row, factor(below[1]), 1.0)

    def rows(b, by=0):
        return pl.ds(8 * b + by, 8)

    def turn_lanes(value, by):
        return value if isinstance(by, int) and by % xs == 0 else pltpu.roll(value, by % xs if isinstance(by, int) else by, 1)

    def turn_rows(value, by):
        return pltpu.roll(value, by % 8, 0)

    def flush(later):
        for ref, at, value in later:
            ref[at + (slice(None),)] = value
        later.clear()

    def up_z(z):
        return factor(jnp.logical_or(z < zs - 1, above[2]))

    def lo_z(z):
        return factor(jnp.logical_or(z > 0, below[2]))

    def up_y(b, value):
        return up_y_last * value if b == blocks - 1 else value

    def lo_y(b, value):
        return lo_y_first * value if b == 0 else value

    def next_x(value):
        return jnp.where(last_lane, 0.0, pltpu.roll(value, xs - 1, 1))

    def prev_x(value):
        return jnp.where(first_lane, 0.0, pltpu.roll(value, 1, 1))

    def next_y(ref, k, z, b, value):
        if b < blocks - 1:
            return ref[k, z, rows(b, 1), :]
        return jnp.where(last_row, 0.0, pltpu.roll(value, 7, 0))

    def prev_y(ref, k, z, b, value):
        if b > 0:
            return ref[k, z, rows(b, -1), :]
        return jnp.where(first_row, 0.0, pltpu.roll(value, 1, 0))

    def next_z(ref, k, z, b):
        if isinstance(z, int):
            return ref[k, z + 1, rows(b), :] if z < zs - 1 else jnp.zeros((8, xs), jnp.float32)
        return factor(z < zs - 1) * ref[k, jnp.minimum(z + 1, zs - 1), rows(b), :]

    def prev_z(ref, k, z, b):
        if isinstance(z, int):
            return ref[k, z - 1, rows(b), :] if z > 0 else jnp.zeros((8, xs), jnp.float32)
        return factor(z > 0) * ref[k, jnp.maximum(z - 1, 0), rows(b), :]

    def shrink_p(t):
        size = t[0] * t[0] + t[1] * t[1] + t[2] * t[2]
        scale = jnp.minimum(1.0, ALPHA1 * lax.rsqrt(size))
        return [scale * part for part in t]

    def shrink_q(s):
        size = (s[XX] * s[XX] + s[YY] * s[YY] + s[ZZ] * s[ZZ]) + 2.0 * (
            s[XY] * s[XY] + s[XZ] * s[XZ] + s[YZ] * s[YZ]
        )
        scale = jnp.minimum(1.0, ALPHA0 * lax.rsqrt(size))
        return [scale * part for part in s]

    half = 0.5 * SIGMA

    def grow_q(q, dx, dy, dz):
        return [
            q[XX] + SIGMA * dx[0], q[YY] + SIGMA * dy[1], q[ZZ] + SIGMA * dz[2],
            q[XY] + half * (dy[0] + dx[1]), q[XZ] + half * (dz[0] + dx[2]),
            q[YZ] + half * (dz[1] + dy[2]),
        ]

    def keep(flag, value):
        return jnp.where(flag, value, 0.0)

    def pack(packed, value, base, j):
        return jnp.where(pair == base + j, pltpu.roll(value, 2 * (base + j) + 1, 1), packed)

    def pack_bar(packed, values, z, b):
        j = z * blocks + b
        packed[0] = pack(packed[0], values[0], 0, j)
        packed[0] = pack(packed[0], values[1], pairs, j)
        packed[1] = pack(packed[1], values[2], 0, j)
        packed[1] = pack(packed[1], values[3], pairs, j)

    def message(src, dst, way, send, recv):
        return pltpu.make_async_remote_copy(
            src_ref=src, dst_ref=dst, send_sem=send, recv_sem=recv,
            device_id=target(WAYS[way]), device_id_type=MESH,
        )

    exchanges = []
    for s in range(ITERS):
        z_up_part = pl.ds(1, 3) if s == 0 else pl.ds(0, 4)
        z_down_part = pl.ds(0, 1) if s == 0 else pl.ds(0, 4)
        ends = (
            (bar.at[z_up_part, zs - 1], z_lo.at[s, z_up_part]),
            (bar.at[z_down_part, 0], z_hi.at[s, z_down_part]),
            (face.at[xf], x_lo.at[s]),
            (face.at[xf], x_hi.at[s]),
            (face.at[top_face], y_lo.at[s]),
            (face.at[u_face], y_hi.at[s]),
            (face.at[xf, pl.ds(0, 1)], d_a.at[s, :, pl.ds(0, 1)]),
            (face.at[xf, pl.ds(7, 1)], d_b.at[s, :, pl.ds(7, 1)]),
            (xe, d_c.at[s]),
            (xe, d_d.at[s]),
            (face.at[top_face, pl.ds(0, 1)], d_e.at[s, :, pl.ds(0, 1)]),
            (face.at[u_face, pl.ds(zs - 1, 1)], d_g.at[s, :, pl.ds(zs - 1, 1)]),
        )
        exchanges.append([
            (message(src, dst, k, send_sem.at[s, k], recv_sem.at[s, k]), goes[k], comes[k])
            for k, (src, dst) in enumerate(ends)
        ])
    duals = [
        (message(src, dst, way, first_send.at[k], first_recv.at[k]), goes[way], comes[way])
        for k, (src, dst, way) in enumerate((
            (p_out.at[:, zs - 1], zp, Z_UP),
            (q_out.at[:, 0], zq, Z_DOWN),
            (p_in.at[:, :, ys - 1], yp, Y_UP),
            (q_in.at[:, :, 0], yq, Y_DOWN),
            (xs_own, xp, X_UP),
            (xs_own, xq, X_DOWN),
        ))
    ]

    def start(moves):
        for copy, there, _ in moves:
            @pl.when(there)
            def _():
                copy.start()

    def sent(moves):
        for copy, there, _ in moves:
            @pl.when(there)
            def _():
                copy.wait_send()

    def got(moves):
        for copy, _, there in moves:
            @pl.when(there)
            def _():
                copy.wait_recv()

    empty = jnp.zeros((8, xs), jnp.float32)

    def each(low, high, body, carry):
        def turn(j, carry):
            one = list(carry)
            body(low + 2 * j, one)
            body(low + 2 * j + 1, one)
            return tuple(one)

        return lax.fori_loop(0, (high - low) // 2, turn, tuple(carry))

    def dual_inside(z, _):
        later = []
        z_up, z_lo_ = up_z(z), lo_z(z)
        for b in range(blocks):
            r = rows(b)
            u = bar[0, z, r, :]
            v = [bar[1 + k, z, r, :] for k in range(3)]
            slopes = (
                next_x(u) - up_x * u,
                next_y(bar, 0, z, b, u) - up_y(b, u),
                next_z(bar, 0, z, b) - z_up * u,
            )
            for k in range(3):
                later.append((p_out, (k, z, r), p_out[k, z, r, :] + SIGMA * (slopes[k] - v[k])))
            dx = [lo_x * v[k] - prev_x(v[k]) for k in range(3)]
            dy = [lo_y(b, v[k]) - prev_y(bar, 1 + k, z, b, v[k]) for k in range(3)]
            dz = [z_lo_ * v[k] - prev_z(bar, 1 + k, z, b) for k in range(3)]
            for k, new in enumerate(grow_q([q_out[k, z, r, :] for k in range(6)], dx, dy, dz)):
                later.append((q_out, (k, z, r), new))
        flush(later)

    def line_up(s):
        cv[0] = jnp.where(odd, turn_lanes(x_hi[s, 0], half_lanes - 2), x_lo[s, 0])
        cv[1] = turn_lanes(x_lo[s, 1], half_lanes)
        cv[2] = x_lo[s, 1]

    def less_q(q, x=None, y=None, z=None):
        q = list(q)
        if x is not None:
            q[XX] = q[XX] - SIGMA * x[0]
            q[XY] = q[XY] - half * x[1]
            q[XZ] = q[XZ] - half * x[2]
        if y is not None:
            q[YY] = q[YY] - SIGMA * y[1]
            q[XY] = q[XY] - half * y[0]
            q[YZ] = q[YZ] - half * y[2]
        if z is not None:
            q[ZZ] = q[ZZ] - SIGMA * z[2]
            q[XZ] = q[XZ] - half * z[0]
            q[YZ] = q[YZ] - half * z[1]
        return q

    def dual(z, s):
        later = []
        for b in range(blocks):
            r = rows(b)
            by = half_lanes - 2 * (z * blocks + b)
            from_x = [turn_lanes(cv[k], by) for k in range(3)]
            t = [p_out[k, z, r, :] for k in range(3)]
            t[0] = t[0] + SIGMA * jnp.where(last_lane, from_x[0], 0.0)
            if b == blocks - 1:
                t[1] = t[1] + SIGMA * jnp.where(last_row, y_hi[s, 0, pl.ds(z, 1), :], 0.0)
            for k in range(3):
                if z == zs - 1:
                    later.append((part_p, (k, r), t[k]))
            if z < zs - 1:
                for k, new in enumerate(shrink_p(t)):
                    later.append((p_out, (k, z, r), new))
            hx = [jnp.where(first_lane, part, 0.0) for part in from_x]
            hy = None
            if b == 0:
                hy = [jnp.where(first_row, y_lo[s, 1 + k, pl.ds(z, 1), :], 0.0) for k in range(3)]
            q = less_q([q_out[k, z, r, :] for k in range(6)], hx, hy)
            if z > 0:
                q = shrink_q(q)
            for k in range(6):
                later.append((part_q, (k, r), q[k]) if z == 0 else (q_out, (k, z, r), q[k]))
        flush(later)

    def dual_ends(s):
        later = []
        for b in range(blocks):
            r = rows(b)
            t = [part_p[k, r, :] for k in range(3)]
            t[2] = t[2] + SIGMA * z_hi[s, 0, r, :]
            for k, new in enumerate(shrink_p(t)):
                later.append((p_out, (k, zs - 1, r), new))
            q = less_q([part_q[k, r, :] for k in range(6)], z=[z_lo[s, 1 + k, r, :] for k in range(3)])
            for k, new in enumerate(shrink_q(q)):
                later.append((q_out, (k, 0, r), new))
        flush(later)

    def spread(row):
        return jnp.broadcast_to(row, (8, xs))

    def column(row, lane_of_first):
        mine = lane == lane_of_first + 2 * blocks * sub
        return jnp.sum(jnp.where(mine, spread(row), 0.0), axis=1, keepdims=True)

    where = ((0, half_lanes), (1, 0), (1, half_lanes))

    def halo_x_inside(s):
        far = pairs - blocks
        up_yc = jnp.where(jnp.logical_and(last_row, (p_pair & (blocks - 1)) == blocks - 1), factor(above[1]), 1.0)
        lo_yc = jnp.where(jnp.logical_and(first_row, (q_pair & (blocks - 1)) == 0), factor(below[1]), 1.0)
        up_zc = jnp.where(p_pair >= far, factor(above[2]), 1.0)
        lo_zc = jnp.where(q_pair < blocks, factor(below[2]), 1.0)
        u = turn_lanes(x_lo[s, 0], half_lanes)
        v = [x_lo[s, 0], turn_lanes(x_lo[s, 1], half_lanes), x_lo[s, 1]]
        own = turn_lanes(face[4], half_lanes - 1)
        moved = turn_rows(u, -1)
        turned = jnp.where((p_pair & (blocks - 1)) == blocks - 1, 0.0, turn_lanes(moved, -2))
        ahead_y = jnp.where(last_row, turned, moved)
        ahead_z = jnp.where(p_pair >= far, 0.0, turn_lanes(u, -2 * blocks))
        slopes = (own - u, ahead_y - up_yc * u, ahead_z - up_zc * u)
        for k in range(3):
            xp[k] = xp[k] + SIGMA * (slopes[k] - v[k])

        v = [turn_lanes(x_hi[s, 0], -2), turn_lanes(x_hi[s, 1], half_lanes - 2), turn_lanes(x_hi[s, 1], -2)]
        mine = [turn_lanes(face[4], -1), turn_lanes(face[5], half_lanes - 1), turn_lanes(face[5], -1)]
        dx, dy, dz = [], [], []
        for k in range(3):
            dx.append(v[k] - mine[k])
            moved = turn_rows(v[k], 1)
            turned = jnp.where((q_pair & (blocks - 1)) == 0, 0.0, turn_lanes(moved, 2))
            dy.append(lo_yc * v[k] - jnp.where(first_row, turned, moved))
            dz.append(lo_zc * v[k] - jnp.where(q_pair < blocks, 0.0, turn_lanes(v[k], 2 * blocks)))
        q = [turn_lanes(xq[k], -2) if s == 0 else xq[k] for k in range(6)]
        for k, new in enumerate(grow_q(q, dx, dy, dz)):
            xq[k] = new

    def halo_x(s):
        far = pairs - blocks
        t = [xp[k] for k in range(3)]
        edge = turn_lanes(spread(d_a[s, 0, pl.ds(0, 1), :]), half_lanes + 2 * (blocks - 1))
        here = jnp.logical_and(last_row, (p_pair & (blocks - 1)) == blocks - 1)
        t[1] = t[1] + SIGMA * jnp.where(here, edge, 0.0)
        edge = turn_lanes(d_c[s, 0], half_lanes + 2 * far)
        t[2] = t[2] + SIGMA * jnp.where(p_pair >= far, edge, 0.0)
        p = [keep(below[0], part) for part in shrink_p(t)]
        here = jnp.logical_and(first_row, (q_pair & (blocks - 1)) == 0)
        edge_y, edge_z = [], []
        for h, base in where:
            edge = turn_lanes(spread(d_b[s, h, pl.ds(7, 1), :]), half_lanes - 2 * blocks - base)
            edge_y.append(jnp.where(here, edge, 0.0))
            edge = turn_lanes(d_d[s, h], half_lanes - 2 - 2 * far - base)
            edge_z.append(jnp.where(q_pair < blocks, edge, 0.0))
        q = shrink_q(less_q([xq[k] for k in range(6)], y=edge_y, z=edge_z))
        q = [keep(above[0], part) for part in q]
        for k in range(3):
            xp[k] = p[k]
        for k in range(6):
            xq[k] = q[k]
        cp[0] = jnp.where(odd, q[XX], p[0])
        cp[1] = q[XY]
        cp[2] = q[XZ]

    def halo_y_inside(s):
        up_zr = jnp.where(last_row, factor(above[2]), 1.0)
        lo_zr = jnp.where(first_row, factor(below[2]), 1.0)
        u = y_lo[s, 0]
        slopes = (
            next_x(u) - up_x * u,
            face[0] - u,
            jnp.where(last_row, 0.0, turn_rows(u, -1)) - up_zr * u,
        )
        for k in range(3):
            yp[k] = yp[k] + SIGMA * (slopes[k] - y_lo[s, 1 + k])
        v = [y_hi[s, 1 + k] for k in range(3)]
        dx = [lo_x * v[k] - prev_x(v[k]) for k in range(3)]
        dy = [v[k] - face[7 + k] for k in range(3)]
        dz = [lo_zr * v[k] - jnp.where(first_row, 0.0, turn_rows(v[k], 1)) for k in range(3)]
        for k, new in enumerate(grow_q([yq[k] for k in range(6)], dx, dy, dz)):
            yq[k] = new

    def halo_y(s):
        t = [yp[k] for k in range(3)]
        edge = column(d_b[s, 0, pl.ds(7, 1), :], 2 * blocks - 1)
        t[0] = t[0] + SIGMA * jnp.where(last_lane, edge, 0.0)
        t[2] = t[2] + SIGMA * jnp.where(last_row, d_e[s, 0, pl.ds(0, 1), :], 0.0)
        p = shrink_p(t)
        edge_x = [
            jnp.where(first_lane, column(d_a[s, h, pl.ds(0, 1), :], base), 0.0) for h, base in where
        ]
        edge_z = [jnp.where(first_row, d_g[s, 1 + k, pl.ds(zs - 1, 1), :], 0.0) for k in range(3)]
        q = shrink_q(less_q([yq[k] for k in range(6)], x=edge_x, z=edge_z))
        for k in range(3):
            yp[k] = keep(below[1], p[k])
        for k in range(6):
            yq[k] = keep(above[1], q[k])

    def halo_z_first():
        later = []
        for b in range(blocks):
            r = rows(b)
            t = [zp[k, r, :] for k in range(3)]
            edge_x = turn_lanes(d_d[0, 0], xs - 2 - 2 * (blocks * (zs - 1) + b))
            t[0] = t[0] + SIGMA * jnp.where(last_lane, edge_x, 0.0)
            if b == blocks - 1:
                t[1] = t[1] + SIGMA * jnp.where(last_row, d_g[0, 0, pl.ds(zs - 1, 1), :], 0.0)
            t[2] = t[2] + SIGMA * bar[0, 0, r, :]
            for k, new in enumerate(shrink_p(t)):
                later.append((zp, (k, r), keep(below[2], new)))

            hx = [
                jnp.where(first_lane, turn_lanes(d_c[0, h], -base - 2 * b), 0.0) for h, base in where
            ]
            hz = [bar[1 + k, zs - 1, r, :] for k in range(3)]
            hy = None
            if b == 0:
                hy = [jnp.where(first_row, d_e[0, 1 + k, pl.ds(0, 1), :], 0.0) for k in range(3)]
            q = less_q([zq[k, r, :] for k in range(6)], hx, hy, hz)
            for k, new in enumerate(shrink_q(q)):
                later.append((zq, (k, r), keep(above[2], new)))
        flush(later)

    def halo_z(s):
        later = []
        for b in range(blocks):
            r = rows(b)
            u = z_lo[s, 0, r, :]
            edge_x = turn_lanes(d_d[s, 0], xs - 2 - 2 * (blocks * (zs - 1) + b))
            if b < blocks - 1:
                ahead_y = z_lo[s, 0, rows(b, 1), :]
            else:
                ahead_y = jnp.where(last_row, d_g[s, 0, pl.ds(zs - 1, 1), :], turn_rows(u, -1))
            slopes = (
                jnp.where(last_lane, edge_x, turn_lanes(u, -1)) - up_x * u,
                ahead_y - up_y(b, u),
                bar[0, 0, r, :] - u,
            )
            p = shrink_p([zp[k, r, :] + SIGMA * (slopes[k] - z_lo[s, 1 + k, r, :]) for k in range(3)])
            for k in range(3):
                later.append((zp, (k, r), keep(below[2], p[k])))

            v = [z_hi[s, 1 + k, r, :] for k in range(3)]
            dx, dy, dz = [], [], []
            for k, (h, base) in enumerate(where):
                edge_x = turn_lanes(d_c[s, h], -base - 2 * b)
                dx.append(lo_x * v[k] - jnp.where(first_lane, edge_x, turn_lanes(v[k], 1)))
                if b > 0:
                    behind_y = z_hi[s, 1 + k, rows(b, -1), :]
                else:
                    behind_y = jnp.where(first_row, d_e[s, 1 + k, pl.ds(0, 1), :], turn_rows(v[k], 1))
                dy.append(lo_y(b, v[k]) - behind_y)
                dz.append(v[k] - bar[1 + k, zs - 1, r, :])
            q = shrink_q(grow_q([zq[k, r, :] for k in range(6)], dx, dy, dz))
            for k in range(6):
                later.append((zq, (k, r), keep(above[2], q[k])))
        flush(later)

    def pack_plane(packed, z):
        for b in range(blocks):
            pack_bar(packed, [bar[k, z, rows(b), :] for k in range(4)], z, b)

    def primal(z, last):
        later = []
        z_up, z_lo_ = up_z(z), lo_z(z)
        at_start = isinstance(z, int) and z == 0
        at_end = isinstance(z, int) and z == zs - 1
        for b in range(blocks):
            r = rows(b)
            by = half_lanes - 2 * (z * blocks + b)
            from_x = [turn_lanes(cp[k], by) for k in range(3)]
            p = [p_out[k, z, r, :] for k in range(3)]
            before_x = jnp.where(first_lane, from_x[0], pltpu.roll(p[0], 1, 1))
            if b > 0:
                before_y = p_out[1, z, rows(b, -1), :]
            else:
                before_y = jnp.where(first_row, yp[1, pl.ds(z, 1), :], pltpu.roll(p[1], 1, 0))
            before_z = zp[2, r, :] if at_start else p_out[2, z - 1, r, :]
            div = (up_x * p[0] - before_x) + (up_y(b, p[1]) - before_y) + (z_up * p[2] - before_z)
            old = u_out[z, r, :]
            new = (old + TAU * div) * gain[z, r, :] + offset[z, r, :]
            later.append((u_out, (z, r), new))
            ahead = [2.0 * new - old]
            q = [q_out[k, z, r, :] for k in range(6)]
            for k, (ax, ay, az) in enumerate(PARTS):
                after_x = jnp.where(last_lane, from_x[k], pltpu.roll(q[ax], xs - 1, 1))
                if b < blocks - 1:
                    after_y = q_out[ay, z, rows(b, 1), :]
                else:
                    after_y = jnp.where(last_row, yq[ay, pl.ds(z, 1), :], pltpu.roll(q[ay], 7, 0))
                after_z = zq[az, r, :] if at_end else q_out[az, z + 1, r, :]
                div2 = (
                    (after_x - lo_x * q[ax]) + (after_y - lo_y(b, q[ay])) + (after_z - z_lo_ * q[az])
                )
                old = v_out[k, z, r, :]
                new = old + TAU * (p[k] + div2)
                later.append((v_out, (k, z, r), new))
                ahead.append(2.0 * new - old)
            if not last:
                for k in range(4):
                    later.append((bar, (k, z, r), ahead[k]))
                    if b == 0:
                        later.append((face, (k, pl.ds(z, 1)), ahead[k][0:1, :]))
                    if b == blocks - 1:
                        later.append((face, (6 + k, pl.ds(z, 1)), ahead[k][7:8, :]))
        flush(later)

    def pack_dual(packed, z):
        for b in range(blocks):
            for k in range(6):
                value = q_out[k, z, rows(b), :]
                if k < 3:
                    value = jnp.where(last_lane, p_out[k, z, rows(b), :], value)
                packed[k] = pack(packed[k], value, pairs, z * blocks + b)

    def prepare(z, carry):
        weight = TAU * gain[z]
        inverse = 1.0 / (1.0 + weight)
        gain[z] = inverse
        offset[z] = weight * offset[z] * inverse
        return carry

    ends, middle = (0, zs - 1), range(1, zs - 1)
    with jax.named_scope("load_uv"):
        for load in loads[:2]:
            load.wait()
    with jax.named_scope("barrier"):
        pl.semaphore_wait(barrier, peers)
    with jax.named_scope("send_z0"):
        start(exchanges[0][:2])
        start(duals[2:4])
    with jax.named_scope("load_face"):
        for load in loads[2:6]:
            load.wait()
        start(exchanges[0][4:6])
    with jax.named_scope("pack_uv"):
        packed = [empty, empty]
        for z in ends:
            pack_plane(packed, z)
        xe[0] = packed[0]
        xe[1] = packed[1]
        for z in middle:
            pack_plane(packed, z)
        face[4] = packed[0]
        face[5] = packed[1]
        start(exchanges[0][8:])
        start(exchanges[0][6:8])
        start(exchanges[0][2:4])
    with jax.named_scope("load_pq"):
        for load in loads[6:8]:
            load.wait()
    with jax.named_scope("pack_pq"):
        packed = [empty] * 6
        for z in ends:
            pack_dual(packed, z)
        for z in ends:
            dual_inside(z, None)
        start(duals[:2])
    with jax.named_scope("pack_pq_rest"):
        for z in middle:
            pack_dual(packed, z)
        for k in range(6):
            xs_own[k] = packed[k]
        start(duals[4:])
    with jax.named_scope("inside0"):
        each(1, zs - 1, dual_inside, ())
    with jax.named_scope("prepare"):
        for load in loads[8:]:
            load.wait()
        lax.fori_loop(0, zs, prepare, 0)

    for s in range(ITERS):
        last = s == ITERS - 1
        moves = exchanges[s]
        if s > 0:
            with jax.named_scope(f"inside{s}"):
                each(0, zs, dual_inside, ())
        with jax.named_scope(f"wait_xy{s}"):
            got(moves[2:6])
            line_up(s)
        with jax.named_scope(f"dual_mid{s}"):
            for z in range(zs):
                dual(z, s)
            if s > 0:
                halo_x_inside(s)
                halo_y_inside(s)
        if s == 0:
            with jax.named_scope(f"wait_pq{s}"):
                got(duals[2:])
                halo_x_inside(s)
                halo_y_inside(s)
        with jax.named_scope(f"wait_diag{s}"):
            got(moves[6:])
        with jax.named_scope(f"halo_xy{s}"):
            halo_x(s)
            halo_y(s)
        with jax.named_scope(f"wait_z{s}"):
            got(moves[:2])
            sent(moves)
        if s == 0:
            with jax.named_scope(f"wait_zpq{s}"):
                got(duals[:2])
                sent(duals)
        with jax.named_scope(f"ends{s}"):
            if s == 0:
                halo_z_first()
            else:
                halo_z(s)
            dual_ends(s)
            for z in ends:
                primal(z, last)
            if not last:
                packed = [empty, empty]
                for z in ends:
                    pack_plane(packed, z)
                xe[0] = packed[0]
                xe[1] = packed[1]
        if not last:
            with jax.named_scope(f"send_z{s}"):
                start(exchanges[s + 1][8:])
                start(exchanges[s + 1][:2])
        with jax.named_scope(f"primal_mid{s}"):
            for z in middle:
                primal(z, last)
            if not last:
                for z in middle:
                    pack_plane(packed, z)
                face[4] = packed[0]
                face[5] = packed[1]
        if not last:
            with jax.named_scope(f"send{s}"):
                start(exchanges[s + 1][6:8])
                start(exchanges[s + 1][2:6])


def copy_out(u_in, v_in, p_in, q_in, u_out, v_out, p_out, q_out, sems):
    pairs = ((q_in, q_out), (p_in, p_out), (v_in, v_out), (u_in, u_out))
    copies = [pltpu.make_async_copy(a, b, sems.at[i]) for i, (a, b) in enumerate(pairs)]
    for copy in copies:
        copy.start()
    for copy in copies:
        copy.wait()


def per_device(noisy_image, fidelity, primal_u, primal_v, dual_p, dual_q):
    zs, ys, xs = primal_u.shape
    blocks = ys // 8
    assert zs == 8 and ys % 8 == 0 and blocks & (blocks - 1) == 0 and 4 * zs * blocks == xs == 128
    f32 = jnp.float32

    def vmem(*shape):
        return pltpu.VMEM(shape, f32)

    results = pl.pallas_call(
        kernel,
        out_shape=tuple(pltpu.VMEM(a.shape, f32) for a in (primal_u, primal_v, dual_p, dual_q)),
        in_specs=[pl.BlockSpec(memory_space=pl.ANY)] * 6,
        out_specs=tuple([pl.BlockSpec(memory_space=pltpu.VMEM)] * 4),
        scratch_shapes=[
            vmem(4, zs, ys, xs),
            vmem(zs, ys, xs),
            vmem(zs, ys, xs),
            vmem(10, 8, xs),
            vmem(ITERS, 4, ys, xs),
            vmem(ITERS, 4, ys, xs),
            vmem(ITERS, 2, 8, xs),
            vmem(ITERS, 2, 8, xs),
            vmem(ITERS, 4, 8, xs),
            vmem(ITERS, 4, 8, xs),
            vmem(ITERS, 2, 8, xs),
            vmem(ITERS, 2, 8, xs),
            vmem(ITERS, 2, 8, xs),
            vmem(ITERS, 2, 8, xs),
            vmem(ITERS, 4, 8, xs),
            vmem(ITERS, 4, 8, xs),
            vmem(3, ys, xs),
            vmem(6, ys, xs),
            vmem(3, 8, xs),
            vmem(6, 8, xs),
            vmem(6, 8, xs),
            vmem(6, 8, xs),
            vmem(6, 8, xs),
            vmem(3, 8, xs),
            vmem(3, 8, xs),
            vmem(2, 8, xs),
            vmem(3, ys, xs),
            vmem(6, ys, xs),
            pltpu.SemaphoreType.DMA((12,)),
            pltpu.SemaphoreType.DMA((ITERS, 12)),
            pltpu.SemaphoreType.DMA((ITERS, 12)),
            pltpu.SemaphoreType.DMA((6,)),
            pltpu.SemaphoreType.DMA((6,)),
        ],
        compiler_params=pltpu.CompilerParams(collective_id=0, has_side_effects=True),
        name="tgv",
    )(noisy_image, fidelity, primal_u, primal_v, dual_p, dual_q)
    return pl.pallas_call(
        copy_out,
        out_shape=tuple(jax.ShapeDtypeStruct(a.shape, f32) for a in results),
        in_specs=[pl.BlockSpec(memory_space=pltpu.VMEM)] * 4,
        out_specs=tuple([pl.BlockSpec(memory_space=pl.ANY)] * 4),
        scratch_shapes=[pltpu.SemaphoreType.DMA((4,))],
        name="out",
    )(*[pltpu.with_memory_space_constraint(r, pltpu.VMEM) for r in results])


def solution(mesh):
    scalar, stack = P("gz", "gy", "gx"), P(None, "gz", "gy", "gx")
    return jax.shard_map(
        per_device,
        mesh=mesh,
        in_specs=(scalar, scalar, scalar, stack, stack, stack),
        out_specs=(scalar, stack, stack, stack),
        check_vma=False,
    )
```

```python
import jax
import jax.numpy as jnp
from jax import lax
from jax.experimental import pallas as pl
from jax.experimental.pallas import tpu as pltpu
from jax.sharding import PartitionSpec as P

ITERS = 3
AXES = ("gx", "gy", "gz")
ALPHA1, ALPHA0, SIGMA, TAU = 0.5, 1.0, 0.2, 0.2
XX, YY, ZZ, XY, XZ, YZ = range(6)
PARTS = ((XX, XY, XZ), (XY, YY, YZ), (XZ, YZ, ZZ))
Y_PARTS, Z_PARTS = (XY, YY, YZ), (XZ, YZ, ZZ)
MESH = pl.DeviceIdType.MESH
Z_UP, Z_DOWN, X_UP, X_DOWN, Y_UP, Y_DOWN, XY_A, XY_B, XZ_A, XZ_B, YZ_A, YZ_B = range(12)
WAYS = (
    (0, 0, 1), (0, 0, -1), (1, 0, 0), (-1, 0, 0), (0, 1, 0), (0, -1, 0),
    (1, -1, 0), (-1, 1, 0), (1, 0, -1), (-1, 0, 1), (0, 1, -1), (0, -1, 1),
)


def primal_plane(z, below, above, u_ref, v_ref, p_ref, q_ref, gain, offset, halo):
    zs, ys, xs = u_ref.shape
    blocks = ys // 8
    cp, row_p, row_q, plane_p, plane_q = halo
    lane = lax.broadcasted_iota(jnp.int32, (8, xs), 1)
    sub = lax.broadcasted_iota(jnp.int32, (8, xs), 0)
    first_lane, last_lane = lane == 0, lane == xs - 1
    first_row, last_row = sub == 0, sub == 7

    def factor(flag):
        return jnp.where(flag, jnp.float32(1), jnp.float32(0))

    up_x = jnp.where(last_lane, factor(above[0]), 1.0)
    lo_x = jnp.where(first_lane, factor(below[0]), 1.0)
    up_z = factor(above[2]) if z == zs - 1 else 1.0
    lo_z = factor(below[2]) if z == 0 else 1.0
    for b in range(blocks):
        r = pl.ds(8 * b, 8)
        up_y = jnp.where(last_row, factor(above[1]), 1.0) if b == blocks - 1 else 1.0
        lo_y = jnp.where(first_row, factor(below[1]), 1.0) if b == 0 else 1.0
        by = xs // 2 - 2 * (z * blocks + b)
        from_x = [pltpu.roll(cp[k], by, 1) for k in range(3)]
        p = [p_ref[k, z, r, :] for k in range(3)]
        q = [q_ref[k, z, r, :] for k in range(6)]
        before_x = jnp.where(first_lane, from_x[0], pltpu.roll(p[0], 1, 1))
        if b > 0:
            before_y = p_ref[1, z, pl.ds(8 * b - 1, 8), :]
        else:
            before_y = jnp.where(first_row, row_p(z), pltpu.roll(p[1], 1, 0))
        before_z = plane_p(r) if z == 0 else p_ref[2, z - 1, r, :]
        div = (up_x * p[0] - before_x) + (up_y * p[1] - before_y) + (up_z * p[2] - before_z)
        old = u_ref[z, r, :]
        pieces = [((old + TAU * div) * gain[z, r, :] + offset[z, r, :], old)]
        for k, (ax, ay, az) in enumerate(PARTS):
            after_x = jnp.where(last_lane, from_x[k], pltpu.roll(q[ax], xs - 1, 1))
            if b < blocks - 1:
                after_y = q_ref[ay, z, pl.ds(8 * b + 1, 8), :]
            else:
                after_y = jnp.where(last_row, row_q(ay, z), pltpu.roll(q[ay], 7, 0))
            after_z = plane_q(az, r) if z == zs - 1 else q_ref[az, z + 1, r, :]
            div2 = (after_x - lo_x * q[ax]) + (after_y - lo_y * q[ay]) + (after_z - lo_z * q[az])
            old = v_ref[k, z, r, :]
            pieces.append((old + TAU * (p[k] + div2), old))
        yield b, r, pieces


def kernel(
    noisy_in, fid_in, u_in, v_in, p_in, q_in,
    u_out, v_out, p_out, q_out, gain, offset, cp, edge_y, edge_z,
    bar, face,
    z_lo, z_hi, x_lo, x_hi, y_lo, y_hi, d_a, d_b, d_c, d_d, d_e, d_g,
    zp, zq, yp, yq, xs_own, xp, xq, cv, xe, part_p, part_q,
    load_sem, send_sem, recv_sem, first_send, first_recv,
):
    zs, ys, xs = u_in.shape
    blocks = ys // 8
    pairs = zs * blocks
    half_lanes = 2 * pairs
    place = [lax.axis_index(a) for a in AXES]
    count = [lax.axis_size(a) for a in AXES]
    below = [place[i] > 0 for i in range(3)]
    above = [place[i] < count[i] - 1 for i in range(3)]

    def exists(way):
        there = None
        for i, by in enumerate(way):
            if by:
                one = above[i] if by > 0 else below[i]
                there = one if there is None else jnp.logical_and(there, one)
        return there

    def target(way):
        return {AXES[i]: place[i] + by for i, by in enumerate(way) if by}

    goes = [exists(way) for way in WAYS]
    comes = [exists(tuple(-by for by in way)) for way in WAYS]
    peers = sum(there.astype(jnp.int32) for there in goes)

    u_face, xf, top_face = pl.ds(0, 4), pl.ds(4, 2), pl.ds(6, 4)
    loads = [
        pltpu.make_async_copy(u_in, bar.at[0], load_sem.at[0]),
        pltpu.make_async_copy(v_in, bar.at[pl.ds(1, 3)], load_sem.at[1]),
        pltpu.make_async_copy(u_in.at[:, 0], face.at[0], load_sem.at[2]),
        pltpu.make_async_copy(v_in.at[:, :, 0], face.at[pl.ds(1, 3)], load_sem.at[3]),
        pltpu.make_async_copy(u_in.at[:, ys - 1], face.at[6], load_sem.at[4]),
        pltpu.make_async_copy(v_in.at[:, :, ys - 1], face.at[pl.ds(7, 3)], load_sem.at[5]),
        pltpu.make_async_copy(q_in, q_out, load_sem.at[6]),
        pltpu.make_async_copy(p_in, p_out, load_sem.at[7]),
        pltpu.make_async_copy(noisy_in, offset, load_sem.at[8]),
        pltpu.make_async_copy(fid_in, gain, load_sem.at[9]),
        pltpu.make_async_copy(u_in, u_out, load_sem.at[10]),
        pltpu.make_async_copy(v_in, v_out, load_sem.at[11]),
    ]
    for load in loads[:2]:
        load.start()

    barrier = pltpu.get_barrier_semaphore()
    for way, there in zip(WAYS, goes):
        @pl.when(there)
        def _():
            pl.semaphore_signal(barrier, inc=1, device_id=target(way), device_id_type=MESH)

    for load in loads[2:8]:
        load.start()

    def clear(there, *refs):
        @pl.when(jnp.logical_not(there))
        def _():
            for ref in refs:
                ref[...] = jnp.zeros(ref.shape, jnp.float32)

    clear(below[0], x_lo, xp)
    clear(above[0], x_hi, xq)
    clear(below[1], y_lo, yp)
    clear(above[1], y_hi, yq)
    clear(below[2], z_lo, zp)
    clear(above[2], z_hi, zq)
    for way, ref in zip(WAYS[6:], (d_a, d_b, d_c, d_d, d_e, d_g)):
        clear(exists(tuple(-by for by in way)), ref)

    lane = lax.broadcasted_iota(jnp.int32, (8, xs), 1)
    sub = lax.broadcasted_iota(jnp.int32, (8, xs), 0)
    pair = lane >> 1
    odd = (lane & 1) == 1
    first_lane, last_lane = lane == 0, lane == xs - 1
    first_row, last_row = sub == 0, sub == 7
    p_pair, q_pair = (lane - half_lanes) >> 1, (lane + 1 - half_lanes) >> 1

    def factor(flag):
        return jnp.where(flag, jnp.float32(1), jnp.float32(0))

    up_x = jnp.where(last_lane, factor(above[0]), 1.0)
    lo_x = jnp.where(first_lane, factor(below[0]), 1.0)
    up_y_last = jnp.where(last_row, factor(above[1]), 1.0)
    lo_y_first = jnp.where(first_row, factor(below[1]), 1.0)

    def rows(b, by=0):
        return pl.ds(8 * b + by, 8)

    def turn_lanes(value, by):
        return value if isinstance(by, int) and by % xs == 0 else pltpu.roll(value, by % xs if isinstance(by, int) else by, 1)

    def turn_rows(value, by):
        return pltpu.roll(value, by % 8, 0)

    def flush(later):
        for ref, at, value in later:
            ref[at + (slice(None),)] = value
        later.clear()

    def up_z(z):
        return factor(jnp.logical_or(z < zs - 1, above[2]))

    def lo_z(z):
        return factor(jnp.logical_or(z > 0, below[2]))

    def up_y(b, value):
        return up_y_last * value if b == blocks - 1 else value

    def lo_y(b, value):
        return lo_y_first * value if b == 0 else value

    def next_x(value):
        return jnp.where(last_lane, 0.0, pltpu.roll(value, xs - 1, 1))

    def prev_x(value):
        return jnp.where(first_lane, 0.0, pltpu.roll(value, 1, 1))

    def next_y(ref, k, z, b, value):
        if b < blocks - 1:
            return ref[k, z, rows(b, 1), :]
        return jnp.where(last_row, 0.0, pltpu.roll(value, 7, 0))

    def prev_y(ref, k, z, b, value):
        if b > 0:
            return ref[k, z, rows(b, -1), :]
        return jnp.where(first_row, 0.0, pltpu.roll(value, 1, 0))

    def next_z(ref, k, z, b):
        if isinstance(z, int):
            return ref[k, z + 1, rows(b), :] if z < zs - 1 else jnp.zeros((8, xs), jnp.float32)
        return factor(z < zs - 1) * ref[k, jnp.minimum(z + 1, zs - 1), rows(b), :]

    def prev_z(ref, k, z, b):
        if isinstance(z, int):
            return ref[k, z - 1, rows(b), :] if z > 0 else jnp.zeros((8, xs), jnp.float32)
        return factor(z > 0) * ref[k, jnp.maximum(z - 1, 0), rows(b), :]

    def shrink_p(t):
        size = t[0] * t[0] + t[1] * t[1] + t[2] * t[2]
        scale = jnp.minimum(1.0, ALPHA1 * lax.rsqrt(size))
        return [scale * part for part in t]

    def shrink_q(s):
        size = (s[XX] * s[XX] + s[YY] * s[YY] + s[ZZ] * s[ZZ]) + 2.0 * (
            s[XY] * s[XY] + s[XZ] * s[XZ] + s[YZ] * s[YZ]
        )
        scale = jnp.minimum(1.0, ALPHA0 * lax.rsqrt(size))
        return [scale * part for part in s]

    half = 0.5 * SIGMA

    def grow_q(q, dx, dy, dz):
        return [
            q[XX] + SIGMA * dx[0], q[YY] + SIGMA * dy[1], q[ZZ] + SIGMA * dz[2],
            q[XY] + half * (dy[0] + dx[1]), q[XZ] + half * (dz[0] + dx[2]),
            q[YZ] + half * (dz[1] + dy[2]),
        ]

    def keep(flag, value):
        return jnp.where(flag, value, 0.0)

    def pack(packed, value, base, j):
        return jnp.where(pair == base + j, pltpu.roll(value, 2 * (base + j) + 1, 1), packed)

    def pack_bar(packed, values, z, b):
        j = z * blocks + b
        packed[0] = pack(packed[0], values[0], 0, j)
        packed[0] = pack(packed[0], values[1], pairs, j)
        packed[1] = pack(packed[1], values[2], 0, j)
        packed[1] = pack(packed[1], values[3], pairs, j)

    def message(src, dst, way, send, recv):
        return pltpu.make_async_remote_copy(
            src_ref=src, dst_ref=dst, send_sem=send, recv_sem=recv,
            device_id=target(WAYS[way]), device_id_type=MESH,
        )

    exchanges = []
    for s in range(ITERS):
        z_up_part = pl.ds(1, 3) if s == 0 else pl.ds(0, 4)
        z_down_part = pl.ds(0, 1) if s == 0 else pl.ds(0, 4)
        ends = (
            (bar.at[z_up_part, zs - 1], z_lo.at[s, z_up_part]),
            (bar.at[z_down_part, 0], z_hi.at[s, z_down_part]),
            (face.at[xf], x_lo.at[s]),
            (face.at[xf], x_hi.at[s]),
            (face.at[top_face], y_lo.at[s]),
            (face.at[u_face], y_hi.at[s]),
            (face.at[xf, pl.ds(0, 1)], d_a.at[s, :, pl.ds(0, 1)]),
            (face.at[xf, pl.ds(7, 1)], d_b.at[s, :, pl.ds(7, 1)]),
            (xe, d_c.at[s]),
            (xe, d_d.at[s]),
            (face.at[top_face, pl.ds(0, 1)], d_e.at[s, :, pl.ds(0, 1)]),
            (face.at[u_face, pl.ds(zs - 1, 1)], d_g.at[s, :, pl.ds(zs - 1, 1)]),
        )
        exchanges.append([
            (message(src, dst, k, send_sem.at[s, k], recv_sem.at[s, k]), goes[k], comes[k])
            for k, (src, dst) in enumerate(ends)
        ])
    duals = [
        (message(src, dst, way, first_send.at[k], first_recv.at[k]), goes[way], comes[way])
        for k, (src, dst, way) in enumerate((
            (p_out.at[:, zs - 1], zp, Z_UP),
            (q_out.at[:, 0], zq, Z_DOWN),
            (p_in.at[:, :, ys - 1], yp, Y_UP),
            (q_in.at[:, :, 0], yq, Y_DOWN),
            (xs_own, xp, X_UP),
            (xs_own, xq, X_DOWN),
        ))
    ]

    def start(moves):
        for copy, there, _ in moves:
            @pl.when(there)
            def _():
                copy.start()

    def sent(moves):
        for copy, there, _ in moves:
            @pl.when(there)
            def _():
                copy.wait_send()

    def got(moves):
        for copy, _, there in moves:
            @pl.when(there)
            def _():
                copy.wait_recv()

    empty = jnp.zeros((8, xs), jnp.float32)

    def each(low, high, body, carry):
        def turn(j, carry):
            one = list(carry)
            body(low + 2 * j, one)
            body(low + 2 * j + 1, one)
            return tuple(one)

        return lax.fori_loop(0, (high - low) // 2, turn, tuple(carry))

    def dual_inside(z, _):
        later = []
        z_up, z_lo_ = up_z(z), lo_z(z)
        for b in range(blocks):
            r = rows(b)
            u = bar[0, z, r, :]
            v = [bar[1 + k, z, r, :] for k in range(3)]
            slopes = (
                next_x(u) - up_x * u,
                next_y(bar, 0, z, b, u) - up_y(b, u),
                next_z(bar, 0, z, b) - z_up * u,
            )
            for k in range(3):
                later.append((p_out, (k, z, r), p_out[k, z, r, :] + SIGMA * (slopes[k] - v[k])))
            dx = [lo_x * v[k] - prev_x(v[k]) for k in range(3)]
            dy = [lo_y(b, v[k]) - prev_y(bar, 1 + k, z, b, v[k]) for k in range(3)]
            dz = [z_lo_ * v[k] - prev_z(bar, 1 + k, z, b) for k in range(3)]
            for k, new in enumerate(grow_q([q_out[k, z, r, :] for k in range(6)], dx, dy, dz)):
                later.append((q_out, (k, z, r), new))
        flush(later)

    def line_up(s):
        cv[0] = jnp.where(odd, turn_lanes(x_hi[s, 0], half_lanes - 2), x_lo[s, 0])
        cv[1] = turn_lanes(x_lo[s, 1], half_lanes)
        cv[2] = x_lo[s, 1]

    def less_q(q, x=None, y=None, z=None):
        q = list(q)
        if x is not None:
            q[XX] = q[XX] - SIGMA * x[0]
            q[XY] = q[XY] - half * x[1]
            q[XZ] = q[XZ] - half * x[2]
        if y is not None:
            q[YY] = q[YY] - SIGMA * y[1]
            q[XY] = q[XY] - half * y[0]
            q[YZ] = q[YZ] - half * y[2]
        if z is not None:
            q[ZZ] = q[ZZ] - SIGMA * z[2]
            q[XZ] = q[XZ] - half * z[0]
            q[YZ] = q[YZ] - half * z[1]
        return q

    def dual(z, s):
        later = []
        for b in range(blocks):
            r = rows(b)
            by = half_lanes - 2 * (z * blocks + b)
            from_x = [turn_lanes(cv[k], by) for k in range(3)]
            t = [p_out[k, z, r, :] for k in range(3)]
            t[0] = t[0] + SIGMA * jnp.where(last_lane, from_x[0], 0.0)
            if b == blocks - 1:
                t[1] = t[1] + SIGMA * jnp.where(last_row, y_hi[s, 0, pl.ds(z, 1), :], 0.0)
            for k in range(3):
                if z == zs - 1:
                    later.append((part_p, (k, r), t[k]))
            if z < zs - 1:
                for k, new in enumerate(shrink_p(t)):
                    later.append((p_out, (k, z, r), new))
            hx = [jnp.where(first_lane, part, 0.0) for part in from_x]
            hy = None
            if b == 0:
                hy = [jnp.where(first_row, y_lo[s, 1 + k, pl.ds(z, 1), :], 0.0) for k in range(3)]
            q = less_q([q_out[k, z, r, :] for k in range(6)], hx, hy)
            if z > 0:
                q = shrink_q(q)
            for k in range(6):
                later.append((part_q, (k, r), q[k]) if z == 0 else (q_out, (k, z, r), q[k]))
        flush(later)

    def dual_ends(s):
        later = []
        for b in range(blocks):
            r = rows(b)
            t = [part_p[k, r, :] for k in range(3)]
            t[2] = t[2] + SIGMA * z_hi[s, 0, r, :]
            for k, new in enumerate(shrink_p(t)):
                later.append((p_out, (k, zs - 1, r), new))
            q = less_q([part_q[k, r, :] for k in range(6)], z=[z_lo[s, 1 + k, r, :] for k in range(3)])
            for k, new in enumerate(shrink_q(q)):
                later.append((q_out, (k, 0, r), new))
        flush(later)

    def spread(row):
        return jnp.broadcast_to(row, (8, xs))

    def column(row, lane_of_first):
        mine = lane == lane_of_first + 2 * blocks * sub
        return jnp.sum(jnp.where(mine, spread(row), 0.0), axis=1, keepdims=True)

    where = ((0, half_lanes), (1, 0), (1, half_lanes))

    def halo_x_inside(s):
        far = pairs - blocks
        up_yc = jnp.where(jnp.logical_and(last_row, (p_pair & (blocks - 1)) == blocks - 1), factor(above[1]), 1.0)
        lo_yc = jnp.where(jnp.logical_and(first_row, (q_pair & (blocks - 1)) == 0), factor(below[1]), 1.0)
        up_zc = jnp.where(p_pair >= far, factor(above[2]), 1.0)
        lo_zc = jnp.where(q_pair < blocks, factor(below[2]), 1.0)
        u = turn_lanes(x_lo[s, 0], half_lanes)
        v = [x_lo[s, 0], turn_lanes(x_lo[s, 1], half_lanes), x_lo[s, 1]]
        own = turn_lanes(face[4], half_lanes - 1)
        moved = turn_rows(u, -1)
        turned = jnp.where((p_pair & (blocks - 1)) == blocks - 1, 0.0, turn_lanes(moved, -2))
        ahead_y = jnp.where(last_row, turned, moved)
        ahead_z = jnp.where(p_pair >= far, 0.0, turn_lanes(u, -2 * blocks))
        slopes = (own - u, ahead_y - up_yc * u, ahead_z - up_zc * u)
        for k in range(3):
            xp[k] = xp[k] + SIGMA * (slopes[k] - v[k])

        v = [turn_lanes(x_hi[s, 0], -2), turn_lanes(x_hi[s, 1], half_lanes - 2), turn_lanes(x_hi[s, 1], -2)]
        mine = [turn_lanes(face[4], -1), turn_lanes(face[5], half_lanes - 1), turn_lanes(face[5], -1)]
        dx, dy, dz = [], [], []
        for k in range(3):
            dx.append(v[k] - mine[k])
            moved = turn_rows(v[k], 1)
            turned = jnp.where((q_pair & (blocks - 1)) == 0, 0.0, turn_lanes(moved, 2))
            dy.append(lo_yc * v[k] - jnp.where(first_row, turned, moved))
            dz.append(lo_zc * v[k] - jnp.where(q_pair < blocks, 0.0, turn_lanes(v[k], 2 * blocks)))
        q = [turn_lanes(xq[k], -2) if s == 0 else xq[k] for k in range(6)]
        for k, new in enumerate(grow_q(q, dx, dy, dz)):
            xq[k] = new

    def halo_x(s):
        far = pairs - blocks
        t = [xp[k] for k in range(3)]
        edge = turn_lanes(spread(d_a[s, 0, pl.ds(0, 1), :]), half_lanes + 2 * (blocks - 1))
        here = jnp.logical_and(last_row, (p_pair & (blocks - 1)) == blocks - 1)
        t[1] = t[1] + SIGMA * jnp.where(here, edge, 0.0)
        edge = turn_lanes(d_c[s, 0], half_lanes + 2 * far)
        t[2] = t[2] + SIGMA * jnp.where(p_pair >= far, edge, 0.0)
        p = [keep(below[0], part) for part in shrink_p(t)]
        here = jnp.logical_and(first_row, (q_pair & (blocks - 1)) == 0)
        edge_y, edge_z = [], []
        for h, base in where:
            edge = turn_lanes(spread(d_b[s, h, pl.ds(7, 1), :]), half_lanes - 2 * blocks - base)
            edge_y.append(jnp.where(here, edge, 0.0))
            edge = turn_lanes(d_d[s, h], half_lanes - 2 - 2 * far - base)
            edge_z.append(jnp.where(q_pair < blocks, edge, 0.0))
        q = shrink_q(less_q([xq[k] for k in range(6)], y=edge_y, z=edge_z))
        q = [keep(above[0], part) for part in q]
        for k in range(3):
            xp[k] = p[k]
        for k in range(6):
            xq[k] = q[k]
        cp[0] = jnp.where(odd, q[XX], p[0])
        cp[1] = q[XY]
        cp[2] = q[XZ]

    def halo_y_inside(s):
        up_zr = jnp.where(last_row, factor(above[2]), 1.0)
        lo_zr = jnp.where(first_row, factor(below[2]), 1.0)
        u = y_lo[s, 0]
        slopes = (
            next_x(u) - up_x * u,
            face[0] - u,
            jnp.where(last_row, 0.0, turn_rows(u, -1)) - up_zr * u,
        )
        for k in range(3):
            yp[k] = yp[k] + SIGMA * (slopes[k] - y_lo[s, 1 + k])
        v = [y_hi[s, 1 + k] for k in range(3)]
        dx = [lo_x * v[k] - prev_x(v[k]) for k in range(3)]
        dy = [v[k] - face[7 + k] for k in range(3)]
        dz = [lo_zr * v[k] - jnp.where(first_row, 0.0, turn_rows(v[k], 1)) for k in range(3)]
        for k, new in enumerate(grow_q([yq[k] for k in range(6)], dx, dy, dz)):
            yq[k] = new

    def halo_y(s):
        t = [yp[k] for k in range(3)]
        edge = column(d_b[s, 0, pl.ds(7, 1), :], 2 * blocks - 1)
        t[0] = t[0] + SIGMA * jnp.where(last_lane, edge, 0.0)
        t[2] = t[2] + SIGMA * jnp.where(last_row, d_e[s, 0, pl.ds(0, 1), :], 0.0)
        p = shrink_p(t)
        edge_x = [
            jnp.where(first_lane, column(d_a[s, h, pl.ds(0, 1), :], base), 0.0) for h, base in where
        ]
        edge_z = [jnp.where(first_row, d_g[s, 1 + k, pl.ds(zs - 1, 1), :], 0.0) for k in range(3)]
        q = shrink_q(less_q([yq[k] for k in range(6)], x=edge_x, z=edge_z))
        for k in range(3):
            yp[k] = keep(below[1], p[k])
        for k in range(6):
            yq[k] = keep(above[1], q[k])

    def halo_z_first():
        later = []
        for b in range(blocks):
            r = rows(b)
            t = [zp[k, r, :] for k in range(3)]
            edge_x = turn_lanes(d_d[0, 0], xs - 2 - 2 * (blocks * (zs - 1) + b))
            t[0] = t[0] + SIGMA * jnp.where(last_lane, edge_x, 0.0)
            if b == blocks - 1:
                t[1] = t[1] + SIGMA * jnp.where(last_row, d_g[0, 0, pl.ds(zs - 1, 1), :], 0.0)
            t[2] = t[2] + SIGMA * bar[0, 0, r, :]
            for k, new in enumerate(shrink_p(t)):
                later.append((zp, (k, r), keep(below[2], new)))

            hx = [
                jnp.where(first_lane, turn_lanes(d_c[0, h], -base - 2 * b), 0.0) for h, base in where
            ]
            hz = [bar[1 + k, zs - 1, r, :] for k in range(3)]
            hy = None
            if b == 0:
                hy = [jnp.where(first_row, d_e[0, 1 + k, pl.ds(0, 1), :], 0.0) for k in range(3)]
            q = less_q([zq[k, r, :] for k in range(6)], hx, hy, hz)
            for k, new in enumerate(shrink_q(q)):
                later.append((zq, (k, r), keep(above[2], new)))
        flush(later)

    def halo_z(s):
        later = []
        for b in range(blocks):
            r = rows(b)
            u = z_lo[s, 0, r, :]
            edge_x = turn_lanes(d_d[s, 0], xs - 2 - 2 * (blocks * (zs - 1) + b))
            if b < blocks - 1:
                ahead_y = z_lo[s, 0, rows(b, 1), :]
            else:
                ahead_y = jnp.where(last_row, d_g[s, 0, pl.ds(zs - 1, 1), :], turn_rows(u, -1))
            slopes = (
                jnp.where(last_lane, edge_x, turn_lanes(u, -1)) - up_x * u,
                ahead_y - up_y(b, u),
                bar[0, 0, r, :] - u,
            )
            p = shrink_p([zp[k, r, :] + SIGMA * (slopes[k] - z_lo[s, 1 + k, r, :]) for k in range(3)])
            for k in range(3):
                later.append((zp, (k, r), keep(below[2], p[k])))

            v = [z_hi[s, 1 + k, r, :] for k in range(3)]
            dx, dy, dz = [], [], []
            for k, (h, base) in enumerate(where):
                edge_x = turn_lanes(d_c[s, h], -base - 2 * b)
                dx.append(lo_x * v[k] - jnp.where(first_lane, edge_x, turn_lanes(v[k], 1)))
                if b > 0:
                    behind_y = z_hi[s, 1 + k, rows(b, -1), :]
                else:
                    behind_y = jnp.where(first_row, d_e[s, 1 + k, pl.ds(0, 1), :], turn_rows(v[k], 1))
                dy.append(lo_y(b, v[k]) - behind_y)
                dz.append(v[k] - bar[1 + k, zs - 1, r, :])
            q = shrink_q(grow_q([zq[k, r, :] for k in range(6)], dx, dy, dz))
            for k in range(6):
                later.append((zq, (k, r), keep(above[2], q[k])))
        flush(later)

    def pack_plane(packed, z):
        for b in range(blocks):
            pack_bar(packed, [bar[k, z, rows(b), :] for k in range(4)], z, b)

    halo = (
        cp,
        lambda z: yp[1, pl.ds(z, 1), :],
        lambda k, z: yq[k, pl.ds(z, 1), :],
        lambda r: zp[2, r, :],
        lambda k, r: zq[k, r, :],
    )

    def primal(z):
        later = []
        for b, r, pieces in primal_plane(z, below, above, u_out, v_out, p_out, q_out, gain, offset, halo):
            for k, (new, old) in enumerate(pieces):
                later.append((u_out, (z, r), new) if k == 0 else (v_out, (k - 1, z, r), new))
                ahead = 2.0 * new - old
                later.append((bar, (k, z, r), ahead))
                if b == 0:
                    later.append((face, (k, pl.ds(z, 1)), ahead[0:1, :]))
                if b == blocks - 1:
                    later.append((face, (6 + k, pl.ds(z, 1)), ahead[7:8, :]))
        flush(later)

    def pack_dual(packed, z):
        for b in range(blocks):
            for k in range(6):
                value = q_out[k, z, rows(b), :]
                if k < 3:
                    value = jnp.where(last_lane, p_out[k, z, rows(b), :], value)
                packed[k] = pack(packed[k], value, pairs, z * blocks + b)

    def prepare(z, carry):
        weight = TAU * gain[z]
        inverse = 1.0 / (1.0 + weight)
        gain[z] = inverse
        offset[z] = weight * offset[z] * inverse
        return carry

    ends, middle = (0, zs - 1), range(1, zs - 1)
    with jax.named_scope("load_uv"):
        for load in loads[:2]:
            load.wait()
    with jax.named_scope("barrier"):
        pl.semaphore_wait(barrier, peers)
    with jax.named_scope("send_z0"):
        start(exchanges[0][:2])
        start(duals[2:4])
        for load in loads[8:]:
            load.start()
    with jax.named_scope("load_face"):
        for load in loads[2:6]:
            load.wait()
        start(exchanges[0][4:6])
    with jax.named_scope("pack_uv"):
        packed = [empty, empty]
        for z in ends:
            pack_plane(packed, z)
        xe[0] = packed[0]
        xe[1] = packed[1]
        for z in middle:
            pack_plane(packed, z)
        face[4] = packed[0]
        face[5] = packed[1]
        start(exchanges[0][8:])
        start(exchanges[0][6:8])
        start(exchanges[0][2:4])
    with jax.named_scope("load_pq"):
        for load in loads[6:8]:
            load.wait()
    with jax.named_scope("pack_pq"):
        packed = [empty] * 6
        for z in ends:
            pack_dual(packed, z)
        for z in ends:
            dual_inside(z, None)
        start(duals[:2])
    with jax.named_scope("pack_pq_rest"):
        for z in middle:
            pack_dual(packed, z)
        for k in range(6):
            xs_own[k] = packed[k]
        start(duals[4:])
    with jax.named_scope("inside0"):
        each(1, zs - 1, dual_inside, ())
    with jax.named_scope("prepare"):
        for load in loads[8:]:
            load.wait()
        lax.fori_loop(0, zs, prepare, 0)

    for s in range(ITERS):
        last = s == ITERS - 1
        moves = exchanges[s]
        if s > 0:
            with jax.named_scope(f"inside{s}"):
                each(0, zs, dual_inside, ())
        with jax.named_scope(f"wait_xy{s}"):
            got(moves[2:6])
            line_up(s)
        with jax.named_scope(f"dual_mid{s}"):
            for z in range(zs):
                dual(z, s)
            if s > 0:
                halo_x_inside(s)
                halo_y_inside(s)
        if s == 0:
            with jax.named_scope(f"wait_pq{s}"):
                got(duals[2:])
                halo_x_inside(s)
                halo_y_inside(s)
        with jax.named_scope(f"wait_diag{s}"):
            got(moves[6:])
        with jax.named_scope(f"halo_xy{s}"):
            halo_x(s)
            halo_y(s)
        with jax.named_scope(f"wait_z{s}"):
            got(moves[:2])
            sent(moves)
        if s == 0:
            with jax.named_scope(f"wait_zpq{s}"):
                got(duals[:2])
                sent(duals)
        with jax.named_scope(f"ends{s}"):
            if s == 0:
                halo_z_first()
            else:
                halo_z(s)
            dual_ends(s)
            if last:
                edge_y[0] = yp[1]
                edge_z[0] = zp[2]
                for at, k in enumerate(Y_PARTS):
                    edge_y[1 + at] = yq[k]
                for at, k in enumerate(Z_PARTS):
                    edge_z[1 + at] = zq[k]
                continue
            packed = [empty, empty]
            for z in ends:
                primal(z)
            for z in ends:
                pack_plane(packed, z)
            xe[0] = packed[0]
            xe[1] = packed[1]
        with jax.named_scope(f"send_z{s}"):
            start(exchanges[s + 1][8:])
            start(exchanges[s + 1][:2])
        with jax.named_scope(f"primal_mid{s}"):
            for z in middle:
                primal(z)
            for z in middle:
                pack_plane(packed, z)
            face[4] = packed[0]
            face[5] = packed[1]
        with jax.named_scope(f"send{s}"):
            start(exchanges[s + 1][6:8])
            start(exchanges[s + 1][2:6])


def last_primal(
    u_in, v_in, p_in, q_in, gain, offset, cp, edge_y, edge_z,
    u_out, v_out, p_out, q_out,
    u_new, v_new, sems,
):
    zs, ys, xs = u_in.shape
    place = [lax.axis_index(a) for a in AXES]
    count = [lax.axis_size(a) for a in AXES]
    below = [place[i] > 0 for i in range(3)]
    above = [place[i] < count[i] - 1 for i in range(3)]
    copies = [pltpu.make_async_copy(q_in.at[k], q_out.at[k], sems.at[k]) for k in range(6)]
    copies += [pltpu.make_async_copy(p_in.at[k], p_out.at[k], sems.at[6 + k]) for k in range(3)]
    for copy in copies:
        copy.start()
    halo = (
        cp,
        lambda z: edge_y[0, pl.ds(z, 1), :],
        lambda k, z: edge_y[1 + Y_PARTS.index(k), pl.ds(z, 1), :],
        lambda r: edge_z[0, r, :],
        lambda k, r: edge_z[1 + Z_PARTS.index(k), r, :],
    )
    for z in range(zs):
        for _, r, pieces in primal_plane(z, below, above, u_in, v_in, p_in, q_in, gain, offset, halo):
            u_new[z, r, :] = pieces[0][0]
            for k in range(3):
                v_new[k, z, r, :] = pieces[1 + k][0]
        if z % 2 == 1:
            two = pl.ds(z - 1, 2)
            mine = [
                pltpu.make_async_copy(v_new.at[:, two], v_out.at[:, two], sems.at[9 + z - 1]),
                pltpu.make_async_copy(u_new.at[two], u_out.at[two], sems.at[9 + z]),
            ]
            for copy in mine:
                copy.start()
            copies += mine
    for copy in copies:
        copy.wait()


def per_device(noisy_image, fidelity, primal_u, primal_v, dual_p, dual_q):
    zs, ys, xs = primal_u.shape
    blocks = ys // 8
    assert zs == 8 and ys % 8 == 0 and blocks & (blocks - 1) == 0 and 4 * zs * blocks == xs == 128
    f32 = jnp.float32

    def vmem(*shape):
        return pltpu.VMEM(shape, f32)

    shapes = [a.shape for a in (primal_u, primal_v, dual_p, dual_q)]
    kept = shapes + [(zs, ys, xs), (zs, ys, xs), (3, 8, xs), (4, 8, xs), (4, ys, xs)]
    results = pl.pallas_call(
        kernel,
        out_shape=tuple(vmem(*shape) for shape in kept),
        in_specs=[pl.BlockSpec(memory_space=pl.ANY)] * 6,
        out_specs=tuple([pl.BlockSpec(memory_space=pltpu.VMEM)] * len(kept)),
        scratch_shapes=[
            vmem(4, zs, ys, xs),
            vmem(10, 8, xs),
            vmem(ITERS, 4, ys, xs),
            vmem(ITERS, 4, ys, xs),
            vmem(ITERS, 2, 8, xs),
            vmem(ITERS, 2, 8, xs),
            vmem(ITERS, 4, 8, xs),
            vmem(ITERS, 4, 8, xs),
            vmem(ITERS, 2, 8, xs),
            vmem(ITERS, 2, 8, xs),
            vmem(ITERS, 2, 8, xs),
            vmem(ITERS, 2, 8, xs),
            vmem(ITERS, 4, 8, xs),
            vmem(ITERS, 4, 8, xs),
            vmem(3, ys, xs),
            vmem(6, ys, xs),
            vmem(3, 8, xs),
            vmem(6, 8, xs),
            vmem(6, 8, xs),
            vmem(6, 8, xs),
            vmem(6, 8, xs),
            vmem(3, 8, xs),
            vmem(2, 8, xs),
            vmem(3, ys, xs),
            vmem(6, ys, xs),
            pltpu.SemaphoreType.DMA((12,)),
            pltpu.SemaphoreType.DMA((ITERS, 12)),
            pltpu.SemaphoreType.DMA((ITERS, 12)),
            pltpu.SemaphoreType.DMA((6,)),
            pltpu.SemaphoreType.DMA((6,)),
        ],
        compiler_params=pltpu.CompilerParams(collective_id=0, has_side_effects=True),
        name="tgv",
    )(noisy_image, fidelity, primal_u, primal_v, dual_p, dual_q)
    return pl.pallas_call(
        last_primal,
        out_shape=tuple(jax.ShapeDtypeStruct(shape, f32) for shape in shapes),
        in_specs=[pl.BlockSpec(memory_space=pltpu.VMEM)] * len(kept),
        out_specs=tuple([pl.BlockSpec(memory_space=pl.ANY)] * 4),
        scratch_shapes=[
            vmem(zs, ys, xs),
            vmem(3, zs, ys, xs),
            pltpu.SemaphoreType.DMA((9 + zs,)),
        ],
        name="out",
    )(*[pltpu.with_memory_space_constraint(r, pltpu.VMEM) for r in results])


def solution(mesh):
    scalar, stack = P("gz", "gy", "gx"), P(None, "gz", "gy", "gx")
    return jax.shard_map(
        per_device,
        mesh=mesh,
        in_specs=(scalar, scalar, scalar, stack, stack, stack),
        out_specs=(scalar, stack, stack, stack),
        check_vma=False,
    )
```

```python
import jax
import jax.numpy as jnp
from jax import lax
from jax.experimental import pallas as pl
from jax.experimental.pallas import tpu as pltpu
from jax.sharding import PartitionSpec as P

ITERS = 3
AXES = ("gx", "gy", "gz")
ALPHA1, ALPHA0, SIGMA, TAU = 0.5, 1.0, 0.2, 0.2
XX, YY, ZZ, XY, XZ, YZ = range(6)
PARTS = ((XX, XY, XZ), (XY, YY, YZ), (XZ, YZ, ZZ))
Y_PARTS, Z_PARTS = (XY, YY, YZ), (XZ, YZ, ZZ)
MESH = pl.DeviceIdType.MESH
Z_UP, Z_DOWN, X_UP, X_DOWN, Y_UP, Y_DOWN, XY_A, XY_B, XZ_A, XZ_B, YZ_A, YZ_B = range(12)
WAYS = (
    (0, 0, 1), (0, 0, -1), (1, 0, 0), (-1, 0, 0), (0, 1, 0), (0, -1, 0),
    (1, -1, 0), (-1, 1, 0), (1, 0, -1), (-1, 0, 1), (0, 1, -1), (0, -1, 1),
)


def primal_plane(z, below, above, u_ref, v_ref, p_ref, q_ref, gain, offset, halo):
    zs, ys, xs = u_ref.shape
    blocks = ys // 8
    cp, row_p, row_q, plane_p, plane_q = halo
    lane = lax.broadcasted_iota(jnp.int32, (8, xs), 1)
    sub = lax.broadcasted_iota(jnp.int32, (8, xs), 0)
    first_lane, last_lane = lane == 0, lane == xs - 1
    first_row, last_row = sub == 0, sub == 7

    def factor(flag):
        return jnp.where(flag, jnp.float32(1), jnp.float32(0))

    up_x = jnp.where(last_lane, factor(above[0]), 1.0)
    lo_x = jnp.where(first_lane, factor(below[0]), 1.0)
    up_z = factor(above[2]) if z == zs - 1 else 1.0
    lo_z = factor(below[2]) if z == 0 else 1.0
    for b in range(blocks):
        r = pl.ds(8 * b, 8)
        up_y = jnp.where(last_row, factor(above[1]), 1.0) if b == blocks - 1 else 1.0
        lo_y = jnp.where(first_row, factor(below[1]), 1.0) if b == 0 else 1.0
        by = xs // 2 - 2 * (z * blocks + b)
        from_x = [pltpu.roll(cp[k], by, 1) for k in range(3)]
        p = [p_ref[k, z, r, :] for k in range(3)]
        q = [q_ref[k, z, r, :] for k in range(6)]
        before_x = jnp.where(first_lane, from_x[0], pltpu.roll(p[0], 1, 1))
        if b > 0:
            before_y = p_ref[1, z, pl.ds(8 * b - 1, 8), :]
        else:
            before_y = jnp.where(first_row, row_p(z), pltpu.roll(p[1], 1, 0))
        before_z = plane_p(r) if z == 0 else p_ref[2, z - 1, r, :]
        div = (up_x * p[0] - before_x) + (up_y * p[1] - before_y) + (up_z * p[2] - before_z)
        old = u_ref[z, r, :]
        pieces = [((old + TAU * div) * gain[z, r, :] + offset[z, r, :], old)]
        for k, (ax, ay, az) in enumerate(PARTS):
            after_x = jnp.where(last_lane, from_x[k], pltpu.roll(q[ax], xs - 1, 1))
            if b < blocks - 1:
                after_y = q_ref[ay, z, pl.ds(8 * b + 1, 8), :]
            else:
                after_y = jnp.where(last_row, row_q(ay, z), pltpu.roll(q[ay], 7, 0))
            after_z = plane_q(az, r) if z == zs - 1 else q_ref[az, z + 1, r, :]
            div2 = (after_x - lo_x * q[ax]) + (after_y - lo_y * q[ay]) + (after_z - lo_z * q[az])
            old = v_ref[k, z, r, :]
            pieces.append((old + TAU * (p[k] + div2), old))
        yield b, r, pieces


def kernel(
    noisy_in, fid_in, u_in, v_in, p_in, q_in,
    u_out, v_out, p_out, q_out, gain, offset, cp, edge_y, edge_z,
    bar, face,
    z_lo, z_hi, x_lo, x_hi, y_lo, y_hi, d_a, d_b, d_c, d_d, d_e, d_g,
    zp, zq, yp, yq, xs_own, xp, xq, cv, xe, part_p, part_q, tz_p, tz_q,
    load_sem, send_sem, recv_sem, first_send, first_recv,
):
    zs, ys, xs = u_in.shape
    blocks = ys // 8
    pairs = zs * blocks
    half_lanes = 2 * pairs
    place = [lax.axis_index(a) for a in AXES]
    count = [lax.axis_size(a) for a in AXES]
    below = [place[i] > 0 for i in range(3)]
    above = [place[i] < count[i] - 1 for i in range(3)]


    def exists(way):
        there = None
        for i, by in enumerate(way):
            if by:
                one = above[i] if by > 0 else below[i]
                there = one if there is None else jnp.logical_and(there, one)
        return there

    def target(way):
        return {AXES[i]: place[i] + by for i, by in enumerate(way) if by}

    goes = [exists(way) for way in WAYS]
    comes = [exists(tuple(-by for by in way)) for way in WAYS]
    peers = sum(there.astype(jnp.int32) for there in goes)

    u_face, xf, top_face = pl.ds(0, 4), pl.ds(4, 2), pl.ds(6, 4)
    loads = [
        pltpu.make_async_copy(u_in, bar.at[0], load_sem.at[0]),
        pltpu.make_async_copy(v_in, bar.at[pl.ds(1, 3)], load_sem.at[1]),
        pltpu.make_async_copy(u_in.at[:, 0], face.at[0], load_sem.at[2]),
        pltpu.make_async_copy(v_in.at[:, :, 0], face.at[pl.ds(1, 3)], load_sem.at[3]),
        pltpu.make_async_copy(u_in.at[:, ys - 1], face.at[6], load_sem.at[4]),
        pltpu.make_async_copy(v_in.at[:, :, ys - 1], face.at[pl.ds(7, 3)], load_sem.at[5]),
        pltpu.make_async_copy(q_in, q_out, load_sem.at[6]),
        pltpu.make_async_copy(p_in, p_out, load_sem.at[7]),
        pltpu.make_async_copy(noisy_in, offset, load_sem.at[8]),
        pltpu.make_async_copy(fid_in, gain, load_sem.at[9]),
        pltpu.make_async_copy(u_in, u_out, load_sem.at[10]),
        pltpu.make_async_copy(v_in, v_out, load_sem.at[11]),
    ]
    for load in loads[:2]:
        load.start()

    barrier = pltpu.get_barrier_semaphore()
    for way, there in zip(WAYS, goes):
        @pl.when(there)
        def _():
            pl.semaphore_signal(barrier, inc=1, device_id=target(way), device_id_type=MESH)

    for load in loads[2:8]:
        load.start()

    def clear(there, *refs):
        @pl.when(jnp.logical_not(there))
        def _():
            for ref in refs:
                ref[...] = jnp.zeros(ref.shape, jnp.float32)

    clear(below[0], x_lo, xp)
    clear(above[0], x_hi, xq)
    clear(below[1], y_lo, yp)
    clear(above[1], y_hi, yq)
    clear(below[2], z_lo, zp)
    clear(above[2], z_hi, zq)
    for way, ref in zip(WAYS[6:], (d_a, d_b, d_c, d_d, d_e, d_g)):
        clear(exists(tuple(-by for by in way)), ref)

    lane = lax.broadcasted_iota(jnp.int32, (8, xs), 1)
    sub = lax.broadcasted_iota(jnp.int32, (8, xs), 0)
    pair = lane >> 1
    odd = (lane & 1) == 1
    first_lane, last_lane = lane == 0, lane == xs - 1
    first_row, last_row = sub == 0, sub == 7
    p_pair, q_pair = (lane - half_lanes) >> 1, (lane + 1 - half_lanes) >> 1

    def factor(flag):
        return jnp.where(flag, jnp.float32(1), jnp.float32(0))

    up_x = jnp.where(last_lane, factor(above[0]), 1.0)
    lo_x = jnp.where(first_lane, factor(below[0]), 1.0)
    up_y_last = jnp.where(last_row, factor(above[1]), 1.0)
    lo_y_first = jnp.where(first_row, factor(below[1]), 1.0)

    def rows(b, by=0):
        return pl.ds(8 * b + by, 8)

    def turn_lanes(value, by):
        return value if isinstance(by, int) and by % xs == 0 else pltpu.roll(value, by % xs if isinstance(by, int) else by, 1)

    def turn_rows(value, by):
        return pltpu.roll(value, by % 8, 0)

    def flush(later):
        for ref, at, value in later:
            ref[at + (slice(None),)] = value
        later.clear()

    def up_z(z):
        return factor(jnp.logical_or(z < zs - 1, above[2]))

    def lo_z(z):
        return factor(jnp.logical_or(z > 0, below[2]))

    def up_y(b, value):
        return up_y_last * value if b == blocks - 1 else value

    def lo_y(b, value):
        return lo_y_first * value if b == 0 else value

    def next_x(value):
        return jnp.where(last_lane, 0.0, pltpu.roll(value, xs - 1, 1))

    def prev_x(value):
        return jnp.where(first_lane, 0.0, pltpu.roll(value, 1, 1))

    def next_y(ref, k, z, b, value):
        if b < blocks - 1:
            return ref[k, z, rows(b, 1), :]
        return jnp.where(last_row, 0.0, pltpu.roll(value, 7, 0))

    def prev_y(ref, k, z, b, value):
        if b > 0:
            return ref[k, z, rows(b, -1), :]
        return jnp.where(first_row, 0.0, pltpu.roll(value, 1, 0))

    def next_z(ref, k, z, b):
        if isinstance(z, int):
            return ref[k, z + 1, rows(b), :] if z < zs - 1 else jnp.zeros((8, xs), jnp.float32)
        return factor(z < zs - 1) * ref[k, jnp.minimum(z + 1, zs - 1), rows(b), :]

    def prev_z(ref, k, z, b):
        if isinstance(z, int):
            return ref[k, z - 1, rows(b), :] if z > 0 else jnp.zeros((8, xs), jnp.float32)
        return factor(z > 0) * ref[k, jnp.maximum(z - 1, 0), rows(b), :]

    def shrink_p(t):
        size = t[0] * t[0] + t[1] * t[1] + t[2] * t[2]
        scale = jnp.minimum(1.0, ALPHA1 * lax.rsqrt(size))
        return [scale * part for part in t]

    def shrink_q(s):
        size = (s[XX] * s[XX] + s[YY] * s[YY] + s[ZZ] * s[ZZ]) + 2.0 * (
            s[XY] * s[XY] + s[XZ] * s[XZ] + s[YZ] * s[YZ]
        )
        scale = jnp.minimum(1.0, ALPHA0 * lax.rsqrt(size))
        return [scale * part for part in s]

    half = 0.5 * SIGMA

    def grow_q(q, dx, dy, dz):
        return [
            q[XX] + SIGMA * dx[0], q[YY] + SIGMA * dy[1], q[ZZ] + SIGMA * dz[2],
            q[XY] + half * (dy[0] + dx[1]), q[XZ] + half * (dz[0] + dx[2]),
            q[YZ] + half * (dz[1] + dy[2]),
        ]

    def keep(flag, value):
        return jnp.where(flag, value, 0.0)

    def pack(packed, value, base, j):
        return jnp.where(pair == base + j, pltpu.roll(value, 2 * (base + j) + 1, 1), packed)

    def pack_bar(packed, values, z, b):
        j = z * blocks + b
        packed[0] = pack(packed[0], values[0], 0, j)
        packed[0] = pack(packed[0], values[1], pairs, j)
        packed[1] = pack(packed[1], values[2], 0, j)
        packed[1] = pack(packed[1], values[3], pairs, j)

    def message(src, dst, way, send, recv):
        return pltpu.make_async_remote_copy(
            src_ref=src, dst_ref=dst, send_sem=send, recv_sem=recv,
            device_id=target(WAYS[way]), device_id_type=MESH,
        )

    exchanges = []
    for s in range(ITERS):
        z_up_part = pl.ds(1, 3) if s == 0 else pl.ds(0, 4)
        z_down_part = pl.ds(0, 1) if s == 0 else pl.ds(0, 4)
        ends = (
            (bar.at[z_up_part, zs - 1], z_lo.at[s, z_up_part]),
            (bar.at[z_down_part, 0], z_hi.at[s, z_down_part]),
            (face.at[xf], x_lo.at[s]),
            (face.at[xf], x_hi.at[s]),
            (face.at[top_face], y_lo.at[s]),
            (face.at[u_face], y_hi.at[s]),
            (face.at[xf, pl.ds(0, 1)], d_a.at[s, :, pl.ds(0, 1)]),
            (face.at[xf, pl.ds(7, 1)], d_b.at[s, :, pl.ds(7, 1)]),
            (xe, d_c.at[s]),
            (xe, d_d.at[s]),
            (face.at[top_face, pl.ds(0, 1)], d_e.at[s, :, pl.ds(0, 1)]),
            (face.at[u_face, pl.ds(zs - 1, 1)], d_g.at[s, :, pl.ds(zs - 1, 1)]),
        )
        exchanges.append([
            (message(src, dst, k, send_sem.at[s, k], recv_sem.at[s, k]), goes[k], comes[k])
            for k, (src, dst) in enumerate(ends)
        ])
    duals = [
        (message(src, dst, way, first_send.at[k], first_recv.at[k]), goes[way], comes[way])
        for k, (src, dst, way) in enumerate((
            (tz_p, zp, Z_UP),
            (tz_q, zq, Z_DOWN),
            (p_in.at[:, :, ys - 1], yp, Y_UP),
            (q_in.at[:, :, 0], yq, Y_DOWN),
            (xs_own, xp, X_UP),
            (xs_own, xq, X_DOWN),
        ))
    ]

    def start(moves, only=None):
        for copy, there, _ in moves:
            @pl.when(there if only is None else jnp.logical_and(there, only))
            def _():
                copy.start()

    def sent(moves):
        for copy, there, _ in moves:
            @pl.when(there)
            def _():
                copy.wait_send()

    def got(moves):
        for copy, _, there in moves:
            @pl.when(there)
            def _():
                copy.wait_recv()

    empty = jnp.zeros((8, xs), jnp.float32)

    def each(low, high, body, carry):
        def turn(j, carry):
            one = list(carry)
            body(low + 2 * j, one)
            body(low + 2 * j + 1, one)
            return tuple(one)

        return lax.fori_loop(0, (high - low) // 2, turn, tuple(carry))

    def dual_block(z, b, for_p=True, for_q=True):
        r = rows(b)
        v = [bar[1 + k, z, r, :] for k in range(3)]
        p = q = None
        if for_p:
            u = bar[0, z, r, :]
            slopes = (
                next_x(u) - up_x * u,
                next_y(bar, 0, z, b, u) - up_y(b, u),
                next_z(bar, 0, z, b) - up_z(z) * u,
            )
            p = [p_out[k, z, r, :] + SIGMA * (slopes[k] - v[k]) for k in range(3)]
        if for_q:
            dx = [lo_x * v[k] - prev_x(v[k]) for k in range(3)]
            dy = [lo_y(b, v[k]) - prev_y(bar, 1 + k, z, b, v[k]) for k in range(3)]
            dz = [lo_z(z) * v[k] - prev_z(bar, 1 + k, z, b) for k in range(3)]
            q = grow_q([q_out[k, z, r, :] for k in range(6)], dx, dy, dz)
        return p, q

    def dual_inside(z, _):
        later = []
        for b in range(blocks):
            p, q = dual_block(z, b)
            later += [(p_out, (k, z, rows(b)), new) for k, new in enumerate(p)]
            later += [(q_out, (k, z, rows(b)), new) for k, new in enumerate(q)]
        flush(later)

    def dual_first():
        later = []
        for b in range(blocks):
            p, q = dual_block(zs - 1, b, for_q=False)[0], dual_block(0, b, for_p=False)[1]
            later += [(tz_p, (k, rows(b)), new) for k, new in enumerate(p)]
            later += [(tz_q, (k, rows(b)), new) for k, new in enumerate(q)]
        flush(later)

    def line_up(s):
        cv[0] = jnp.where(odd, turn_lanes(x_hi[s, 0], half_lanes - 2), x_lo[s, 0])
        cv[1] = turn_lanes(x_lo[s, 1], half_lanes)
        cv[2] = x_lo[s, 1]

    def less_q(q, x=None, y=None, z=None):
        q = list(q)
        if x is not None:
            q[XX] = q[XX] - SIGMA * x[0]
            q[XY] = q[XY] - half * x[1]
            q[XZ] = q[XZ] - half * x[2]
        if y is not None:
            q[YY] = q[YY] - SIGMA * y[1]
            q[XY] = q[XY] - half * y[0]
            q[YZ] = q[YZ] - half * y[2]
        if z is not None:
            q[ZZ] = q[ZZ] - SIGMA * z[2]
            q[XZ] = q[XZ] - half * z[0]
            q[YZ] = q[YZ] - half * z[1]
        return q

    def dual(z, s):
        later = []
        for b in range(blocks):
            r = rows(b)
            by = half_lanes - 2 * (z * blocks + b)
            from_x = [turn_lanes(cv[k], by) for k in range(3)]
            t = [p_out[k, z, r, :] for k in range(3)]
            t[0] = t[0] + SIGMA * jnp.where(last_lane, from_x[0], 0.0)
            if b == blocks - 1:
                t[1] = t[1] + SIGMA * jnp.where(last_row, y_hi[s, 0, pl.ds(z, 1), :], 0.0)
            for k in range(3):
                if z == zs - 1:
                    later.append((part_p, (k, r), t[k]))
            if z < zs - 1:
                for k, new in enumerate(shrink_p(t)):
                    later.append((p_out, (k, z, r), new))
            hx = [jnp.where(first_lane, part, 0.0) for part in from_x]
            hy = None
            if b == 0:
                hy = [jnp.where(first_row, y_lo[s, 1 + k, pl.ds(z, 1), :], 0.0) for k in range(3)]
            q = less_q([q_out[k, z, r, :] for k in range(6)], hx, hy)
            if z > 0:
                q = shrink_q(q)
            for k in range(6):
                later.append((part_q, (k, r), q[k]) if z == 0 else (q_out, (k, z, r), q[k]))
        flush(later)

    def dual_ends(s):
        later = []
        for b in range(blocks):
            r = rows(b)
            t = [part_p[k, r, :] for k in range(3)]
            t[2] = t[2] + SIGMA * z_hi[s, 0, r, :]
            for k, new in enumerate(shrink_p(t)):
                later.append((p_out, (k, zs - 1, r), new))
            q = less_q([part_q[k, r, :] for k in range(6)], z=[z_lo[s, 1 + k, r, :] for k in range(3)])
            for k, new in enumerate(shrink_q(q)):
                later.append((q_out, (k, 0, r), new))
        flush(later)

    def spread(row):
        return jnp.broadcast_to(row, (8, xs))

    def column(row, lane_of_first):
        mine = lane == lane_of_first + 2 * blocks * sub
        return jnp.sum(jnp.where(mine, spread(row), 0.0), axis=1, keepdims=True)

    where = ((0, half_lanes), (1, 0), (1, half_lanes))

    def halo_x_inside(s):
        far = pairs - blocks
        up_yc = jnp.where(jnp.logical_and(last_row, (p_pair & (blocks - 1)) == blocks - 1), factor(above[1]), 1.0)
        lo_yc = jnp.where(jnp.logical_and(first_row, (q_pair & (blocks - 1)) == 0), factor(below[1]), 1.0)
        up_zc = jnp.where(p_pair >= far, factor(above[2]), 1.0)
        lo_zc = jnp.where(q_pair < blocks, factor(below[2]), 1.0)
        u = turn_lanes(x_lo[s, 0], half_lanes)
        v = [x_lo[s, 0], turn_lanes(x_lo[s, 1], half_lanes), x_lo[s, 1]]
        own = turn_lanes(face[4], half_lanes - 1)
        moved = turn_rows(u, -1)
        turned = jnp.where((p_pair & (blocks - 1)) == blocks - 1, 0.0, turn_lanes(moved, -2))
        ahead_y = jnp.where(last_row, turned, moved)
        ahead_z = jnp.where(p_pair >= far, 0.0, turn_lanes(u, -2 * blocks))
        slopes = (own - u, ahead_y - up_yc * u, ahead_z - up_zc * u)
        for k in range(3):
            xp[k] = xp[k] + SIGMA * (slopes[k] - v[k])

        v = [turn_lanes(x_hi[s, 0], -2), turn_lanes(x_hi[s, 1], half_lanes - 2), turn_lanes(x_hi[s, 1], -2)]
        mine = [turn_lanes(face[4], -1), turn_lanes(face[5], half_lanes - 1), turn_lanes(face[5], -1)]
        dx, dy, dz = [], [], []
        for k in range(3):
            dx.append(v[k] - mine[k])
            moved = turn_rows(v[k], 1)
            turned = jnp.where((q_pair & (blocks - 1)) == 0, 0.0, turn_lanes(moved, 2))
            dy.append(lo_yc * v[k] - jnp.where(first_row, turned, moved))
            dz.append(lo_zc * v[k] - jnp.where(q_pair < blocks, 0.0, turn_lanes(v[k], 2 * blocks)))
        q = [turn_lanes(xq[k], -2) if s == 0 else xq[k] for k in range(6)]
        for k, new in enumerate(grow_q(q, dx, dy, dz)):
            xq[k] = new

    def halo_x(s):
        far = pairs - blocks
        t = [xp[k] for k in range(3)]
        edge = turn_lanes(spread(d_a[s, 0, pl.ds(0, 1), :]), half_lanes + 2 * (blocks - 1))
        here = jnp.logical_and(last_row, (p_pair & (blocks - 1)) == blocks - 1)
        t[1] = t[1] + SIGMA * jnp.where(here, edge, 0.0)
        edge = turn_lanes(d_c[s, 0], half_lanes + 2 * far)
        t[2] = t[2] + SIGMA * jnp.where(p_pair >= far, edge, 0.0)
        p = [keep(below[0], part) for part in shrink_p(t)]
        here = jnp.logical_and(first_row, (q_pair & (blocks - 1)) == 0)
        edge_y, edge_z = [], []
        for h, base in where:
            edge = turn_lanes(spread(d_b[s, h, pl.ds(7, 1), :]), half_lanes - 2 * blocks - base)
            edge_y.append(jnp.where(here, edge, 0.0))
            edge = turn_lanes(d_d[s, h], half_lanes - 2 - 2 * far - base)
            edge_z.append(jnp.where(q_pair < blocks, edge, 0.0))
        q = shrink_q(less_q([xq[k] for k in range(6)], y=edge_y, z=edge_z))
        q = [keep(above[0], part) for part in q]
        for k in range(3):
            xp[k] = p[k]
        for k in range(6):
            xq[k] = q[k]
        cp[0] = jnp.where(odd, q[XX], p[0])
        cp[1] = q[XY]
        cp[2] = q[XZ]

    def halo_y_inside(s):
        up_zr = jnp.where(last_row, factor(above[2]), 1.0)
        lo_zr = jnp.where(first_row, factor(below[2]), 1.0)
        u = y_lo[s, 0]
        slopes = (
            next_x(u) - up_x * u,
            face[0] - u,
            jnp.where(last_row, 0.0, turn_rows(u, -1)) - up_zr * u,
        )
        for k in range(3):
            yp[k] = yp[k] + SIGMA * (slopes[k] - y_lo[s, 1 + k])
        v = [y_hi[s, 1 + k] for k in range(3)]
        dx = [lo_x * v[k] - prev_x(v[k]) for k in range(3)]
        dy = [v[k] - face[7 + k] for k in range(3)]
        dz = [lo_zr * v[k] - jnp.where(first_row, 0.0, turn_rows(v[k], 1)) for k in range(3)]
        for k, new in enumerate(grow_q([yq[k] for k in range(6)], dx, dy, dz)):
            yq[k] = new

    def halo_y(s):
        t = [yp[k] for k in range(3)]
        edge = column(d_b[s, 0, pl.ds(7, 1), :], 2 * blocks - 1)
        t[0] = t[0] + SIGMA * jnp.where(last_lane, edge, 0.0)
        t[2] = t[2] + SIGMA * jnp.where(last_row, d_e[s, 0, pl.ds(0, 1), :], 0.0)
        p = shrink_p(t)
        edge_x = [
            jnp.where(first_lane, column(d_a[s, h, pl.ds(0, 1), :], base), 0.0) for h, base in where
        ]
        edge_z = [jnp.where(first_row, d_g[s, 1 + k, pl.ds(zs - 1, 1), :], 0.0) for k in range(3)]
        q = shrink_q(less_q([yq[k] for k in range(6)], x=edge_x, z=edge_z))
        for k in range(3):
            yp[k] = keep(below[1], p[k])
        for k in range(6):
            yq[k] = keep(above[1], q[k])

    def halo_z_first():
        later = []
        for b in range(blocks):
            r = rows(b)
            t = [zp[k, r, :] for k in range(3)]
            edge_x = turn_lanes(d_d[0, 0], xs - 2 - 2 * (blocks * (zs - 1) + b))
            t[0] = t[0] + SIGMA * jnp.where(last_lane, edge_x, 0.0)
            if b == blocks - 1:
                t[1] = t[1] + SIGMA * jnp.where(last_row, d_g[0, 0, pl.ds(zs - 1, 1), :], 0.0)
            t[2] = t[2] + SIGMA * bar[0, 0, r, :]
            for k, new in enumerate(shrink_p(t)):
                later.append((zp, (k, r), keep(below[2], new)))

            hx = [
                jnp.where(first_lane, turn_lanes(d_c[0, h], -base - 2 * b), 0.0) for h, base in where
            ]
            hz = [bar[1 + k, zs - 1, r, :] for k in range(3)]
            hy = None
            if b == 0:
                hy = [jnp.where(first_row, d_e[0, 1 + k, pl.ds(0, 1), :], 0.0) for k in range(3)]
            q = less_q([zq[k, r, :] for k in range(6)], hx, hy, hz)
            for k, new in enumerate(shrink_q(q)):
                later.append((zq, (k, r), keep(above[2], new)))
        flush(later)

    def halo_z(s):
        later = []
        for b in range(blocks):
            r = rows(b)
            u = z_lo[s, 0, r, :]
            edge_x = turn_lanes(d_d[s, 0], xs - 2 - 2 * (blocks * (zs - 1) + b))
            if b < blocks - 1:
                ahead_y = z_lo[s, 0, rows(b, 1), :]
            else:
                ahead_y = jnp.where(last_row, d_g[s, 0, pl.ds(zs - 1, 1), :], turn_rows(u, -1))
            slopes = (
                jnp.where(last_lane, edge_x, turn_lanes(u, -1)) - up_x * u,
                ahead_y - up_y(b, u),
                bar[0, 0, r, :] - u,
            )
            p = shrink_p([zp[k, r, :] + SIGMA * (slopes[k] - z_lo[s, 1 + k, r, :]) for k in range(3)])
            for k in range(3):
                later.append((zp, (k, r), keep(below[2], p[k])))

            v = [z_hi[s, 1 + k, r, :] for k in range(3)]
            dx, dy, dz = [], [], []
            for k, (h, base) in enumerate(where):
                edge_x = turn_lanes(d_c[s, h], -base - 2 * b)
                dx.append(lo_x * v[k] - jnp.where(first_lane, edge_x, turn_lanes(v[k], 1)))
                if b > 0:
                    behind_y = z_hi[s, 1 + k, rows(b, -1), :]
                else:
                    behind_y = jnp.where(first_row, d_e[s, 1 + k, pl.ds(0, 1), :], turn_rows(v[k], 1))
                dy.append(lo_y(b, v[k]) - behind_y)
                dz.append(v[k] - bar[1 + k, zs - 1, r, :])
            q = shrink_q(grow_q([zq[k, r, :] for k in range(6)], dx, dy, dz))
            for k in range(6):
                later.append((zq, (k, r), keep(above[2], q[k])))
        flush(later)

    def pack_plane(packed, z):
        for b in range(blocks):
            pack_bar(packed, [bar[k, z, rows(b), :] for k in range(4)], z, b)

    halo = (
        cp,
        lambda z: yp[1, pl.ds(z, 1), :],
        lambda k, z: yq[k, pl.ds(z, 1), :],
        lambda r: zp[2, r, :],
        lambda k, r: zq[k, r, :],
    )

    def primal(z):
        later = []
        for b, r, pieces in primal_plane(z, below, above, u_out, v_out, p_out, q_out, gain, offset, halo):
            for k, (new, old) in enumerate(pieces):
                later.append((u_out, (z, r), new) if k == 0 else (v_out, (k - 1, z, r), new))
                ahead = 2.0 * new - old
                later.append((bar, (k, z, r), ahead))
                if b == 0:
                    later.append((face, (k, pl.ds(z, 1)), ahead[0:1, :]))
                if b == blocks - 1:
                    later.append((face, (6 + k, pl.ds(z, 1)), ahead[7:8, :]))
        flush(later)

    def pack_dual(packed, z):
        for b in range(blocks):
            for k in range(6):
                value = q_out[k, z, rows(b), :]
                if k < 3:
                    value = jnp.where(last_lane, p_out[k, z, rows(b), :], value)
                packed[k] = pack(packed[k], value, pairs, z * blocks + b)

    def prepare(z, carry):
        weight = TAU * gain[z]
        inverse = 1.0 / (1.0 + weight)
        gain[z] = inverse
        offset[z] = weight * offset[z] * inverse
        return carry

    ends, middle = (0, zs - 1), range(1, zs - 1)
    with jax.named_scope("load_uv"):
        for load in loads[:2]:
            load.wait()
    with jax.named_scope("barrier"):
        pl.semaphore_wait(barrier, peers)
    with jax.named_scope("send_z0"):
        start(exchanges[0][:2])
        for load in loads[2:6]:
            load.wait()
        start(exchanges[0][4:6])
    with jax.named_scope("load_pq"):
        for load in loads[6:8]:
            load.wait()
        for load in loads[8:]:
            load.start()
    with jax.named_scope("first_z"):
        packed = [empty, empty]
        for z in ends:
            pack_plane(packed, z)
        dual_first()
        xe[0] = packed[0]
        xe[1] = packed[1]
        start(exchanges[0][8:])
        start(duals[:2])
    with jax.named_scope("pack_uv"):
        for z in middle:
            pack_plane(packed, z)
        face[4] = packed[0]
        face[5] = packed[1]
        start(exchanges[0][6:8])
        start(exchanges[0][2:4])
        start(duals[2:4])
    with jax.named_scope("pack_pq"):
        packed = [empty] * 6
        for z in range(zs):
            pack_dual(packed, z)
        for k in range(6):
            xs_own[k] = packed[k]
        start(duals[4:])
    with jax.named_scope("inside0"):
        each(0, zs, dual_inside, ())
    with jax.named_scope("prepare"):
        for load in loads[8:]:
            load.wait()
        lax.fori_loop(0, zs, prepare, 0)

    for s in range(ITERS):
        last = s == ITERS - 1
        moves = exchanges[s]
        if s > 0:
            with jax.named_scope(f"inside{s}"):
                each(0, zs, dual_inside, ())
        with jax.named_scope(f"wait_xy{s}"):
            got(moves[2:6])
            line_up(s)
        with jax.named_scope(f"dual_mid{s}"):
            for z in range(zs):
                dual(z, s)
            if s > 0:
                halo_x_inside(s)
                halo_y_inside(s)
        if s == 0:
            with jax.named_scope(f"wait_pq{s}"):
                got(duals[2:])
                halo_x_inside(s)
                halo_y_inside(s)
        with jax.named_scope(f"wait_diag{s}"):
            got(moves[6:])
        with jax.named_scope(f"halo_xy{s}"):
            halo_x(s)
            halo_y(s)
        with jax.named_scope(f"wait_z{s}"):
            got(moves[:2])
            sent(moves)
        if s == 0:
            with jax.named_scope(f"wait_zpq{s}"):
                got(duals[:2])
                sent(duals)
        with jax.named_scope(f"ends{s}"):
            if s == 0:
                halo_z_first()
            else:
                halo_z(s)
            dual_ends(s)
            if last:
                edge_y[0] = yp[1]
                edge_z[0] = zp[2]
                for at, k in enumerate(Y_PARTS):
                    edge_y[1 + at] = yq[k]
                for at, k in enumerate(Z_PARTS):
                    edge_z[1 + at] = zq[k]
                continue
            packed = [empty, empty]
            for z in ends:
                primal(z)
            for z in ends:
                pack_plane(packed, z)
            xe[0] = packed[0]
            xe[1] = packed[1]
        with jax.named_scope(f"send_z{s}"):
            start(exchanges[s + 1][8:])
            start(exchanges[s + 1][:2])
        with jax.named_scope(f"primal_mid{s}"):
            for z in middle:
                primal(z)
            for z in middle:
                pack_plane(packed, z)
            face[4] = packed[0]
            face[5] = packed[1]
        with jax.named_scope(f"send{s}"):
            start(exchanges[s + 1][6:8])
            start(exchanges[s + 1][2:6])


def last_primal(
    u_in, v_in, p_in, q_in, gain, offset, cp, edge_y, edge_z,
    u_out, v_out, p_out, q_out,
    u_new, v_new, sems,
):
    zs, ys, xs = u_in.shape
    place = [lax.axis_index(a) for a in AXES]
    count = [lax.axis_size(a) for a in AXES]
    below = [place[i] > 0 for i in range(3)]
    above = [place[i] < count[i] - 1 for i in range(3)]
    copies = [pltpu.make_async_copy(q_in.at[k], q_out.at[k], sems.at[k]) for k in range(6)]
    copies += [pltpu.make_async_copy(p_in.at[k], p_out.at[k], sems.at[6 + k]) for k in range(3)]
    for copy in copies:
        copy.start()
    halo = (
        cp,
        lambda z: edge_y[0, pl.ds(z, 1), :],
        lambda k, z: edge_y[1 + Y_PARTS.index(k), pl.ds(z, 1), :],
        lambda r: edge_z[0, r, :],
        lambda k, r: edge_z[1 + Z_PARTS.index(k), r, :],
    )
    for z in range(zs):
        for _, r, pieces in primal_plane(z, below, above, u_in, v_in, p_in, q_in, gain, offset, halo):
            u_new[z, r, :] = pieces[0][0]
            for k in range(3):
                v_new[k, z, r, :] = pieces[1 + k][0]
        if z % 2 == 1:
            two = pl.ds(z - 1, 2)
            mine = [
                pltpu.make_async_copy(v_new.at[:, two], v_out.at[:, two], sems.at[9 + z - 1]),
                pltpu.make_async_copy(u_new.at[two], u_out.at[two], sems.at[9 + z]),
            ]
            for copy in mine:
                copy.start()
            copies += mine
    for copy in copies:
        copy.wait()


def per_device(noisy_image, fidelity, primal_u, primal_v, dual_p, dual_q):
    zs, ys, xs = primal_u.shape
    blocks = ys // 8
    assert zs == 8 and ys % 8 == 0 and blocks & (blocks - 1) == 0 and 4 * zs * blocks == xs == 128
    f32 = jnp.float32

    def vmem(*shape):
        return pltpu.VMEM(shape, f32)

    shapes = [a.shape for a in (primal_u, primal_v, dual_p, dual_q)]
    kept = shapes + [(zs, ys, xs), (zs, ys, xs), (3, 8, xs), (4, 8, xs), (4, ys, xs)]
    results = pl.pallas_call(
        kernel,
        out_shape=tuple(vmem(*shape) for shape in kept),
        in_specs=[pl.BlockSpec(memory_space=pl.ANY)] * 6,
        out_specs=tuple([pl.BlockSpec(memory_space=pltpu.VMEM)] * len(kept)),
        scratch_shapes=[
            vmem(4, zs, ys, xs),
            vmem(10, 8, xs),
            vmem(ITERS, 4, ys, xs),
            vmem(ITERS, 4, ys, xs),
            vmem(ITERS, 2, 8, xs),
            vmem(ITERS, 2, 8, xs),
            vmem(ITERS, 4, 8, xs),
            vmem(ITERS, 4, 8, xs),
            vmem(ITERS, 2, 8, xs),
            vmem(ITERS, 2, 8, xs),
            vmem(ITERS, 2, 8, xs),
            vmem(ITERS, 2, 8, xs),
            vmem(ITERS, 4, 8, xs),
            vmem(ITERS, 4, 8, xs),
            vmem(3, ys, xs),
            vmem(6, ys, xs),
            vmem(3, 8, xs),
            vmem(6, 8, xs),
            vmem(6, 8, xs),
            vmem(6, 8, xs),
            vmem(6, 8, xs),
            vmem(3, 8, xs),
            vmem(2, 8, xs),
            vmem(3, ys, xs),
            vmem(6, ys, xs),
            vmem(3, ys, xs),
            vmem(6, ys, xs),
            pltpu.SemaphoreType.DMA((12,)),
            pltpu.SemaphoreType.DMA((ITERS, 12)),
            pltpu.SemaphoreType.DMA((ITERS, 12)),
            pltpu.SemaphoreType.DMA((6,)),
            pltpu.SemaphoreType.DMA((6,)),
        ],
        compiler_params=pltpu.CompilerParams(collective_id=0, has_side_effects=True),
        name="tgv",
    )(noisy_image, fidelity, primal_u, primal_v, dual_p, dual_q)
    return pl.pallas_call(
        last_primal,
        out_shape=tuple(jax.ShapeDtypeStruct(shape, f32) for shape in shapes),
        in_specs=[pl.BlockSpec(memory_space=pltpu.VMEM)] * len(kept),
        out_specs=tuple([pl.BlockSpec(memory_space=pl.ANY)] * 4),
        scratch_shapes=[
            vmem(zs, ys, xs),
            vmem(3, zs, ys, xs),
            pltpu.SemaphoreType.DMA((9 + zs,)),
        ],
        name="out",
    )(*[pltpu.with_memory_space_constraint(r, pltpu.VMEM) for r in results])


def solution(mesh):
    scalar, stack = P("gz", "gy", "gx"), P(None, "gz", "gy", "gx")
    return jax.shard_map(
        per_device,
        mesh=mesh,
        in_specs=(scalar, scalar, scalar, stack, stack, stack),
        out_specs=(scalar, stack, stack, stack),
        check_vma=False,
    )
```

```python
import jax
import jax.numpy as jnp
from jax import lax
from jax.experimental import pallas as pl
from jax.experimental.pallas import tpu as pltpu
from jax.sharding import PartitionSpec as P

ITERS = 3
AXES = ("gx", "gy", "gz")
ALPHA1, ALPHA0, SIGMA, TAU = 0.5, 1.0, 0.2, 0.2
XX, YY, ZZ, XY, XZ, YZ = range(6)
PARTS = ((XX, XY, XZ), (XY, YY, YZ), (XZ, YZ, ZZ))
Y_PARTS, Z_PARTS = (XY, YY, YZ), (XZ, YZ, ZZ)
MESH = pl.DeviceIdType.MESH
Z_UP, Z_DOWN, X_UP, X_DOWN, Y_UP, Y_DOWN, XY_A, XY_B, XZ_A, XZ_B, YZ_A, YZ_B = range(12)
WAYS = (
    (0, 0, 1), (0, 0, -1), (1, 0, 0), (-1, 0, 0), (0, 1, 0), (0, -1, 0),
    (1, -1, 0), (-1, 1, 0), (1, 0, -1), (-1, 0, 1), (0, 1, -1), (0, -1, 1),
)


def primal_plane(z, below, above, u_ref, v_ref, p_ref, q_ref, gain, offset, halo, only=None):
    zs, ys, xs = u_ref.shape
    blocks = ys // 8
    cp, row_p, row_q, plane_p, plane_q = halo
    lane = lax.broadcasted_iota(jnp.int32, (8, xs), 1)
    sub = lax.broadcasted_iota(jnp.int32, (8, xs), 0)
    first_lane, last_lane = lane == 0, lane == xs - 1
    first_row, last_row = sub == 0, sub == 7

    def factor(flag):
        return jnp.where(flag, jnp.float32(1), jnp.float32(0))

    up_x = jnp.where(last_lane, factor(above[0]), 1.0)
    lo_x = jnp.where(first_lane, factor(below[0]), 1.0)
    up_z = factor(above[2]) if z == zs - 1 else 1.0
    lo_z = factor(below[2]) if z == 0 else 1.0
    for b in range(blocks) if only is None else only:
        r = pl.ds(8 * b, 8)
        up_y = jnp.where(last_row, factor(above[1]), 1.0) if b == blocks - 1 else 1.0
        lo_y = jnp.where(first_row, factor(below[1]), 1.0) if b == 0 else 1.0
        by = xs // 2 - 2 * (z * blocks + b)
        from_x = [pltpu.roll(cp[k], by, 1) for k in range(3)]
        p = [p_ref[k, z, r, :] for k in range(3)]
        q = [q_ref[k, z, r, :] for k in range(6)]
        before_x = jnp.where(first_lane, from_x[0], pltpu.roll(p[0], 1, 1))
        if b > 0:
            before_y = p_ref[1, z, pl.ds(8 * b - 1, 8), :]
        else:
            before_y = jnp.where(first_row, row_p(z), pltpu.roll(p[1], 1, 0))
        before_z = plane_p(r) if z == 0 else p_ref[2, z - 1, r, :]
        div = (up_x * p[0] - before_x) + (up_y * p[1] - before_y) + (up_z * p[2] - before_z)
        old = u_ref[z, r, :]
        pieces = [((old + TAU * div) * gain[z, r, :] + offset[z, r, :], old)]
        for k, (ax, ay, az) in enumerate(PARTS):
            after_x = jnp.where(last_lane, from_x[k], pltpu.roll(q[ax], xs - 1, 1))
            if b < blocks - 1:
                after_y = q_ref[ay, z, pl.ds(8 * b + 1, 8), :]
            else:
                after_y = jnp.where(last_row, row_q(ay, z), pltpu.roll(q[ay], 7, 0))
            after_z = plane_q(az, r) if z == zs - 1 else q_ref[az, z + 1, r, :]
            div2 = (after_x - lo_x * q[ax]) + (after_y - lo_y * q[ay]) + (after_z - lo_z * q[az])
            old = v_ref[k, z, r, :]
            pieces.append((old + TAU * (p[k] + div2), old))
        yield b, r, pieces


def kernel(
    noisy_in, fid_in, u_in, v_in, p_in, q_in,
    u_out, v_out, p_out, q_out, gain, offset, cp, edge_y, edge_z,
    bar, face,
    z_lo, z_hi, x_lo, x_hi, y_lo, y_hi, d_a, d_b, d_c, d_d, d_e, d_g,
    zp, zq, yp, yq, xs_own, xp, xq, cv, xe, part_p, part_q, tz_p, tz_q,
    load_sem, send_sem, recv_sem, first_send, first_recv,
):
    zs, ys, xs = u_in.shape
    blocks = ys // 8
    pairs = zs * blocks
    half_lanes = 2 * pairs
    place = [lax.axis_index(a) for a in AXES]
    count = [lax.axis_size(a) for a in AXES]
    below = [place[i] > 0 for i in range(3)]
    above = [place[i] < count[i] - 1 for i in range(3)]


    def exists(way):
        there = None
        for i, by in enumerate(way):
            if by:
                one = above[i] if by > 0 else below[i]
                there = one if there is None else jnp.logical_and(there, one)
        return there

    def target(way):
        return {AXES[i]: place[i] + by for i, by in enumerate(way) if by}

    goes = [exists(way) for way in WAYS]
    comes = [exists(tuple(-by for by in way)) for way in WAYS]
    peers = sum(there.astype(jnp.int32) for there in goes)

    u_face, xf, top_face = pl.ds(0, 4), pl.ds(4, 2), pl.ds(6, 4)
    loads = [
        pltpu.make_async_copy(u_in, bar.at[0], load_sem.at[0]),
        pltpu.make_async_copy(v_in, bar.at[pl.ds(1, 3)], load_sem.at[1]),
        pltpu.make_async_copy(u_in.at[:, 0], face.at[0], load_sem.at[2]),
        pltpu.make_async_copy(v_in.at[:, :, 0], face.at[pl.ds(1, 3)], load_sem.at[3]),
        pltpu.make_async_copy(u_in.at[:, ys - 1], face.at[6], load_sem.at[4]),
        pltpu.make_async_copy(v_in.at[:, :, ys - 1], face.at[pl.ds(7, 3)], load_sem.at[5]),
        pltpu.make_async_copy(q_in, q_out, load_sem.at[6]),
        pltpu.make_async_copy(p_in, p_out, load_sem.at[7]),
        pltpu.make_async_copy(noisy_in, offset, load_sem.at[8]),
        pltpu.make_async_copy(fid_in, gain, load_sem.at[9]),
        pltpu.make_async_copy(u_in, u_out, load_sem.at[10]),
        pltpu.make_async_copy(v_in, v_out, load_sem.at[11]),
    ]
    for load in loads[:2]:
        load.start()

    barrier = pltpu.get_barrier_semaphore()
    for way, there in zip(WAYS, goes):
        @pl.when(there)
        def _():
            pl.semaphore_signal(barrier, inc=1, device_id=target(way), device_id_type=MESH)

    for load in loads[2:8]:
        load.start()

    def clear(there, *refs):
        @pl.when(jnp.logical_not(there))
        def _():
            for ref in refs:
                ref[...] = jnp.zeros(ref.shape, jnp.float32)

    clear(below[0], x_lo, xp)
    clear(above[0], x_hi, xq)
    clear(below[1], y_lo, yp)
    clear(above[1], y_hi, yq)
    clear(below[2], z_lo, zp)
    clear(above[2], z_hi, zq)
    for way, ref in zip(WAYS[6:], (d_a, d_b, d_c, d_d, d_e, d_g)):
        clear(exists(tuple(-by for by in way)), ref)

    lane = lax.broadcasted_iota(jnp.int32, (8, xs), 1)
    sub = lax.broadcasted_iota(jnp.int32, (8, xs), 0)
    pair = lane >> 1
    odd = (lane & 1) == 1
    first_lane, last_lane = lane == 0, lane == xs - 1
    first_row, last_row = sub == 0, sub == 7
    p_pair, q_pair = (lane - half_lanes) >> 1, (lane + 1 - half_lanes) >> 1

    def factor(flag):
        return jnp.where(flag, jnp.float32(1), jnp.float32(0))

    up_x = jnp.where(last_lane, factor(above[0]), 1.0)
    lo_x = jnp.where(first_lane, factor(below[0]), 1.0)
    up_y_last = jnp.where(last_row, factor(above[1]), 1.0)
    lo_y_first = jnp.where(first_row, factor(below[1]), 1.0)

    def rows(b, by=0):
        return pl.ds(8 * b + by, 8)

    def turn_lanes(value, by):
        return value if isinstance(by, int) and by % xs == 0 else pltpu.roll(value, by % xs if isinstance(by, int) else by, 1)

    def turn_rows(value, by):
        return pltpu.roll(value, by % 8, 0)

    def flush(later):
        for ref, at, value in later:
            ref[at + (slice(None),)] = value
        later.clear()

    def up_z(z):
        return factor(jnp.logical_or(z < zs - 1, above[2]))

    def lo_z(z):
        return factor(jnp.logical_or(z > 0, below[2]))

    def up_y(b, value):
        return up_y_last * value if b == blocks - 1 else value

    def lo_y(b, value):
        return lo_y_first * value if b == 0 else value

    def next_x(value):
        return jnp.where(last_lane, 0.0, pltpu.roll(value, xs - 1, 1))

    def prev_x(value):
        return jnp.where(first_lane, 0.0, pltpu.roll(value, 1, 1))

    def next_y(ref, k, z, b, value):
        if b < blocks - 1:
            return ref[k, z, rows(b, 1), :]
        return jnp.where(last_row, 0.0, pltpu.roll(value, 7, 0))

    def prev_y(ref, k, z, b, value):
        if b > 0:
            return ref[k, z, rows(b, -1), :]
        return jnp.where(first_row, 0.0, pltpu.roll(value, 1, 0))

    def next_z(ref, k, z, b):
        if isinstance(z, int):
            return ref[k, z + 1, rows(b), :] if z < zs - 1 else jnp.zeros((8, xs), jnp.float32)
        return factor(z < zs - 1) * ref[k, jnp.minimum(z + 1, zs - 1), rows(b), :]

    def prev_z(ref, k, z, b):
        if isinstance(z, int):
            return ref[k, z - 1, rows(b), :] if z > 0 else jnp.zeros((8, xs), jnp.float32)
        return factor(z > 0) * ref[k, jnp.maximum(z - 1, 0), rows(b), :]

    def shrink_p(t):
        size = t[0] * t[0] + t[1] * t[1] + t[2] * t[2]
        scale = jnp.minimum(1.0, ALPHA1 * lax.rsqrt(size))
        return [scale * part for part in t]

    def shrink_q(s):
        size = (s[XX] * s[XX] + s[YY] * s[YY] + s[ZZ] * s[ZZ]) + 2.0 * (
            s[XY] * s[XY] + s[XZ] * s[XZ] + s[YZ] * s[YZ]
        )
        scale = jnp.minimum(1.0, ALPHA0 * lax.rsqrt(size))
        return [scale * part for part in s]

    half = 0.5 * SIGMA

    def grow_q(q, dx, dy, dz):
        return [
            q[XX] + SIGMA * dx[0], q[YY] + SIGMA * dy[1], q[ZZ] + SIGMA * dz[2],
            q[XY] + half * (dy[0] + dx[1]), q[XZ] + half * (dz[0] + dx[2]),
            q[YZ] + half * (dz[1] + dy[2]),
        ]

    def keep(flag, value):
        return jnp.where(flag, value, 0.0)

    def pack(packed, value, base, j):
        return jnp.where(pair == base + j, pltpu.roll(value, 2 * (base + j) + 1, 1), packed)

    def pack_bar(packed, values, z, b):
        j = z * blocks + b
        packed[0] = pack(packed[0], values[0], 0, j)
        packed[0] = pack(packed[0], values[1], pairs, j)
        packed[1] = pack(packed[1], values[2], 0, j)
        packed[1] = pack(packed[1], values[3], pairs, j)

    def message(src, dst, way, send, recv):
        return pltpu.make_async_remote_copy(
            src_ref=src, dst_ref=dst, send_sem=send, recv_sem=recv,
            device_id=target(WAYS[way]), device_id_type=MESH,
        )

    ahead_rows, early = ys - 8, 8 * (blocks // 2)
    exchanges = []
    for s in range(ITERS):
        z_up_part = pl.ds(1, 3) if s == 0 else pl.ds(0, 4)
        z_down_part = pl.ds(0, 1) if s == 0 else pl.ds(0, 4)
        z_rows = pl.ds(early, ys - early) if s == 1 else pl.ds(0, ys)
        ends = (
            (bar.at[z_up_part, zs - 1, z_rows], z_lo.at[s, z_up_part, z_rows]),
            (bar.at[z_down_part, 0, z_rows], z_hi.at[s, z_down_part, z_rows]),
            (face.at[xf], x_lo.at[s]),
            (face.at[xf], x_hi.at[s]),
            (face.at[top_face], y_lo.at[s]),
            (face.at[u_face], y_hi.at[s]),
            (face.at[xf, pl.ds(0, 1)], d_a.at[s, :, pl.ds(0, 1)]),
            (face.at[xf, pl.ds(7, 1)], d_b.at[s, :, pl.ds(7, 1)]),
            (xe, d_c.at[s]),
            (xe, d_d.at[s]),
            (face.at[top_face, pl.ds(0, 1)], d_e.at[s, :, pl.ds(0, 1)]),
            (face.at[u_face, pl.ds(zs - 1, 1)], d_g.at[s, :, pl.ds(zs - 1, 1)]),
        )
        exchanges.append([
            (message(src, dst, k, send_sem.at[s, k], recv_sem.at[s, k]), goes[k], comes[k])
            for k, (src, dst) in enumerate(ends)
        ])
    duals = [
        (message(src, dst, way, first_send.at[k], first_recv.at[k]), goes[way], comes[way])
        for k, (src, dst, way) in enumerate((
            (tz_p.at[:, pl.ds(0, ahead_rows)], zp.at[:, pl.ds(0, ahead_rows)], Z_UP),
            (tz_q.at[:, pl.ds(0, ahead_rows)], zq.at[:, pl.ds(0, ahead_rows)], Z_DOWN),
            (p_in.at[:, :, ys - 1], yp, Y_UP),
            (q_in.at[:, :, 0], yq, Y_DOWN),
            (xs_own, xp, X_UP),
            (xs_own, xq, X_DOWN),
            (tz_p.at[:, pl.ds(ahead_rows, 8)], zp.at[:, pl.ds(ahead_rows, 8)], Z_UP),
            (tz_q.at[:, pl.ds(ahead_rows, 8)], zq.at[:, pl.ds(ahead_rows, 8)], Z_DOWN),
            (bar.at[:, zs - 1, pl.ds(0, early)], z_lo.at[1, :, pl.ds(0, early)], Z_UP),
            (bar.at[:, 0, pl.ds(0, early)], z_hi.at[1, :, pl.ds(0, early)], Z_DOWN),
        ))
    ]

    def start(moves, only=None):
        for copy, there, _ in moves:
            @pl.when(there if only is None else jnp.logical_and(there, only))
            def _():
                copy.start()

    def sent(moves):
        for copy, there, _ in moves:
            @pl.when(there)
            def _():
                copy.wait_send()

    def got(moves):
        for copy, _, there in moves:
            @pl.when(there)
            def _():
                copy.wait_recv()

    empty = jnp.zeros((8, xs), jnp.float32)

    def each(low, high, body, carry):
        def turn(j, carry):
            one = list(carry)
            body(low + 2 * j, one)
            body(low + 2 * j + 1, one)
            return tuple(one)

        return lax.fori_loop(0, (high - low) // 2, turn, tuple(carry))

    def dual_block(z, b, for_p=True, for_q=True):
        r = rows(b)
        v = [bar[1 + k, z, r, :] for k in range(3)]
        p = q = None
        if for_p:
            u = bar[0, z, r, :]
            slopes = (
                next_x(u) - up_x * u,
                next_y(bar, 0, z, b, u) - up_y(b, u),
                next_z(bar, 0, z, b) - up_z(z) * u,
            )
            p = [p_out[k, z, r, :] + SIGMA * (slopes[k] - v[k]) for k in range(3)]
        if for_q:
            dx = [lo_x * v[k] - prev_x(v[k]) for k in range(3)]
            dy = [lo_y(b, v[k]) - prev_y(bar, 1 + k, z, b, v[k]) for k in range(3)]
            dz = [lo_z(z) * v[k] - prev_z(bar, 1 + k, z, b) for k in range(3)]
            q = grow_q([q_out[k, z, r, :] for k in range(6)], dx, dy, dz)
        return p, q

    def dual_inside(z, _):
        later = []
        for b in range(blocks):
            p, q = dual_block(z, b)
            later += [(p_out, (k, z, rows(b)), new) for k, new in enumerate(p)]
            later += [(q_out, (k, z, rows(b)), new) for k, new in enumerate(q)]
        flush(later)

    def dual_first():
        later = []
        for b in range(blocks):
            p, q = dual_block(zs - 1, b, for_q=False)[0], dual_block(0, b, for_p=False)[1]
            later += [(tz_p, (k, rows(b)), new) for k, new in enumerate(p)]
            later += [(tz_q, (k, rows(b)), new) for k, new in enumerate(q)]
        flush(later)

    def line_up(s):
        cv[0] = jnp.where(odd, turn_lanes(x_hi[s, 0], half_lanes - 2), x_lo[s, 0])
        cv[1] = turn_lanes(x_lo[s, 1], half_lanes)
        cv[2] = x_lo[s, 1]

    def less_q(q, x=None, y=None, z=None):
        q = list(q)
        if x is not None:
            q[XX] = q[XX] - SIGMA * x[0]
            q[XY] = q[XY] - half * x[1]
            q[XZ] = q[XZ] - half * x[2]
        if y is not None:
            q[YY] = q[YY] - SIGMA * y[1]
            q[XY] = q[XY] - half * y[0]
            q[YZ] = q[YZ] - half * y[2]
        if z is not None:
            q[ZZ] = q[ZZ] - SIGMA * z[2]
            q[XZ] = q[XZ] - half * z[0]
            q[YZ] = q[YZ] - half * z[1]
        return q

    def dual(z, s):
        later = []
        for b in range(blocks):
            r = rows(b)
            by = half_lanes - 2 * (z * blocks + b)
            from_x = [turn_lanes(cv[k], by) for k in range(3)]
            t = [p_out[k, z, r, :] for k in range(3)]
            t[0] = t[0] + SIGMA * jnp.where(last_lane, from_x[0], 0.0)
            if b == blocks - 1:
                t[1] = t[1] + SIGMA * jnp.where(last_row, y_hi[s, 0, pl.ds(z, 1), :], 0.0)
            for k in range(3):
                if z == zs - 1:
                    later.append((part_p, (k, r), t[k]))
            if z < zs - 1:
                for k, new in enumerate(shrink_p(t)):
                    later.append((p_out, (k, z, r), new))
            hx = [jnp.where(first_lane, part, 0.0) for part in from_x]
            hy = None
            if b == 0:
                hy = [jnp.where(first_row, y_lo[s, 1 + k, pl.ds(z, 1), :], 0.0) for k in range(3)]
            q = less_q([q_out[k, z, r, :] for k in range(6)], hx, hy)
            if z > 0:
                q = shrink_q(q)
            for k in range(6):
                later.append((part_q, (k, r), q[k]) if z == 0 else (q_out, (k, z, r), q[k]))
        flush(later)

    def dual_ends(s, only=range(blocks)):
        later = []
        for b in only:
            r = rows(b)
            t = [part_p[k, r, :] for k in range(3)]
            t[2] = t[2] + SIGMA * z_hi[s, 0, r, :]
            for k, new in enumerate(shrink_p(t)):
                later.append((p_out, (k, zs - 1, r), new))
            q = less_q([part_q[k, r, :] for k in range(6)], z=[z_lo[s, 1 + k, r, :] for k in range(3)])
            for k, new in enumerate(shrink_q(q)):
                later.append((q_out, (k, 0, r), new))
        flush(later)

    def spread(row):
        return jnp.broadcast_to(row, (8, xs))

    def column(row, lane_of_first):
        mine = lane == lane_of_first + 2 * blocks * sub
        return jnp.sum(jnp.where(mine, spread(row), 0.0), axis=1, keepdims=True)

    where = ((0, half_lanes), (1, 0), (1, half_lanes))

    def halo_x_inside(s):
        far = pairs - blocks
        up_yc = jnp.where(jnp.logical_and(last_row, (p_pair & (blocks - 1)) == blocks - 1), factor(above[1]), 1.0)
        lo_yc = jnp.where(jnp.logical_and(first_row, (q_pair & (blocks - 1)) == 0), factor(below[1]), 1.0)
        up_zc = jnp.where(p_pair >= far, factor(above[2]), 1.0)
        lo_zc = jnp.where(q_pair < blocks, factor(below[2]), 1.0)
        u = turn_lanes(x_lo[s, 0], half_lanes)
        v = [x_lo[s, 0], turn_lanes(x_lo[s, 1], half_lanes), x_lo[s, 1]]
        own = turn_lanes(face[4], half_lanes - 1)
        moved = turn_rows(u, -1)
        turned = jnp.where((p_pair & (blocks - 1)) == blocks - 1, 0.0, turn_lanes(moved, -2))
        ahead_y = jnp.where(last_row, turned, moved)
        ahead_z = jnp.where(p_pair >= far, 0.0, turn_lanes(u, -2 * blocks))
        slopes = (own - u, ahead_y - up_yc * u, ahead_z - up_zc * u)
        for k in range(3):
            xp[k] = xp[k] + SIGMA * (slopes[k] - v[k])

        v = [turn_lanes(x_hi[s, 0], -2), turn_lanes(x_hi[s, 1], half_lanes - 2), turn_lanes(x_hi[s, 1], -2)]
        mine = [turn_lanes(face[4], -1), turn_lanes(face[5], half_lanes - 1), turn_lanes(face[5], -1)]
        dx, dy, dz = [], [], []
        for k in range(3):
            dx.append(v[k] - mine[k])
            moved = turn_rows(v[k], 1)
            turned = jnp.where((q_pair & (blocks - 1)) == 0, 0.0, turn_lanes(moved, 2))
            dy.append(lo_yc * v[k] - jnp.where(first_row, turned, moved))
            dz.append(lo_zc * v[k] - jnp.where(q_pair < blocks, 0.0, turn_lanes(v[k], 2 * blocks)))
        q = [turn_lanes(xq[k], -2) if s == 0 else xq[k] for k in range(6)]
        for k, new in enumerate(grow_q(q, dx, dy, dz)):
            xq[k] = new

    def halo_x(s):
        far = pairs - blocks
        t = [xp[k] for k in range(3)]
        edge = turn_lanes(spread(d_a[s, 0, pl.ds(0, 1), :]), half_lanes + 2 * (blocks - 1))
        here = jnp.logical_and(last_row, (p_pair & (blocks - 1)) == blocks - 1)
        t[1] = t[1] + SIGMA * jnp.where(here, edge, 0.0)
        edge = turn_lanes(d_c[s, 0], half_lanes + 2 * far)
        t[2] = t[2] + SIGMA * jnp.where(p_pair >= far, edge, 0.0)
        p = [keep(below[0], part) for part in shrink_p(t)]
        here = jnp.logical_and(first_row, (q_pair & (blocks - 1)) == 0)
        edge_y, edge_z = [], []
        for h, base in where:
            edge = turn_lanes(spread(d_b[s, h, pl.ds(7, 1), :]), half_lanes - 2 * blocks - base)
            edge_y.append(jnp.where(here, edge, 0.0))
            edge = turn_lanes(d_d[s, h], half_lanes - 2 - 2 * far - base)
            edge_z.append(jnp.where(q_pair < blocks, edge, 0.0))
        q = shrink_q(less_q([xq[k] for k in range(6)], y=edge_y, z=edge_z))
        q = [keep(above[0], part) for part in q]
        for k in range(3):
            xp[k] = p[k]
        for k in range(6):
            xq[k] = q[k]
        cp[0] = jnp.where(odd, q[XX], p[0])
        cp[1] = q[XY]
        cp[2] = q[XZ]

    def halo_y_inside(s):
        up_zr = jnp.where(last_row, factor(above[2]), 1.0)
        lo_zr = jnp.where(first_row, factor(below[2]), 1.0)
        u = y_lo[s, 0]
        slopes = (
            next_x(u) - up_x * u,
            face[0] - u,
            jnp.where(last_row, 0.0, turn_rows(u, -1)) - up_zr * u,
        )
        for k in range(3):
            yp[k] = yp[k] + SIGMA * (slopes[k] - y_lo[s, 1 + k])
        v = [y_hi[s, 1 + k] for k in range(3)]
        dx = [lo_x * v[k] - prev_x(v[k]) for k in range(3)]
        dy = [v[k] - face[7 + k] for k in range(3)]
        dz = [lo_zr * v[k] - jnp.where(first_row, 0.0, turn_rows(v[k], 1)) for k in range(3)]
        for k, new in enumerate(grow_q([yq[k] for k in range(6)], dx, dy, dz)):
            yq[k] = new

    def halo_y(s):
        t = [yp[k] for k in range(3)]
        edge = column(d_b[s, 0, pl.ds(7, 1), :], 2 * blocks - 1)
        t[0] = t[0] + SIGMA * jnp.where(last_lane, edge, 0.0)
        t[2] = t[2] + SIGMA * jnp.where(last_row, d_e[s, 0, pl.ds(0, 1), :], 0.0)
        p = shrink_p(t)
        edge_x = [
            jnp.where(first_lane, column(d_a[s, h, pl.ds(0, 1), :], base), 0.0) for h, base in where
        ]
        edge_z = [jnp.where(first_row, d_g[s, 1 + k, pl.ds(zs - 1, 1), :], 0.0) for k in range(3)]
        q = shrink_q(less_q([yq[k] for k in range(6)], x=edge_x, z=edge_z))
        for k in range(3):
            yp[k] = keep(below[1], p[k])
        for k in range(6):
            yq[k] = keep(above[1], q[k])

    def halo_z_first(only):
        later = []
        for b in only:
            r = rows(b)
            t = [zp[k, r, :] for k in range(3)]
            edge_x = turn_lanes(d_d[0, 0], xs - 2 - 2 * (blocks * (zs - 1) + b))
            t[0] = t[0] + SIGMA * jnp.where(last_lane, edge_x, 0.0)
            if b == blocks - 1:
                t[1] = t[1] + SIGMA * jnp.where(last_row, d_g[0, 0, pl.ds(zs - 1, 1), :], 0.0)
            t[2] = t[2] + SIGMA * bar[0, 0, r, :]
            for k, new in enumerate(shrink_p(t)):
                later.append((zp, (k, r), keep(below[2], new)))

            hx = [
                jnp.where(first_lane, turn_lanes(d_c[0, h], -base - 2 * b), 0.0) for h, base in where
            ]
            hz = [bar[1 + k, zs - 1, r, :] for k in range(3)]
            hy = None
            if b == 0:
                hy = [jnp.where(first_row, d_e[0, 1 + k, pl.ds(0, 1), :], 0.0) for k in range(3)]
            q = less_q([zq[k, r, :] for k in range(6)], hx, hy, hz)
            for k, new in enumerate(shrink_q(q)):
                later.append((zq, (k, r), keep(above[2], new)))
        flush(later)

    def halo_z(s):
        later = []
        for b in range(blocks):
            r = rows(b)
            u = z_lo[s, 0, r, :]
            edge_x = turn_lanes(d_d[s, 0], xs - 2 - 2 * (blocks * (zs - 1) + b))
            if b < blocks - 1:
                ahead_y = z_lo[s, 0, rows(b, 1), :]
            else:
                ahead_y = jnp.where(last_row, d_g[s, 0, pl.ds(zs - 1, 1), :], turn_rows(u, -1))
            slopes = (
                jnp.where(last_lane, edge_x, turn_lanes(u, -1)) - up_x * u,
                ahead_y - up_y(b, u),
                bar[0, 0, r, :] - u,
            )
            p = shrink_p([zp[k, r, :] + SIGMA * (slopes[k] - z_lo[s, 1 + k, r, :]) for k in range(3)])
            for k in range(3):
                later.append((zp, (k, r), keep(below[2], p[k])))

            v = [z_hi[s, 1 + k, r, :] for k in range(3)]
            dx, dy, dz = [], [], []
            for k, (h, base) in enumerate(where):
                edge_x = turn_lanes(d_c[s, h], -base - 2 * b)
                dx.append(lo_x * v[k] - jnp.where(first_lane, edge_x, turn_lanes(v[k], 1)))
                if b > 0:
                    behind_y = z_hi[s, 1 + k, rows(b, -1), :]
                else:
                    behind_y = jnp.where(first_row, d_e[s, 1 + k, pl.ds(0, 1), :], turn_rows(v[k], 1))
                dy.append(lo_y(b, v[k]) - behind_y)
                dz.append(v[k] - bar[1 + k, zs - 1, r, :])
            q = shrink_q(grow_q([zq[k, r, :] for k in range(6)], dx, dy, dz))
            for k in range(6):
                later.append((zq, (k, r), keep(above[2], q[k])))
        flush(later)

    def pack_plane(packed, z):
        for b in range(blocks):
            pack_bar(packed, [bar[k, z, rows(b), :] for k in range(4)], z, b)

    halo = (
        cp,
        lambda z: yp[1, pl.ds(z, 1), :],
        lambda k, z: yq[k, pl.ds(z, 1), :],
        lambda r: zp[2, r, :],
        lambda k, r: zq[k, r, :],
    )

    def primal(z, only=None):
        later = []
        for b, r, pieces in primal_plane(z, below, above, u_out, v_out, p_out, q_out, gain, offset, halo, only):
            for k, (new, old) in enumerate(pieces):
                later.append((u_out, (z, r), new) if k == 0 else (v_out, (k - 1, z, r), new))
                ahead = 2.0 * new - old
                later.append((bar, (k, z, r), ahead))
                if b == 0:
                    later.append((face, (k, pl.ds(z, 1)), ahead[0:1, :]))
                if b == blocks - 1:
                    later.append((face, (6 + k, pl.ds(z, 1)), ahead[7:8, :]))
        flush(later)

    def pack_dual(packed, z):
        for b in range(blocks):
            for k in range(6):
                value = q_out[k, z, rows(b), :]
                if k < 3:
                    value = jnp.where(last_lane, p_out[k, z, rows(b), :], value)
                packed[k] = pack(packed[k], value, pairs, z * blocks + b)

    def prepare(z, carry):
        weight = TAU * gain[z]
        inverse = 1.0 / (1.0 + weight)
        gain[z] = inverse
        offset[z] = weight * offset[z] * inverse
        return carry

    ends, middle = (0, zs - 1), range(1, zs - 1)
    with jax.named_scope("load_uv"):
        for load in loads[:2]:
            load.wait()
    with jax.named_scope("barrier"):
        pl.semaphore_wait(barrier, peers)
    with jax.named_scope("send_z0"):
        start(exchanges[0][:2])
        for load in loads[2:6]:
            load.wait()
        start(exchanges[0][4:6])
    with jax.named_scope("load_pq"):
        for load in loads[6:8]:
            load.wait()
        for load in loads[8:]:
            load.start()
    with jax.named_scope("first_z"):
        packed = [empty, empty]
        for z in ends:
            pack_plane(packed, z)
        dual_first()
        xe[0] = packed[0]
        xe[1] = packed[1]
        start(exchanges[0][8:])
        start(duals[:2])
        start(duals[6:8])
    with jax.named_scope("pack_uv"):
        for z in middle:
            pack_plane(packed, z)
        face[4] = packed[0]
        face[5] = packed[1]
        start(exchanges[0][6:8])
        start(exchanges[0][2:4])
        start(duals[2:4])
    with jax.named_scope("pack_pq"):
        packed = [empty] * 6
        for z in range(zs):
            pack_dual(packed, z)
        for k in range(6):
            xs_own[k] = packed[k]
        start(duals[4:6])
    with jax.named_scope("inside0"):
        each(0, zs, dual_inside, ())
    with jax.named_scope("prepare"):
        for load in loads[8:]:
            load.wait()
        lax.fori_loop(0, zs, prepare, 0)

    for s in range(ITERS):
        last = s == ITERS - 1
        moves = exchanges[s]
        if s > 0:
            with jax.named_scope(f"inside{s}"):
                each(0, zs, dual_inside, ())
        with jax.named_scope(f"wait_xy{s}"):
            got(moves[2:6])
            line_up(s)
        with jax.named_scope(f"dual_mid{s}"):
            for z in range(zs):
                dual(z, s)
            if s > 0:
                halo_x_inside(s)
                halo_y_inside(s)
        if s == 0:
            with jax.named_scope(f"wait_pq{s}"):
                got(duals[2:6])
                halo_x_inside(s)
                halo_y_inside(s)
        with jax.named_scope(f"wait_diag{s}"):
            got(moves[6:])
        with jax.named_scope(f"halo_xy{s}"):
            halo_x(s)
            halo_y(s)
        with jax.named_scope(f"wait_z{s}"):
            got(moves[:2])
            sent(moves)
        if s == 0:
            with jax.named_scope(f"wait_zpq{s}"):
                got(duals[:2])
            with jax.named_scope("early"):
                halo_z_first(range(blocks - 1))
                dual_ends(s, range(blocks - 1))
                for z in ends:
                    primal(z, range(blocks // 2))
                start(duals[8:])
            with jax.named_scope("middle"):
                for z in middle:
                    primal(z)
            with jax.named_scope("wait_zpq_rest"):
                got(duals[6:8])
                sent(duals[:8])
        elif s == 1:
            with jax.named_scope("wait_early"):
                got(duals[8:])
                sent(duals[8:])
        with jax.named_scope(f"ends{s}"):
            packed = [empty, empty]
            if s == 0:
                halo_z_first([blocks - 1])
                dual_ends(s, [blocks - 1])
                for z in ends:
                    primal(z, range(blocks // 2, blocks))
            else:
                halo_z(s)
                dual_ends(s)
                if last:
                    edge_y[0] = yp[1]
                    edge_z[0] = zp[2]
                    for at, k in enumerate(Y_PARTS):
                        edge_y[1 + at] = yq[k]
                    for at, k in enumerate(Z_PARTS):
                        edge_z[1 + at] = zq[k]
                    continue
                for z in ends:
                    primal(z)
            for z in ends:
                pack_plane(packed, z)
            xe[0] = packed[0]
            xe[1] = packed[1]
        with jax.named_scope(f"send_z{s}"):
            start(exchanges[s + 1][8:])
            start(exchanges[s + 1][:2])
        with jax.named_scope(f"primal_mid{s}"):
            if s > 0:
                for z in middle:
                    primal(z)
            for z in middle:
                pack_plane(packed, z)
            face[4] = packed[0]
            face[5] = packed[1]
        with jax.named_scope(f"send{s}"):
            start(exchanges[s + 1][6:8])
            start(exchanges[s + 1][2:6])


def last_primal(
    u_in, v_in, p_in, q_in, gain, offset, cp, edge_y, edge_z,
    u_out, v_out, p_out, q_out,
    u_new, v_new, sems,
):
    zs, ys, xs = u_in.shape
    place = [lax.axis_index(a) for a in AXES]
    count = [lax.axis_size(a) for a in AXES]
    below = [place[i] > 0 for i in range(3)]
    above = [place[i] < count[i] - 1 for i in range(3)]
    copies = [pltpu.make_async_copy(q_in.at[k], q_out.at[k], sems.at[k]) for k in range(6)]
    copies += [pltpu.make_async_copy(p_in.at[k], p_out.at[k], sems.at[6 + k]) for k in range(3)]
    for copy in copies:
        copy.start()
    halo = (
        cp,
        lambda z: edge_y[0, pl.ds(z, 1), :],
        lambda k, z: edge_y[1 + Y_PARTS.index(k), pl.ds(z, 1), :],
        lambda r: edge_z[0, r, :],
        lambda k, r: edge_z[1 + Z_PARTS.index(k), r, :],
    )
    for z in range(zs):
        for _, r, pieces in primal_plane(z, below, above, u_in, v_in, p_in, q_in, gain, offset, halo):
            u_new[z, r, :] = pieces[0][0]
            for k in range(3):
                v_new[k, z, r, :] = pieces[1 + k][0]
        if z % 2 == 1:
            two = pl.ds(z - 1, 2)
            mine = [
                pltpu.make_async_copy(v_new.at[:, two], v_out.at[:, two], sems.at[9 + z - 1]),
                pltpu.make_async_copy(u_new.at[two], u_out.at[two], sems.at[9 + z]),
            ]
            for copy in mine:
                copy.start()
            copies += mine
    for copy in copies:
        copy.wait()


def per_device(noisy_image, fidelity, primal_u, primal_v, dual_p, dual_q):
    zs, ys, xs = primal_u.shape
    blocks = ys // 8
    assert zs == 8 and ys % 8 == 0 and blocks & (blocks - 1) == 0 and 4 * zs * blocks == xs == 128
    f32 = jnp.float32

    def vmem(*shape):
        return pltpu.VMEM(shape, f32)

    shapes = [a.shape for a in (primal_u, primal_v, dual_p, dual_q)]
    kept = shapes + [(zs, ys, xs), (zs, ys, xs), (3, 8, xs), (4, 8, xs), (4, ys, xs)]
    results = pl.pallas_call(
        kernel,
        out_shape=tuple(vmem(*shape) for shape in kept),
        in_specs=[pl.BlockSpec(memory_space=pl.ANY)] * 6,
        out_specs=tuple([pl.BlockSpec(memory_space=pltpu.VMEM)] * len(kept)),
        scratch_shapes=[
            vmem(4, zs, ys, xs),
            vmem(10, 8, xs),
            vmem(ITERS, 4, ys, xs),
            vmem(ITERS, 4, ys, xs),
            vmem(ITERS, 2, 8, xs),
            vmem(ITERS, 2, 8, xs),
            vmem(ITERS, 4, 8, xs),
            vmem(ITERS, 4, 8, xs),
            vmem(ITERS, 2, 8, xs),
            vmem(ITERS, 2, 8, xs),
            vmem(ITERS, 2, 8, xs),
            vmem(ITERS, 2, 8, xs),
            vmem(ITERS, 4, 8, xs),
            vmem(ITERS, 4, 8, xs),
            vmem(3, ys, xs),
            vmem(6, ys, xs),
            vmem(3, 8, xs),
            vmem(6, 8, xs),
            vmem(6, 8, xs),
            vmem(6, 8, xs),
            vmem(6, 8, xs),
            vmem(3, 8, xs),
            vmem(2, 8, xs),
            vmem(3, ys, xs),
            vmem(6, ys, xs),
            vmem(3, ys, xs),
            vmem(6, ys, xs),
            pltpu.SemaphoreType.DMA((12,)),
            pltpu.SemaphoreType.DMA((ITERS, 12)),
            pltpu.SemaphoreType.DMA((ITERS, 12)),
            pltpu.SemaphoreType.DMA((10,)),
            pltpu.SemaphoreType.DMA((10,)),
        ],
        compiler_params=pltpu.CompilerParams(collective_id=0, has_side_effects=True),
        name="tgv",
    )(noisy_image, fidelity, primal_u, primal_v, dual_p, dual_q)
    return pl.pallas_call(
        last_primal,
        out_shape=tuple(jax.ShapeDtypeStruct(shape, f32) for shape in shapes),
        in_specs=[pl.BlockSpec(memory_space=pltpu.VMEM)] * len(kept),
        out_specs=tuple([pl.BlockSpec(memory_space=pl.ANY)] * 4),
        scratch_shapes=[
            vmem(zs, ys, xs),
            vmem(3, zs, ys, xs),
            pltpu.SemaphoreType.DMA((9 + zs,)),
        ],
        name="out",
    )(*[pltpu.with_memory_space_constraint(r, pltpu.VMEM) for r in results])


def solution(mesh):
    scalar, stack = P("gz", "gy", "gx"), P(None, "gz", "gy", "gx")
    return jax.shard_map(
        per_device,
        mesh=mesh,
        in_specs=(scalar, scalar, scalar, stack, stack, stack),
        out_specs=(scalar, stack, stack, stack),
        check_vma=False,
    )
```

```python
import jax
import jax.numpy as jnp
from jax import lax
from jax.experimental import pallas as pl
from jax.experimental.pallas import tpu as pltpu
from jax.sharding import PartitionSpec as P

ITERS = 3
AXES = ("gx", "gy", "gz")
ALPHA1, ALPHA0, SIGMA, TAU = 0.5, 1.0, 0.2, 0.2
XX, YY, ZZ, XY, XZ, YZ = range(6)
PARTS = ((XX, XY, XZ), (XY, YY, YZ), (XZ, YZ, ZZ))
Y_PARTS, Z_PARTS = (XY, YY, YZ), (XZ, YZ, ZZ)
MESH = pl.DeviceIdType.MESH
Z_UP, Z_DOWN, X_UP, X_DOWN, Y_UP, Y_DOWN, XY_A, XY_B, XZ_A, XZ_B, YZ_A, YZ_B = range(12)
WAYS = (
    (0, 0, 1), (0, 0, -1), (1, 0, 0), (-1, 0, 0), (0, 1, 0), (0, -1, 0),
    (1, -1, 0), (-1, 1, 0), (1, 0, -1), (-1, 0, 1), (0, 1, -1), (0, -1, 1),
)


def primal_plane(z, below, above, u_ref, v_ref, p_ref, q_ref, gain, offset, halo, only=None):
    zs, ys, xs = u_ref.shape
    blocks = ys // 8
    cp, row_p, row_q, plane_p, plane_q = halo
    lane = lax.broadcasted_iota(jnp.int32, (8, xs), 1)
    sub = lax.broadcasted_iota(jnp.int32, (8, xs), 0)
    first_lane, last_lane = lane == 0, lane == xs - 1
    first_row, last_row = sub == 0, sub == 7

    def factor(flag):
        return jnp.where(flag, jnp.float32(1), jnp.float32(0))

    up_x = jnp.where(last_lane, factor(above[0]), 1.0)
    lo_x = jnp.where(first_lane, factor(below[0]), 1.0)
    up_z = factor(above[2]) if z == zs - 1 else 1.0
    lo_z = factor(below[2]) if z == 0 else 1.0
    for b in range(blocks) if only is None else only:
        r = pl.ds(8 * b, 8)
        up_y = jnp.where(last_row, factor(above[1]), 1.0) if b == blocks - 1 else 1.0
        lo_y = jnp.where(first_row, factor(below[1]), 1.0) if b == 0 else 1.0
        by = xs // 2 - 2 * (z * blocks + b)
        from_x = [pltpu.roll(cp[k], by, 1) for k in range(3)]
        p = [p_ref[k, z, r, :] for k in range(3)]
        q = [q_ref[k, z, r, :] for k in range(6)]
        before_x = jnp.where(first_lane, from_x[0], pltpu.roll(p[0], 1, 1))
        if b > 0:
            before_y = p_ref[1, z, pl.ds(8 * b - 1, 8), :]
        else:
            before_y = jnp.where(first_row, row_p(z), pltpu.roll(p[1], 1, 0))
        before_z = plane_p(r) if z == 0 else p_ref[2, z - 1, r, :]
        div = (up_x * p[0] - before_x) + (up_y * p[1] - before_y) + (up_z * p[2] - before_z)
        old = u_ref[z, r, :]
        pieces = [((old + TAU * div) * gain[z, r, :] + offset[z, r, :], old)]
        for k, (ax, ay, az) in enumerate(PARTS):
            after_x = jnp.where(last_lane, from_x[k], pltpu.roll(q[ax], xs - 1, 1))
            if b < blocks - 1:
                after_y = q_ref[ay, z, pl.ds(8 * b + 1, 8), :]
            else:
                after_y = jnp.where(last_row, row_q(ay, z), pltpu.roll(q[ay], 7, 0))
            after_z = plane_q(az, r) if z == zs - 1 else q_ref[az, z + 1, r, :]
            div2 = (after_x - lo_x * q[ax]) + (after_y - lo_y * q[ay]) + (after_z - lo_z * q[az])
            old = v_ref[k, z, r, :]
            pieces.append((old + TAU * (p[k] + div2), old))
        yield b, r, pieces


def kernel(*refs):
    dma = pltpu.SemaphoreType.DMA
    pl.run_scoped(lambda *own: exchange_kernel(*own, *refs), dma((5,)), dma((12,)), dma((10,)), dma((2, 12)), dma((10,)))


def exchange_kernel(
    load_sem, send_sem, first_send, recv_sem, first_recv,
    noisy_in, fid_in, u_in, v_in, p_in, q_in,
    u_out, v_out, p_out, q_out, gain, offset, cp, edge_y, edge_z,
    bar, face,
    z_lo, z_hi, x_lo, x_hi, y_lo, y_hi, d_a, d_b, d_c, d_d, d_e, d_g,
    zp, zq, yp, yq, xs_own, xp, xq, cv, xe, part_p, part_q, tz_p, tz_q,
):
    zs, ys, xs = u_in.shape
    blocks = ys // 8
    pairs = zs * blocks
    half_lanes = 2 * pairs
    place = [lax.axis_index(a) for a in AXES]
    count = [lax.axis_size(a) for a in AXES]
    below = [place[i] > 0 for i in range(3)]
    above = [place[i] < count[i] - 1 for i in range(3)]


    def exists(way):
        there = None
        for i, by in enumerate(way):
            if by:
                one = above[i] if by > 0 else below[i]
                there = one if there is None else jnp.logical_and(there, one)
        return there

    def target(way):
        return {AXES[i]: place[i] + by for i, by in enumerate(way) if by}

    goes = [exists(way) for way in WAYS]
    comes = [exists(tuple(-by for by in way)) for way in WAYS]
    peers = sum(there.astype(jnp.int32) for there in goes)

    u_face, xf, top_face = pl.ds(0, 4), pl.ds(4, 2), pl.ds(6, 4)
    def load(group, *pairs):
        return [pltpu.make_async_copy(src, dst, load_sem.at[group]) for src, dst in pairs]

    loads = (
        load(0, (u_in, bar.at[0]), (v_in, bar.at[pl.ds(1, 3)])),
        load(
            1,
            (u_in.at[:, 0], face.at[0]), (v_in.at[:, :, 0], face.at[pl.ds(1, 3)]),
            (u_in.at[:, ys - 1], face.at[6]), (v_in.at[:, :, ys - 1], face.at[pl.ds(7, 3)]),
        ),
        load(2, (q_in, q_out)),
        load(3, (p_in, p_out)),
        load(4, (noisy_in, offset), (fid_in, gain), (u_in, u_out), (v_in, v_out)),
    )
    whole = (bar, face.at[pl.ds(0, 8)], q_out, p_out, q_out)

    def begin(*groups):
        for k in groups:
            for copy in loads[k]:
                copy.start()

    def loaded(*groups):
        for k in groups:
            pltpu.make_async_copy(whole[k], whole[k], load_sem.at[k]).wait()

    begin(0)

    barrier = pltpu.get_barrier_semaphore()
    for way, there in zip(WAYS, goes):
        @pl.when(there)
        def _():
            pl.semaphore_signal(barrier, inc=1, device_id=target(way), device_id_type=MESH)

    begin(1, 2, 3)

    def clear(there, *refs):
        @pl.when(jnp.logical_not(there))
        def _():
            for ref in refs:
                ref[...] = jnp.zeros(ref.shape, jnp.float32)

    clear(below[0], x_lo, xp)
    clear(above[0], x_hi, xq)
    clear(below[1], y_lo, yp)
    clear(above[1], y_hi, yq)
    clear(below[2], z_lo, zp)
    clear(above[2], z_hi, zq)
    for way, ref in zip(WAYS[6:], (d_a, d_b, d_c, d_d, d_e, d_g)):
        clear(exists(tuple(-by for by in way)), ref)

    lane = lax.broadcasted_iota(jnp.int32, (8, xs), 1)
    sub = lax.broadcasted_iota(jnp.int32, (8, xs), 0)
    pair = lane >> 1
    odd = (lane & 1) == 1
    first_lane, last_lane = lane == 0, lane == xs - 1
    first_row, last_row = sub == 0, sub == 7
    p_pair, q_pair = (lane - half_lanes) >> 1, (lane + 1 - half_lanes) >> 1

    def factor(flag):
        return jnp.where(flag, jnp.float32(1), jnp.float32(0))

    up_x = jnp.where(last_lane, factor(above[0]), 1.0)
    lo_x = jnp.where(first_lane, factor(below[0]), 1.0)
    up_y_last = jnp.where(last_row, factor(above[1]), 1.0)
    lo_y_first = jnp.where(first_row, factor(below[1]), 1.0)

    def rows(b, by=0):
        return pl.ds(8 * b + by, 8)

    def turn_lanes(value, by):
        return value if isinstance(by, int) and by % xs == 0 else pltpu.roll(value, by % xs if isinstance(by, int) else by, 1)

    def turn_rows(value, by):
        return pltpu.roll(value, by % 8, 0)

    def flush(later):
        for ref, at, value in later:
            ref[at + (slice(None),)] = value
        later.clear()

    def up_z(z):
        return factor(jnp.logical_or(z < zs - 1, above[2]))

    def lo_z(z):
        return factor(jnp.logical_or(z > 0, below[2]))

    def up_y(b, value):
        return up_y_last * value if b == blocks - 1 else value

    def lo_y(b, value):
        return lo_y_first * value if b == 0 else value

    def next_x(value):
        return jnp.where(last_lane, 0.0, pltpu.roll(value, xs - 1, 1))

    def prev_x(value):
        return jnp.where(first_lane, 0.0, pltpu.roll(value, 1, 1))

    def next_y(ref, k, z, b, value):
        if b < blocks - 1:
            return ref[k, z, rows(b, 1), :]
        return jnp.where(last_row, 0.0, pltpu.roll(value, 7, 0))

    def prev_y(ref, k, z, b, value):
        if b > 0:
            return ref[k, z, rows(b, -1), :]
        return jnp.where(first_row, 0.0, pltpu.roll(value, 1, 0))

    def next_z(ref, k, z, b):
        if isinstance(z, int):
            return ref[k, z + 1, rows(b), :] if z < zs - 1 else jnp.zeros((8, xs), jnp.float32)
        return factor(z < zs - 1) * ref[k, jnp.minimum(z + 1, zs - 1), rows(b), :]

    def prev_z(ref, k, z, b):
        if isinstance(z, int):
            return ref[k, z - 1, rows(b), :] if z > 0 else jnp.zeros((8, xs), jnp.float32)
        return factor(z > 0) * ref[k, jnp.maximum(z - 1, 0), rows(b), :]

    def shrink_p(t):
        size = t[0] * t[0] + t[1] * t[1] + t[2] * t[2]
        scale = jnp.minimum(1.0, ALPHA1 * lax.rsqrt(size))
        return [scale * part for part in t]

    def shrink_q(s):
        size = (s[XX] * s[XX] + s[YY] * s[YY] + s[ZZ] * s[ZZ]) + 2.0 * (
            s[XY] * s[XY] + s[XZ] * s[XZ] + s[YZ] * s[YZ]
        )
        scale = jnp.minimum(1.0, ALPHA0 * lax.rsqrt(size))
        return [scale * part for part in s]

    half = 0.5 * SIGMA

    def grow_q(q, dx, dy, dz):
        return [
            q[XX] + SIGMA * dx[0], q[YY] + SIGMA * dy[1], q[ZZ] + SIGMA * dz[2],
            q[XY] + half * (dy[0] + dx[1]), q[XZ] + half * (dz[0] + dx[2]),
            q[YZ] + half * (dz[1] + dy[2]),
        ]

    def keep(flag, value):
        return jnp.where(flag, value, 0.0)

    def pack(packed, value, base, j):
        return jnp.where(pair == base + j, pltpu.roll(value, 2 * (base + j) + 1, 1), packed)

    def pack_bar(packed, values, z, b):
        j = z * blocks + b
        packed[0] = pack(packed[0], values[0], 0, j)
        packed[0] = pack(packed[0], values[1], pairs, j)
        packed[1] = pack(packed[1], values[2], 0, j)
        packed[1] = pack(packed[1], values[3], pairs, j)

    def message(src, dst, way, send, recv):
        return pltpu.make_async_remote_copy(
            src_ref=src, dst_ref=dst, send_sem=send, recv_sem=recv,
            device_id=target(WAYS[way]), device_id_type=MESH,
        )

    ahead_rows, early = ys - 8, 8 * (blocks // 2)
    exchanges = []
    for s in range(ITERS):
        z_up_part = pl.ds(1, 3) if s == 0 else pl.ds(0, 4)
        z_down_part = pl.ds(0, 1) if s == 0 else pl.ds(0, 4)
        z_rows = pl.ds(early, ys - early) if s == 1 else pl.ds(0, ys)
        ends = (
            (bar.at[z_up_part, zs - 1, z_rows], z_lo.at[s, z_up_part, z_rows]),
            (bar.at[z_down_part, 0, z_rows], z_hi.at[s, z_down_part, z_rows]),
            (face.at[xf], x_lo.at[s]),
            (face.at[xf], x_hi.at[s]),
            (face.at[top_face], y_lo.at[s]),
            (face.at[u_face], y_hi.at[s]),
            (face.at[xf, pl.ds(0, 1)], d_a.at[s, :, pl.ds(0, 1)]),
            (face.at[xf, pl.ds(7, 1)], d_b.at[s, :, pl.ds(7, 1)]),
            (xe, d_c.at[s]),
            (xe, d_d.at[s]),
            (face.at[top_face, pl.ds(0, 1)], d_e.at[s, :, pl.ds(0, 1)]),
            (face.at[u_face, pl.ds(zs - 1, 1)], d_g.at[s, :, pl.ds(zs - 1, 1)]),
        )
        exchanges.append([
            (message(src, dst, k, send_sem.at[k], recv_sem.at[s % 2, k]), goes[k], comes[k])
            for k, (src, dst) in enumerate(ends)
        ])
    duals = [
        (message(src, dst, way, first_send.at[k], first_recv.at[k]), goes[way], comes[way])
        for k, (src, dst, way) in enumerate((
            (tz_p.at[:, pl.ds(0, ahead_rows)], zp.at[:, pl.ds(0, ahead_rows)], Z_UP),
            (tz_q.at[:, pl.ds(0, ahead_rows)], zq.at[:, pl.ds(0, ahead_rows)], Z_DOWN),
            (p_in.at[:, :, ys - 1], yp, Y_UP),
            (q_in.at[:, :, 0], yq, Y_DOWN),
            (xs_own, xp, X_UP),
            (xs_own, xq, X_DOWN),
            (tz_p.at[:, pl.ds(ahead_rows, 8)], zp.at[:, pl.ds(ahead_rows, 8)], Z_UP),
            (tz_q.at[:, pl.ds(ahead_rows, 8)], zq.at[:, pl.ds(ahead_rows, 8)], Z_DOWN),
            (bar.at[:, zs - 1, pl.ds(0, early)], z_lo.at[1, :, pl.ds(0, early)], Z_UP),
            (bar.at[:, 0, pl.ds(0, early)], z_hi.at[1, :, pl.ds(0, early)], Z_DOWN),
        ))
    ]

    def start(moves, only=None):
        for copy, there, _ in moves:
            @pl.when(there if only is None else jnp.logical_and(there, only))
            def _():
                copy.start()

    def sent(moves):
        for copy, there, _ in moves:
            @pl.when(there)
            def _():
                copy.wait_send()

    def got(moves):
        for copy, _, there in moves:
            @pl.when(there)
            def _():
                copy.wait_recv()

    empty = jnp.zeros((8, xs), jnp.float32)

    def each(low, high, body, carry):
        def turn(j, carry):
            one = list(carry)
            body(low + 2 * j, one)
            body(low + 2 * j + 1, one)
            return tuple(one)

        return lax.fori_loop(0, (high - low) // 2, turn, tuple(carry))

    def dual_block(z, b, for_p=True, for_q=True):
        r = rows(b)
        v = [bar[1 + k, z, r, :] for k in range(3)]
        p = q = None
        if for_p:
            u = bar[0, z, r, :]
            slopes = (
                next_x(u) - up_x * u,
                next_y(bar, 0, z, b, u) - up_y(b, u),
                next_z(bar, 0, z, b) - up_z(z) * u,
            )
            p = [p_out[k, z, r, :] + SIGMA * (slopes[k] - v[k]) for k in range(3)]
        if for_q:
            dx = [lo_x * v[k] - prev_x(v[k]) for k in range(3)]
            dy = [lo_y(b, v[k]) - prev_y(bar, 1 + k, z, b, v[k]) for k in range(3)]
            dz = [lo_z(z) * v[k] - prev_z(bar, 1 + k, z, b) for k in range(3)]
            q = grow_q([q_out[k, z, r, :] for k in range(6)], dx, dy, dz)
        return p, q

    def dual_inside(z, _):
        later = []
        for b in range(blocks):
            p, q = dual_block(z, b)
            later += [(p_out, (k, z, rows(b)), new) for k, new in enumerate(p)]
            later += [(q_out, (k, z, rows(b)), new) for k, new in enumerate(q)]
        flush(later)

    def dual_first():
        later = []
        for b in range(blocks):
            p, q = dual_block(zs - 1, b, for_q=False)[0], dual_block(0, b, for_p=False)[1]
            later += [(tz_p, (k, rows(b)), new) for k, new in enumerate(p)]
            later += [(tz_q, (k, rows(b)), new) for k, new in enumerate(q)]
        flush(later)

    def line_up(s):
        cv[0] = jnp.where(odd, turn_lanes(x_hi[s, 0], half_lanes - 2), x_lo[s, 0])
        cv[1] = turn_lanes(x_lo[s, 1], half_lanes)
        cv[2] = x_lo[s, 1]

    def less_q(q, x=None, y=None, z=None):
        q = list(q)
        if x is not None:
            q[XX] = q[XX] - SIGMA * x[0]
            q[XY] = q[XY] - half * x[1]
            q[XZ] = q[XZ] - half * x[2]
        if y is not None:
            q[YY] = q[YY] - SIGMA * y[1]
            q[XY] = q[XY] - half * y[0]
            q[YZ] = q[YZ] - half * y[2]
        if z is not None:
            q[ZZ] = q[ZZ] - SIGMA * z[2]
            q[XZ] = q[XZ] - half * z[0]
            q[YZ] = q[YZ] - half * z[1]
        return q

    def dual(z, s):
        later = []
        for b in range(blocks):
            r = rows(b)
            by = half_lanes - 2 * (z * blocks + b)
            from_x = [turn_lanes(cv[k], by) for k in range(3)]
            t = [p_out[k, z, r, :] for k in range(3)]
            t[0] = t[0] + SIGMA * jnp.where(last_lane, from_x[0], 0.0)
            if b == blocks - 1:
                t[1] = t[1] + SIGMA * jnp.where(last_row, y_hi[s, 0, pl.ds(z, 1), :], 0.0)
            for k in range(3):
                if z == zs - 1:
                    later.append((part_p, (k, r), t[k]))
            if z < zs - 1:
                for k, new in enumerate(shrink_p(t)):
                    later.append((p_out, (k, z, r), new))
            hx = [jnp.where(first_lane, part, 0.0) for part in from_x]
            hy = None
            if b == 0:
                hy = [jnp.where(first_row, y_lo[s, 1 + k, pl.ds(z, 1), :], 0.0) for k in range(3)]
            q = less_q([q_out[k, z, r, :] for k in range(6)], hx, hy)
            if z > 0:
                q = shrink_q(q)
            for k in range(6):
                later.append((part_q, (k, r), q[k]) if z == 0 else (q_out, (k, z, r), q[k]))
        flush(later)

    def dual_ends(s, only=range(blocks)):
        later = []
        for b in only:
            r = rows(b)
            t = [part_p[k, r, :] for k in range(3)]
            t[2] = t[2] + SIGMA * z_hi[s, 0, r, :]
            for k, new in enumerate(shrink_p(t)):
                later.append((p_out, (k, zs - 1, r), new))
            q = less_q([part_q[k, r, :] for k in range(6)], z=[z_lo[s, 1 + k, r, :] for k in range(3)])
            for k, new in enumerate(shrink_q(q)):
                later.append((q_out, (k, 0, r), new))
        flush(later)

    def spread(row):
        return jnp.broadcast_to(row, (8, xs))

    def column(row, lane_of_first):
        mine = lane == lane_of_first + 2 * blocks * sub
        return jnp.sum(jnp.where(mine, spread(row), 0.0), axis=1, keepdims=True)

    where = ((0, half_lanes), (1, 0), (1, half_lanes))

    def halo_x_inside(s):
        far = pairs - blocks
        up_yc = jnp.where(jnp.logical_and(last_row, (p_pair & (blocks - 1)) == blocks - 1), factor(above[1]), 1.0)
        lo_yc = jnp.where(jnp.logical_and(first_row, (q_pair & (blocks - 1)) == 0), factor(below[1]), 1.0)
        up_zc = jnp.where(p_pair >= far, factor(above[2]), 1.0)
        lo_zc = jnp.where(q_pair < blocks, factor(below[2]), 1.0)
        u = turn_lanes(x_lo[s, 0], half_lanes)
        v = [x_lo[s, 0], turn_lanes(x_lo[s, 1], half_lanes), x_lo[s, 1]]
        own = turn_lanes(face[4], half_lanes - 1)
        moved = turn_rows(u, -1)
        turned = jnp.where((p_pair & (blocks - 1)) == blocks - 1, 0.0, turn_lanes(moved, -2))
        ahead_y = jnp.where(last_row, turned, moved)
        ahead_z = jnp.where(p_pair >= far, 0.0, turn_lanes(u, -2 * blocks))
        slopes = (own - u, ahead_y - up_yc * u, ahead_z - up_zc * u)
        for k in range(3):
            xp[k] = xp[k] + SIGMA * (slopes[k] - v[k])

        v = [turn_lanes(x_hi[s, 0], -2), turn_lanes(x_hi[s, 1], half_lanes - 2), turn_lanes(x_hi[s, 1], -2)]
        mine = [turn_lanes(face[4], -1), turn_lanes(face[5], half_lanes - 1), turn_lanes(face[5], -1)]
        dx, dy, dz = [], [], []
        for k in range(3):
            dx.append(v[k] - mine[k])
            moved = turn_rows(v[k], 1)
            turned = jnp.where((q_pair & (blocks - 1)) == 0, 0.0, turn_lanes(moved, 2))
            dy.append(lo_yc * v[k] - jnp.where(first_row, turned, moved))
            dz.append(lo_zc * v[k] - jnp.where(q_pair < blocks, 0.0, turn_lanes(v[k], 2 * blocks)))
        q = [turn_lanes(xq[k], -2) if s == 0 else xq[k] for k in range(6)]
        for k, new in enumerate(grow_q(q, dx, dy, dz)):
            xq[k] = new

    def halo_x(s):
        far = pairs - blocks
        t = [xp[k] for k in range(3)]
        edge = turn_lanes(spread(d_a[s, 0, pl.ds(0, 1), :]), half_lanes + 2 * (blocks - 1))
        here = jnp.logical_and(last_row, (p_pair & (blocks - 1)) == blocks - 1)
        t[1] = t[1] + SIGMA * jnp.where(here, edge, 0.0)
        edge = turn_lanes(d_c[s, 0], half_lanes + 2 * far)
        t[2] = t[2] + SIGMA * jnp.where(p_pair >= far, edge, 0.0)
        p = [keep(below[0], part) for part in shrink_p(t)]
        here = jnp.logical_and(first_row, (q_pair & (blocks - 1)) == 0)
        edge_y, edge_z = [], []
        for h, base in where:
            edge = turn_lanes(spread(d_b[s, h, pl.ds(7, 1), :]), half_lanes - 2 * blocks - base)
            edge_y.append(jnp.where(here, edge, 0.0))
            edge = turn_lanes(d_d[s, h], half_lanes - 2 - 2 * far - base)
            edge_z.append(jnp.where(q_pair < blocks, edge, 0.0))
        q = shrink_q(less_q([xq[k] for k in range(6)], y=edge_y, z=edge_z))
        q = [keep(above[0], part) for part in q]
        for k in range(3):
            xp[k] = p[k]
        for k in range(6):
            xq[k] = q[k]
        cp[0] = jnp.where(odd, q[XX], p[0])
        cp[1] = q[XY]
        cp[2] = q[XZ]

    def halo_y_inside(s):
        up_zr = jnp.where(last_row, factor(above[2]), 1.0)
        lo_zr = jnp.where(first_row, factor(below[2]), 1.0)
        u = y_lo[s, 0]
        slopes = (
            next_x(u) - up_x * u,
            face[0] - u,
            jnp.where(last_row, 0.0, turn_rows(u, -1)) - up_zr * u,
        )
        for k in range(3):
            yp[k] = yp[k] + SIGMA * (slopes[k] - y_lo[s, 1 + k])
        v = [y_hi[s, 1 + k] for k in range(3)]
        dx = [lo_x * v[k] - prev_x(v[k]) for k in range(3)]
        dy = [v[k] - face[7 + k] for k in range(3)]
        dz = [lo_zr * v[k] - jnp.where(first_row, 0.0, turn_rows(v[k], 1)) for k in range(3)]
        for k, new in enumerate(grow_q([yq[k] for k in range(6)], dx, dy, dz)):
            yq[k] = new

    def halo_y(s):
        t = [yp[k] for k in range(3)]
        edge = column(d_b[s, 0, pl.ds(7, 1), :], 2 * blocks - 1)
        t[0] = t[0] + SIGMA * jnp.where(last_lane, edge, 0.0)
        t[2] = t[2] + SIGMA * jnp.where(last_row, d_e[s, 0, pl.ds(0, 1), :], 0.0)
        p = shrink_p(t)
        edge_x = [
            jnp.where(first_lane, column(d_a[s, h, pl.ds(0, 1), :], base), 0.0) for h, base in where
        ]
        edge_z = [jnp.where(first_row, d_g[s, 1 + k, pl.ds(zs - 1, 1), :], 0.0) for k in range(3)]
        q = shrink_q(less_q([yq[k] for k in range(6)], x=edge_x, z=edge_z))
        for k in range(3):
            yp[k] = keep(below[1], p[k])
        for k in range(6):
            yq[k] = keep(above[1], q[k])

    def halo_z_first(only):
        later = []
        for b in only:
            r = rows(b)
            t = [zp[k, r, :] for k in range(3)]
            edge_x = turn_lanes(d_d[0, 0], xs - 2 - 2 * (blocks * (zs - 1) + b))
            t[0] = t[0] + SIGMA * jnp.where(last_lane, edge_x, 0.0)
            if b == blocks - 1:
                t[1] = t[1] + SIGMA * jnp.where(last_row, d_g[0, 0, pl.ds(zs - 1, 1), :], 0.0)
            t[2] = t[2] + SIGMA * bar[0, 0, r, :]
            for k, new in enumerate(shrink_p(t)):
                later.append((zp, (k, r), keep(below[2], new)))

            hx = [
                jnp.where(first_lane, turn_lanes(d_c[0, h], -base - 2 * b), 0.0) for h, base in where
            ]
            hz = [bar[1 + k, zs - 1, r, :] for k in range(3)]
            hy = None
            if b == 0:
                hy = [jnp.where(first_row, d_e[0, 1 + k, pl.ds(0, 1), :], 0.0) for k in range(3)]
            q = less_q([zq[k, r, :] for k in range(6)], hx, hy, hz)
            for k, new in enumerate(shrink_q(q)):
                later.append((zq, (k, r), keep(above[2], new)))
        flush(later)

    def halo_z(s):
        later = []
        for b in range(blocks):
            r = rows(b)
            u = z_lo[s, 0, r, :]
            edge_x = turn_lanes(d_d[s, 0], xs - 2 - 2 * (blocks * (zs - 1) + b))
            if b < blocks - 1:
                ahead_y = z_lo[s, 0, rows(b, 1), :]
            else:
                ahead_y = jnp.where(last_row, d_g[s, 0, pl.ds(zs - 1, 1), :], turn_rows(u, -1))
            slopes = (
                jnp.where(last_lane, edge_x, turn_lanes(u, -1)) - up_x * u,
                ahead_y - up_y(b, u),
                bar[0, 0, r, :] - u,
            )
            p = shrink_p([zp[k, r, :] + SIGMA * (slopes[k] - z_lo[s, 1 + k, r, :]) for k in range(3)])
            for k in range(3):
                later.append((zp, (k, r), keep(below[2], p[k])))

            v = [z_hi[s, 1 + k, r, :] for k in range(3)]
            dx, dy, dz = [], [], []
            for k, (h, base) in enumerate(where):
                edge_x = turn_lanes(d_c[s, h], -base - 2 * b)
                dx.append(lo_x * v[k] - jnp.where(first_lane, edge_x, turn_lanes(v[k], 1)))
                if b > 0:
                    behind_y = z_hi[s, 1 + k, rows(b, -1), :]
                else:
                    behind_y = jnp.where(first_row, d_e[s, 1 + k, pl.ds(0, 1), :], turn_rows(v[k], 1))
                dy.append(lo_y(b, v[k]) - behind_y)
                dz.append(v[k] - bar[1 + k, zs - 1, r, :])
            q = shrink_q(grow_q([zq[k, r, :] for k in range(6)], dx, dy, dz))
            for k in range(6):
                later.append((zq, (k, r), keep(above[2], q[k])))
        flush(later)

    def pack_plane(packed, z):
        for b in range(blocks):
            pack_bar(packed, [bar[k, z, rows(b), :] for k in range(4)], z, b)

    halo = (
        cp,
        lambda z: yp[1, pl.ds(z, 1), :],
        lambda k, z: yq[k, pl.ds(z, 1), :],
        lambda r: zp[2, r, :],
        lambda k, r: zq[k, r, :],
    )

    def primal(z, only=None):
        later = []
        for b, r, pieces in primal_plane(z, below, above, u_out, v_out, p_out, q_out, gain, offset, halo, only):
            for k, (new, old) in enumerate(pieces):
                later.append((u_out, (z, r), new) if k == 0 else (v_out, (k - 1, z, r), new))
                ahead = 2.0 * new - old
                later.append((bar, (k, z, r), ahead))
                if b == 0:
                    later.append((face, (k, pl.ds(z, 1)), ahead[0:1, :]))
                if b == blocks - 1:
                    later.append((face, (6 + k, pl.ds(z, 1)), ahead[7:8, :]))
        flush(later)

    def pack_dual(packed, z):
        for b in range(blocks):
            for k in range(6):
                value = q_out[k, z, rows(b), :]
                if k < 3:
                    value = jnp.where(last_lane, p_out[k, z, rows(b), :], value)
                packed[k] = pack(packed[k], value, pairs, z * blocks + b)

    def prepare(z, carry):
        weight = TAU * gain[z]
        inverse = 1.0 / (1.0 + weight)
        gain[z] = inverse
        offset[z] = weight * offset[z] * inverse
        return carry

    ends, middle = (0, zs - 1), range(1, zs - 1)
    with jax.named_scope("load_uv"):
        loaded(0)
    with jax.named_scope("barrier"):
        pl.semaphore_wait(barrier, peers)
    with jax.named_scope("send_z0"):
        start(exchanges[0][:2])
        loaded(1)
        start(exchanges[0][4:6])
    with jax.named_scope("load_pq"):
        loaded(2, 3)
        begin(4)
    with jax.named_scope("first_z"):
        packed = [empty, empty]
        for z in ends:
            pack_plane(packed, z)
        dual_first()
        xe[0] = packed[0]
        xe[1] = packed[1]
        start(exchanges[0][8:])
        start(duals[:2])
        start(duals[6:8])
    with jax.named_scope("pack_uv"):
        for z in middle:
            pack_plane(packed, z)
        face[4] = packed[0]
        face[5] = packed[1]
        start(exchanges[0][6:8])
        start(exchanges[0][2:4])
        start(duals[2:4])
    with jax.named_scope("pack_pq"):
        packed = [empty] * 6
        for z in range(zs):
            pack_dual(packed, z)
        for k in range(6):
            xs_own[k] = packed[k]
        start(duals[4:6])
    with jax.named_scope("inside0"):
        each(0, zs, dual_inside, ())
    with jax.named_scope("prepare"):
        loaded(4)
        lax.fori_loop(0, zs, prepare, 0)

    for s in range(ITERS):
        last = s == ITERS - 1
        moves = exchanges[s]
        if s > 0:
            with jax.named_scope(f"inside{s}"):
                each(0, zs, dual_inside, ())
        with jax.named_scope(f"wait_xy{s}"):
            got(moves[2:6])
            line_up(s)
        with jax.named_scope(f"dual_mid{s}"):
            for z in range(zs):
                dual(z, s)
            if s > 0:
                halo_x_inside(s)
                halo_y_inside(s)
        if s == 0:
            with jax.named_scope(f"wait_pq{s}"):
                got(duals[2:6])
                halo_x_inside(s)
                halo_y_inside(s)
        with jax.named_scope(f"wait_diag{s}"):
            got(moves[6:])
        with jax.named_scope(f"halo_xy{s}"):
            halo_x(s)
            halo_y(s)
        with jax.named_scope(f"wait_z{s}"):
            got(moves[:2])
            sent(moves)
        if s == 0:
            with jax.named_scope(f"wait_zpq{s}"):
                got(duals[:2])
            with jax.named_scope("early"):
                halo_z_first(range(blocks - 1))
                dual_ends(s, range(blocks - 1))
                for z in ends:
                    primal(z, range(blocks // 2))
                start(duals[8:])
            with jax.named_scope("middle"):
                for z in middle:
                    primal(z)
            with jax.named_scope("wait_zpq_rest"):
                got(duals[6:8])
                sent(duals[:8])
        elif s == 1:
            with jax.named_scope("wait_early"):
                got(duals[8:])
                sent(duals[8:])
        with jax.named_scope(f"ends{s}"):
            packed = [empty, empty]
            if s == 0:
                halo_z_first([blocks - 1])
                dual_ends(s, [blocks - 1])
                for z in ends:
                    primal(z, range(blocks // 2, blocks))
            else:
                halo_z(s)
                dual_ends(s)
                if last:
                    edge_y[0] = yp[1]
                    edge_z[0] = zp[2]
                    for at, k in enumerate(Y_PARTS):
                        edge_y[1 + at] = yq[k]
                    for at, k in enumerate(Z_PARTS):
                        edge_z[1 + at] = zq[k]
                    continue
                for z in ends:
                    primal(z)
            for z in ends:
                pack_plane(packed, z)
            xe[0] = packed[0]
            xe[1] = packed[1]
        with jax.named_scope(f"send_z{s}"):
            start(exchanges[s + 1][8:])
            start(exchanges[s + 1][:2])
        with jax.named_scope(f"primal_mid{s}"):
            if s > 0:
                for z in middle:
                    primal(z)
            for z in middle:
                pack_plane(packed, z)
            face[4] = packed[0]
            face[5] = packed[1]
        with jax.named_scope(f"send{s}"):
            start(exchanges[s + 1][6:8])
            start(exchanges[s + 1][2:6])


def last_primal(*refs):
    pl.run_scoped(lambda sems: finish_kernel(sems, *refs), pltpu.SemaphoreType.DMA((4,)))


def finish_kernel(
    sems, u_in, v_in, p_in, q_in, gain, offset, cp, edge_y, edge_z,
    u_out, v_out, p_out, q_out,
    u_new, v_new,
):
    zs, ys, xs = u_in.shape
    place = [lax.axis_index(a) for a in AXES]
    count = [lax.axis_size(a) for a in AXES]
    below = [place[i] > 0 for i in range(3)]
    above = [place[i] < count[i] - 1 for i in range(3)]
    for k in range(6):
        pltpu.make_async_copy(q_in.at[k], q_out.at[k], sems.at[0]).start()
    for k in range(3):
        pltpu.make_async_copy(p_in.at[k], p_out.at[k], sems.at[1]).start()
    halo = (
        cp,
        lambda z: edge_y[0, pl.ds(z, 1), :],
        lambda k, z: edge_y[1 + Y_PARTS.index(k), pl.ds(z, 1), :],
        lambda r: edge_z[0, r, :],
        lambda k, r: edge_z[1 + Z_PARTS.index(k), r, :],
    )
    for z in range(zs):
        for _, r, pieces in primal_plane(z, below, above, u_in, v_in, p_in, q_in, gain, offset, halo):
            u_new[z, r, :] = pieces[0][0]
            for k in range(3):
                v_new[k, z, r, :] = pieces[1 + k][0]
        if z % 2 == 1:
            two = pl.ds(z - 1, 2)
            pltpu.make_async_copy(v_new.at[:, two], v_out.at[:, two], sems.at[2]).start()
            pltpu.make_async_copy(u_new.at[two], u_out.at[two], sems.at[3]).start()
    for k, (src, dst) in enumerate(((q_in, q_out), (p_in, p_out), (v_new, v_out), (u_new, u_out))):
        pltpu.make_async_copy(src, dst, sems.at[k]).wait()


def per_device(noisy_image, fidelity, primal_u, primal_v, dual_p, dual_q):
    zs, ys, xs = primal_u.shape
    blocks = ys // 8
    assert zs == 8 and ys % 8 == 0 and blocks & (blocks - 1) == 0 and 4 * zs * blocks == xs == 128
    f32 = jnp.float32

    def vmem(*shape):
        return pltpu.VMEM(shape, f32)

    shapes = [a.shape for a in (primal_u, primal_v, dual_p, dual_q)]
    kept = shapes + [(zs, ys, xs), (zs, ys, xs), (3, 8, xs), (4, 8, xs), (4, ys, xs)]
    results = pl.pallas_call(
        kernel,
        out_shape=tuple(vmem(*shape) for shape in kept),
        in_specs=[pl.BlockSpec(memory_space=pl.ANY)] * 6,
        out_specs=tuple([pl.BlockSpec(memory_space=pltpu.VMEM)] * len(kept)),
        scratch_shapes=[
            vmem(4, zs, ys, xs),
            vmem(10, 8, xs),
            vmem(ITERS, 4, ys, xs),
            vmem(ITERS, 4, ys, xs),
            vmem(ITERS, 2, 8, xs),
            vmem(ITERS, 2, 8, xs),
            vmem(ITERS, 4, 8, xs),
            vmem(ITERS, 4, 8, xs),
            vmem(ITERS, 2, 8, xs),
            vmem(ITERS, 2, 8, xs),
            vmem(ITERS, 2, 8, xs),
            vmem(ITERS, 2, 8, xs),
            vmem(ITERS, 4, 8, xs),
            vmem(ITERS, 4, 8, xs),
            vmem(3, ys, xs),
            vmem(6, ys, xs),
            vmem(3, 8, xs),
            vmem(6, 8, xs),
            vmem(6, 8, xs),
            vmem(6, 8, xs),
            vmem(6, 8, xs),
            vmem(3, 8, xs),
            vmem(2, 8, xs),
            vmem(3, ys, xs),
            vmem(6, ys, xs),
            vmem(3, ys, xs),
            vmem(6, ys, xs),
        ],
        compiler_params=pltpu.CompilerParams(collective_id=0, has_side_effects=True),
        name="tgv",
    )(noisy_image, fidelity, primal_u, primal_v, dual_p, dual_q)
    return pl.pallas_call(
        last_primal,
        out_shape=tuple(jax.ShapeDtypeStruct(shape, f32) for shape in shapes),
        in_specs=[pl.BlockSpec(memory_space=pltpu.VMEM)] * len(kept),
        out_specs=tuple([pl.BlockSpec(memory_space=pl.ANY)] * 4),
        scratch_shapes=[
            vmem(zs, ys, xs),
            vmem(3, zs, ys, xs),
        ],
        name="out",
    )(*[pltpu.with_memory_space_constraint(r, pltpu.VMEM) for r in results])


def solution(mesh):
    scalar, stack = P("gz", "gy", "gx"), P(None, "gz", "gy", "gx")
    return jax.shard_map(
        per_device,
        mesh=mesh,
        in_specs=(scalar, scalar, scalar, stack, stack, stack),
        out_specs=(scalar, stack, stack, stack),
        check_vma=False,
    )
```

```python
import jax
import jax.numpy as jnp
from jax import lax
from jax.experimental import pallas as pl
from jax.experimental.pallas import tpu as pltpu
from jax.sharding import PartitionSpec as P

ITERS = 3
AXES = ("gx", "gy", "gz")
ALPHA1, ALPHA0, SIGMA, TAU = 0.5, 1.0, 0.2, 0.2
XX, YY, ZZ, XY, XZ, YZ = range(6)
PARTS = ((XX, XY, XZ), (XY, YY, YZ), (XZ, YZ, ZZ))
Y_PARTS, Z_PARTS = (XY, YY, YZ), (XZ, YZ, ZZ)
MESH = pl.DeviceIdType.MESH
Z_UP, Z_DOWN, X_UP, X_DOWN, Y_UP, Y_DOWN, XY_A, XY_B, XZ_A, XZ_B, YZ_A, YZ_B = range(12)
WAYS = (
    (0, 0, 1), (0, 0, -1), (1, 0, 0), (-1, 0, 0), (0, 1, 0), (0, -1, 0),
    (1, -1, 0), (-1, 1, 0), (1, 0, -1), (-1, 0, 1), (0, 1, -1), (0, -1, 1),
)


def primal_plane(z, below, above, u_ref, v_ref, p_ref, q_ref, gain, offset, halo, only=None):
    zs, ys, xs = u_ref.shape
    blocks = ys // 8
    cp, row_p, row_q, plane_p, plane_q = halo
    lane = lax.broadcasted_iota(jnp.int32, (8, xs), 1)
    sub = lax.broadcasted_iota(jnp.int32, (8, xs), 0)
    first_lane, last_lane = lane == 0, lane == xs - 1
    first_row, last_row = sub == 0, sub == 7

    def factor(flag):
        return jnp.where(flag, jnp.float32(1), jnp.float32(0))

    up_x = jnp.where(last_lane, factor(above[0]), 1.0)
    lo_x = jnp.where(first_lane, factor(below[0]), 1.0)
    up_z = factor(above[2]) if z == zs - 1 else 1.0
    lo_z = factor(below[2]) if z == 0 else 1.0
    for b in range(blocks) if only is None else only:
        r = pl.ds(8 * b, 8)
        up_y = jnp.where(last_row, factor(above[1]), 1.0) if b == blocks - 1 else 1.0
        lo_y = jnp.where(first_row, factor(below[1]), 1.0) if b == 0 else 1.0
        by = xs // 2 - 2 * (z * blocks + b)
        from_x = [pltpu.roll(cp[k], by, 1) for k in range(3)]
        p = [p_ref[k, z, r, :] for k in range(3)]
        q = [q_ref[k, z, r, :] for k in range(6)]
        before_x = jnp.where(first_lane, from_x[0], pltpu.roll(p[0], 1, 1))
        if b > 0:
            before_y = p_ref[1, z, pl.ds(8 * b - 1, 8), :]
        else:
            before_y = jnp.where(first_row, row_p(z), pltpu.roll(p[1], 1, 0))
        before_z = plane_p(r) if z == 0 else p_ref[2, z - 1, r, :]
        div = (up_x * p[0] - before_x) + (up_y * p[1] - before_y) + (up_z * p[2] - before_z)
        old = u_ref[z, r, :]
        pieces = [((old + TAU * div) * gain[z, r, :] + offset[z, r, :], old)]
        for k, (ax, ay, az) in enumerate(PARTS):
            after_x = jnp.where(last_lane, from_x[k], pltpu.roll(q[ax], xs - 1, 1))
            if b < blocks - 1:
                after_y = q_ref[ay, z, pl.ds(8 * b + 1, 8), :]
            else:
                after_y = jnp.where(last_row, row_q(ay, z), pltpu.roll(q[ay], 7, 0))
            after_z = plane_q(az, r) if z == zs - 1 else q_ref[az, z + 1, r, :]
            div2 = (after_x - lo_x * q[ax]) + (after_y - lo_y * q[ay]) + (after_z - lo_z * q[az])
            old = v_ref[k, z, r, :]
            pieces.append((old + TAU * (p[k] + div2), old))
        yield b, r, pieces


def kernel(*refs):
    dma = pltpu.SemaphoreType.DMA
    pl.run_scoped(lambda *own: exchange_kernel(*own, *refs), dma((8,)), dma((12,)), dma((10,)), dma((2, 12)), dma((10,)))


def exchange_kernel(
    load_sem, send_sem, first_send, recv_sem, first_recv,
    noisy_in, fid_in, u_in, v_in, p_in, q_in,
    u_out, v_out, p_out, q_out, gain, offset, cp, edge_y, edge_z,
    bar, face,
    z_lo, z_hi, x_lo, x_hi, y_lo, y_hi, d_a, d_b, d_c, d_d, d_e, d_g,
    zp, zq, yp, yq, xs_own, xp, xq, cv, xe, part_p, part_q, tz_p, tz_q,
):
    zs, ys, xs = u_in.shape
    blocks = ys // 8
    pairs = zs * blocks
    half_lanes = 2 * pairs
    place = [lax.axis_index(a) for a in AXES]
    count = [lax.axis_size(a) for a in AXES]
    below = [place[i] > 0 for i in range(3)]
    above = [place[i] < count[i] - 1 for i in range(3)]


    def exists(way):
        there = None
        for i, by in enumerate(way):
            if by:
                one = above[i] if by > 0 else below[i]
                there = one if there is None else jnp.logical_and(there, one)
        return there

    def target(way):
        return {AXES[i]: place[i] + by for i, by in enumerate(way) if by}

    goes = [exists(way) for way in WAYS]
    comes = [exists(tuple(-by for by in way)) for way in WAYS]
    peers = sum(there.astype(jnp.int32) for there in goes)

    u_face, xf, top_face = pl.ds(0, 4), pl.ds(4, 2), pl.ds(6, 4)
    def load(group, *pairs):
        return [pltpu.make_async_copy(src, dst, load_sem.at[group]) for src, dst in pairs]

    inner = pl.ds(1, zs - 2)
    loads = (
        load(0, *[
            pair for z in (0, zs - 1)
            for pair in ((u_in.at[z], bar.at[0, z]), (v_in.at[:, z], bar.at[pl.ds(1, 3), z]))
        ]),
        load(
            1,
            (u_in.at[:, 0], face.at[0]), (v_in.at[:, :, 0], face.at[pl.ds(1, 3)]),
            (u_in.at[:, ys - 1], face.at[6]), (v_in.at[:, :, ys - 1], face.at[pl.ds(7, 3)]),
        ),
        load(2, (q_in.at[:, 0], q_out.at[:, 0])),
        load(3, (p_in.at[:, zs - 1], p_out.at[:, zs - 1])),
        load(4, (noisy_in, offset), (fid_in, gain), (u_in, u_out), (v_in, v_out)),
        load(5, (u_in.at[inner], bar.at[0, inner]), (v_in.at[:, inner], bar.at[pl.ds(1, 3), inner])),
        load(6, (q_in.at[:, pl.ds(1, zs - 1)], q_out.at[:, pl.ds(1, zs - 1)])),
        load(7, (p_in.at[:, pl.ds(0, zs - 1)], p_out.at[:, pl.ds(0, zs - 1)])),
    )
    whole = (
        bar.at[:, pl.ds(0, 2)], face.at[pl.ds(0, 8)], tz_q, tz_p, q_out,
        bar.at[:, inner], q_out.at[:, pl.ds(1, zs - 1)], p_out.at[:, pl.ds(0, zs - 1)],
    )

    def begin(*groups):
        for k in groups:
            for copy in loads[k]:
                copy.start()

    def loaded(*groups):
        for k in groups:
            pltpu.make_async_copy(whole[k], whole[k], load_sem.at[k]).wait()

    begin(0, 2, 3)

    barrier = pltpu.get_barrier_semaphore()
    for way, there in zip(WAYS, goes):
        @pl.when(there)
        def _():
            pl.semaphore_signal(barrier, inc=1, device_id=target(way), device_id_type=MESH)

    begin(1, 5, 6, 7)

    def clear(there, *refs):
        @pl.when(jnp.logical_not(there))
        def _():
            for ref in refs:
                ref[...] = jnp.zeros(ref.shape, jnp.float32)

    clear(below[0], x_lo, xp)
    clear(above[0], x_hi, xq)
    clear(below[1], y_lo, yp)
    clear(above[1], y_hi, yq)
    clear(below[2], z_lo, zp)
    clear(above[2], z_hi, zq)
    for way, ref in zip(WAYS[6:], (d_a, d_b, d_c, d_d, d_e, d_g)):
        clear(exists(tuple(-by for by in way)), ref)

    lane = lax.broadcasted_iota(jnp.int32, (8, xs), 1)
    sub = lax.broadcasted_iota(jnp.int32, (8, xs), 0)
    pair = lane >> 1
    odd = (lane & 1) == 1
    first_lane, last_lane = lane == 0, lane == xs - 1
    first_row, last_row = sub == 0, sub == 7
    p_pair, q_pair = (lane - half_lanes) >> 1, (lane + 1 - half_lanes) >> 1

    def factor(flag):
        return jnp.where(flag, jnp.float32(1), jnp.float32(0))

    up_x = jnp.where(last_lane, factor(above[0]), 1.0)
    lo_x = jnp.where(first_lane, factor(below[0]), 1.0)
    up_y_last = jnp.where(last_row, factor(above[1]), 1.0)
    lo_y_first = jnp.where(first_row, factor(below[1]), 1.0)

    def rows(b, by=0):
        return pl.ds(8 * b + by, 8)

    def turn_lanes(value, by):
        return value if isinstance(by, int) and by % xs == 0 else pltpu.roll(value, by % xs if isinstance(by, int) else by, 1)

    def turn_rows(value, by):
        return pltpu.roll(value, by % 8, 0)

    def flush(later):
        for ref, at, value in later:
            ref[at + (slice(None),)] = value
        later.clear()

    def up_z(z):
        return factor(jnp.logical_or(z < zs - 1, above[2]))

    def lo_z(z):
        return factor(jnp.logical_or(z > 0, below[2]))

    def up_y(b, value):
        return up_y_last * value if b == blocks - 1 else value

    def lo_y(b, value):
        return lo_y_first * value if b == 0 else value

    def next_x(value):
        return jnp.where(last_lane, 0.0, pltpu.roll(value, xs - 1, 1))

    def prev_x(value):
        return jnp.where(first_lane, 0.0, pltpu.roll(value, 1, 1))

    def next_y(ref, k, z, b, value):
        if b < blocks - 1:
            return ref[k, z, rows(b, 1), :]
        return jnp.where(last_row, 0.0, pltpu.roll(value, 7, 0))

    def prev_y(ref, k, z, b, value):
        if b > 0:
            return ref[k, z, rows(b, -1), :]
        return jnp.where(first_row, 0.0, pltpu.roll(value, 1, 0))

    def next_z(ref, k, z, b):
        if isinstance(z, int):
            return ref[k, z + 1, rows(b), :] if z < zs - 1 else jnp.zeros((8, xs), jnp.float32)
        return factor(z < zs - 1) * ref[k, jnp.minimum(z + 1, zs - 1), rows(b), :]

    def prev_z(ref, k, z, b):
        if isinstance(z, int):
            return ref[k, z - 1, rows(b), :] if z > 0 else jnp.zeros((8, xs), jnp.float32)
        return factor(z > 0) * ref[k, jnp.maximum(z - 1, 0), rows(b), :]

    def shrink_p(t):
        size = t[0] * t[0] + t[1] * t[1] + t[2] * t[2]
        scale = jnp.minimum(1.0, ALPHA1 * lax.rsqrt(size))
        return [scale * part for part in t]

    def shrink_q(s):
        size = (s[XX] * s[XX] + s[YY] * s[YY] + s[ZZ] * s[ZZ]) + 2.0 * (
            s[XY] * s[XY] + s[XZ] * s[XZ] + s[YZ] * s[YZ]
        )
        scale = jnp.minimum(1.0, ALPHA0 * lax.rsqrt(size))
        return [scale * part for part in s]

    half = 0.5 * SIGMA

    def grow_q(q, dx, dy, dz):
        return [
            q[XX] + SIGMA * dx[0], q[YY] + SIGMA * dy[1], q[ZZ] + SIGMA * dz[2],
            q[XY] + half * (dy[0] + dx[1]), q[XZ] + half * (dz[0] + dx[2]),
            q[YZ] + half * (dz[1] + dy[2]),
        ]

    def keep(flag, value):
        return jnp.where(flag, value, 0.0)

    def pack(packed, value, base, j):
        return jnp.where(pair == base + j, pltpu.roll(value, 2 * (base + j) + 1, 1), packed)

    def pack_bar(packed, values, z, b):
        j = z * blocks + b
        packed[0] = pack(packed[0], values[0], 0, j)
        packed[0] = pack(packed[0], values[1], pairs, j)
        packed[1] = pack(packed[1], values[2], 0, j)
        packed[1] = pack(packed[1], values[3], pairs, j)

    def message(src, dst, way, send, recv):
        return pltpu.make_async_remote_copy(
            src_ref=src, dst_ref=dst, send_sem=send, recv_sem=recv,
            device_id=target(WAYS[way]), device_id_type=MESH,
        )

    ahead_rows, early = ys - 8, 8 * (blocks // 2)
    exchanges = []
    for s in range(ITERS):
        z_up_part = pl.ds(1, 3) if s == 0 else pl.ds(0, 4)
        z_down_part = pl.ds(0, 1) if s == 0 else pl.ds(0, 4)
        z_rows = pl.ds(early, ys - early) if s == 1 else pl.ds(0, ys)
        ends = (
            (bar.at[z_up_part, zs - 1, z_rows], z_lo.at[s, z_up_part, z_rows]),
            (bar.at[z_down_part, 0, z_rows], z_hi.at[s, z_down_part, z_rows]),
            (face.at[xf], x_lo.at[s]),
            (face.at[xf], x_hi.at[s]),
            (face.at[top_face], y_lo.at[s]),
            (face.at[u_face], y_hi.at[s]),
            (face.at[xf, pl.ds(0, 1)], d_a.at[s, :, pl.ds(0, 1)]),
            (face.at[xf, pl.ds(7, 1)], d_b.at[s, :, pl.ds(7, 1)]),
            (xe, d_c.at[s]),
            (xe, d_d.at[s]),
            (face.at[top_face, pl.ds(0, 1)], d_e.at[s, :, pl.ds(0, 1)]),
            (face.at[u_face, pl.ds(zs - 1, 1)], d_g.at[s, :, pl.ds(zs - 1, 1)]),
        )
        exchanges.append([
            (message(src, dst, k, send_sem.at[k], recv_sem.at[s % 2, k]), goes[k], comes[k])
            for k, (src, dst) in enumerate(ends)
        ])
    duals = [
        (message(src, dst, way, first_send.at[k], first_recv.at[k]), goes[way], comes[way])
        for k, (src, dst, way) in enumerate((
            (tz_p.at[:, pl.ds(0, ahead_rows)], zp.at[:, pl.ds(0, ahead_rows)], Z_UP),
            (tz_q.at[:, pl.ds(0, ahead_rows)], zq.at[:, pl.ds(0, ahead_rows)], Z_DOWN),
            (p_in.at[:, :, ys - 1], yp, Y_UP),
            (q_in.at[:, :, 0], yq, Y_DOWN),
            (xs_own, xp, X_UP),
            (xs_own, xq, X_DOWN),
            (tz_p.at[:, pl.ds(ahead_rows, 8)], zp.at[:, pl.ds(ahead_rows, 8)], Z_UP),
            (tz_q.at[:, pl.ds(ahead_rows, 8)], zq.at[:, pl.ds(ahead_rows, 8)], Z_DOWN),
            (bar.at[:, zs - 1, pl.ds(0, early)], z_lo.at[1, :, pl.ds(0, early)], Z_UP),
            (bar.at[:, 0, pl.ds(0, early)], z_hi.at[1, :, pl.ds(0, early)], Z_DOWN),
        ))
    ]

    def start(moves, only=None):
        for copy, there, _ in moves:
            @pl.when(there if only is None else jnp.logical_and(there, only))
            def _():
                copy.start()

    def sent(moves):
        for copy, there, _ in moves:
            @pl.when(there)
            def _():
                copy.wait_send()

    def got(moves):
        for copy, _, there in moves:
            @pl.when(there)
            def _():
                copy.wait_recv()

    empty = jnp.zeros((8, xs), jnp.float32)

    def each(low, high, body, carry):
        def turn(j, carry):
            one = list(carry)
            body(low + 2 * j, one)
            body(low + 2 * j + 1, one)
            return tuple(one)

        return lax.fori_loop(0, (high - low) // 2, turn, tuple(carry))

    def dual_block(z, b, for_p=True, for_q=True):
        r = rows(b)
        v = [bar[1 + k, z, r, :] for k in range(3)]
        p = q = None
        if for_p:
            u = bar[0, z, r, :]
            slopes = (
                next_x(u) - up_x * u,
                next_y(bar, 0, z, b, u) - up_y(b, u),
                next_z(bar, 0, z, b) - up_z(z) * u,
            )
            p = [p_out[k, z, r, :] + SIGMA * (slopes[k] - v[k]) for k in range(3)]
        if for_q:
            dx = [lo_x * v[k] - prev_x(v[k]) for k in range(3)]
            dy = [lo_y(b, v[k]) - prev_y(bar, 1 + k, z, b, v[k]) for k in range(3)]
            dz = [lo_z(z) * v[k] - prev_z(bar, 1 + k, z, b) for k in range(3)]
            q = grow_q([q_out[k, z, r, :] for k in range(6)], dx, dy, dz)
        return p, q

    def dual_inside(z, _):
        later = []
        for b in range(blocks):
            p, q = dual_block(z, b)
            later += [(p_out, (k, z, rows(b)), new) for k, new in enumerate(p)]
            later += [(q_out, (k, z, rows(b)), new) for k, new in enumerate(q)]
        flush(later)

    def dual_first():
        later = []
        for b in range(blocks):
            p, q = dual_block(zs - 1, b, for_q=False)[0], dual_block(0, b, for_p=False)[1]
            later += [(tz_p, (k, rows(b)), new) for k, new in enumerate(p)]
            later += [(tz_q, (k, rows(b)), new) for k, new in enumerate(q)]
        flush(later)

    def line_up(s):
        cv[0] = SIGMA * jnp.where(odd, turn_lanes(x_hi[s, 0], half_lanes - 2), x_lo[s, 0])
        cv[1] = half * turn_lanes(x_lo[s, 1], half_lanes)
        cv[2] = half * x_lo[s, 1]

    def less_q(q, x=None, y=None, z=None):
        q = list(q)
        if x is not None:
            q[XX] = q[XX] - SIGMA * x[0]
            q[XY] = q[XY] - half * x[1]
            q[XZ] = q[XZ] - half * x[2]
        if y is not None:
            q[YY] = q[YY] - SIGMA * y[1]
            q[XY] = q[XY] - half * y[0]
            q[YZ] = q[YZ] - half * y[2]
        if z is not None:
            q[ZZ] = q[ZZ] - SIGMA * z[2]
            q[XZ] = q[XZ] - half * z[0]
            q[YZ] = q[YZ] - half * z[1]
        return q

    def dual(z, s):
        later = []
        for b in range(blocks):
            r = rows(b)
            by = half_lanes - 2 * (z * blocks + b)
            from_x = [turn_lanes(cv[k], by) for k in range(3)]
            t = [p_out[k, z, r, :] for k in range(3)]
            t[0] = t[0] + jnp.where(last_lane, from_x[0], 0.0)
            if b == blocks - 1:
                t[1] = t[1] + SIGMA * jnp.where(last_row, y_hi[s, 0, pl.ds(z, 1), :], 0.0)
            for k in range(3):
                if z == zs - 1:
                    later.append((part_p, (k, r), t[k]))
            if z < zs - 1:
                for k, new in enumerate(shrink_p(t)):
                    later.append((p_out, (k, z, r), new))
            hx = [jnp.where(first_lane, part, 0.0) for part in from_x]
            hy = None
            if b == 0:
                hy = [jnp.where(first_row, y_lo[s, 1 + k, pl.ds(z, 1), :], 0.0) for k in range(3)]
            q = less_q([q_out[k, z, r, :] for k in range(6)], y=hy)
            for k, part in zip((XX, XY, XZ), hx):
                q[k] = q[k] - part
            if z > 0:
                q = shrink_q(q)
            for k in range(6):
                later.append((part_q, (k, r), q[k]) if z == 0 else (q_out, (k, z, r), q[k]))
        flush(later)

    def dual_ends(s, only=range(blocks)):
        later = []
        for b in only:
            r = rows(b)
            t = [part_p[k, r, :] for k in range(3)]
            t[2] = t[2] + SIGMA * z_hi[s, 0, r, :]
            for k, new in enumerate(shrink_p(t)):
                later.append((p_out, (k, zs - 1, r), new))
            q = less_q([part_q[k, r, :] for k in range(6)], z=[z_lo[s, 1 + k, r, :] for k in range(3)])
            for k, new in enumerate(shrink_q(q)):
                later.append((q_out, (k, 0, r), new))
        flush(later)

    def spread(row):
        return jnp.broadcast_to(row, (8, xs))

    def column(row, lane_of_first):
        mine = lane == lane_of_first + 2 * blocks * sub
        return jnp.sum(jnp.where(mine, spread(row), 0.0), axis=1, keepdims=True)

    where = ((0, half_lanes), (1, 0), (1, half_lanes))

    def halo_x_inside(s):
        far = pairs - blocks
        up_yc = jnp.where(jnp.logical_and(last_row, (p_pair & (blocks - 1)) == blocks - 1), factor(above[1]), 1.0)
        lo_yc = jnp.where(jnp.logical_and(first_row, (q_pair & (blocks - 1)) == 0), factor(below[1]), 1.0)
        up_zc = jnp.where(p_pair >= far, factor(above[2]), 1.0)
        lo_zc = jnp.where(q_pair < blocks, factor(below[2]), 1.0)
        u = turn_lanes(x_lo[s, 0], half_lanes)
        v = [x_lo[s, 0], turn_lanes(x_lo[s, 1], half_lanes), x_lo[s, 1]]
        own = turn_lanes(face[4], half_lanes - 1)
        moved = turn_rows(u, -1)
        turned = jnp.where((p_pair & (blocks - 1)) == blocks - 1, 0.0, turn_lanes(moved, -2))
        ahead_y = jnp.where(last_row, turned, moved)
        ahead_z = jnp.where(p_pair >= far, 0.0, turn_lanes(u, -2 * blocks))
        slopes = (own - u, ahead_y - up_yc * u, ahead_z - up_zc * u)
        for k in range(3):
            xp[k] = xp[k] + SIGMA * (slopes[k] - v[k])

        v = [turn_lanes(x_hi[s, 0], -2), turn_lanes(x_hi[s, 1], half_lanes - 2), turn_lanes(x_hi[s, 1], -2)]
        mine = [turn_lanes(face[4], -1), turn_lanes(face[5], half_lanes - 1), turn_lanes(face[5], -1)]
        dx, dy, dz = [], [], []
        for k in range(3):
            dx.append(v[k] - mine[k])
            moved = turn_rows(v[k], 1)
            turned = jnp.where((q_pair & (blocks - 1)) == 0, 0.0, turn_lanes(moved, 2))
            dy.append(lo_yc * v[k] - jnp.where(first_row, turned, moved))
            dz.append(lo_zc * v[k] - jnp.where(q_pair < blocks, 0.0, turn_lanes(v[k], 2 * blocks)))
        q = [turn_lanes(xq[k], -2) if s == 0 else xq[k] for k in range(6)]
        for k, new in enumerate(grow_q(q, dx, dy, dz)):
            xq[k] = new

    def halo_x(s):
        far = pairs - blocks
        t = [xp[k] for k in range(3)]
        edge = turn_lanes(spread(d_a[s, 0, pl.ds(0, 1), :]), half_lanes + 2 * (blocks - 1))
        here = jnp.logical_and(last_row, (p_pair & (blocks - 1)) == blocks - 1)
        t[1] = t[1] + SIGMA * jnp.where(here, edge, 0.0)
        edge = turn_lanes(d_c[s, 0], half_lanes + 2 * far)
        t[2] = t[2] + SIGMA * jnp.where(p_pair >= far, edge, 0.0)
        p = [keep(below[0], part) for part in shrink_p(t)]
        here = jnp.logical_and(first_row, (q_pair & (blocks - 1)) == 0)
        edge_y, edge_z = [], []
        for h, base in where:
            edge = turn_lanes(spread(d_b[s, h, pl.ds(7, 1), :]), half_lanes - 2 * blocks - base)
            edge_y.append(jnp.where(here, edge, 0.0))
            edge = turn_lanes(d_d[s, h], half_lanes - 2 - 2 * far - base)
            edge_z.append(jnp.where(q_pair < blocks, edge, 0.0))
        q = shrink_q(less_q([xq[k] for k in range(6)], y=edge_y, z=edge_z))
        q = [keep(above[0], part) for part in q]
        for k in range(3):
            xp[k] = p[k]
        for k in range(6):
            xq[k] = q[k]
        cp[0] = jnp.where(odd, q[XX], p[0])
        cp[1] = q[XY]
        cp[2] = q[XZ]

    def halo_y_inside(s):
        up_zr = jnp.where(last_row, factor(above[2]), 1.0)
        lo_zr = jnp.where(first_row, factor(below[2]), 1.0)
        u = y_lo[s, 0]
        slopes = (
            next_x(u) - up_x * u,
            face[0] - u,
            jnp.where(last_row, 0.0, turn_rows(u, -1)) - up_zr * u,
        )
        for k in range(3):
            yp[k] = yp[k] + SIGMA * (slopes[k] - y_lo[s, 1 + k])
        v = [y_hi[s, 1 + k] for k in range(3)]
        dx = [lo_x * v[k] - prev_x(v[k]) for k in range(3)]
        dy = [v[k] - face[7 + k] for k in range(3)]
        dz = [lo_zr * v[k] - jnp.where(first_row, 0.0, turn_rows(v[k], 1)) for k in range(3)]
        for k, new in enumerate(grow_q([yq[k] for k in range(6)], dx, dy, dz)):
            yq[k] = new

    def halo_y(s):
        t = [yp[k] for k in range(3)]
        edge = column(d_b[s, 0, pl.ds(7, 1), :], 2 * blocks - 1)
        t[0] = t[0] + SIGMA * jnp.where(last_lane, edge, 0.0)
        t[2] = t[2] + SIGMA * jnp.where(last_row, d_e[s, 0, pl.ds(0, 1), :], 0.0)
        p = shrink_p(t)
        edge_x = [
            jnp.where(first_lane, column(d_a[s, h, pl.ds(0, 1), :], base), 0.0) for h, base in where
        ]
        edge_z = [jnp.where(first_row, d_g[s, 1 + k, pl.ds(zs - 1, 1), :], 0.0) for k in range(3)]
        q = shrink_q(less_q([yq[k] for k in range(6)], x=edge_x, z=edge_z))
        for k in range(3):
            yp[k] = keep(below[1], p[k])
        for k in range(6):
            yq[k] = keep(above[1], q[k])

    def halo_z_first(only):
        later = []
        for b in only:
            r = rows(b)
            t = [zp[k, r, :] for k in range(3)]
            edge_x = turn_lanes(d_d[0, 0], xs - 2 - 2 * (blocks * (zs - 1) + b))
            t[0] = t[0] + SIGMA * jnp.where(last_lane, edge_x, 0.0)
            if b == blocks - 1:
                t[1] = t[1] + SIGMA * jnp.where(last_row, d_g[0, 0, pl.ds(zs - 1, 1), :], 0.0)
            t[2] = t[2] + SIGMA * bar[0, 0, r, :]
            for k, new in enumerate(shrink_p(t)):
                later.append((zp, (k, r), keep(below[2], new)))

            hx = [
                jnp.where(first_lane, turn_lanes(d_c[0, h], -base - 2 * b), 0.0) for h, base in where
            ]
            hz = [bar[1 + k, zs - 1, r, :] for k in range(3)]
            hy = None
            if b == 0:
                hy = [jnp.where(first_row, d_e[0, 1 + k, pl.ds(0, 1), :], 0.0) for k in range(3)]
            q = less_q([zq[k, r, :] for k in range(6)], hx, hy, hz)
            for k, new in enumerate(shrink_q(q)):
                later.append((zq, (k, r), keep(above[2], new)))
        flush(later)

    def halo_z(s):
        later = []
        for b in range(blocks):
            r = rows(b)
            u = z_lo[s, 0, r, :]
            edge_x = turn_lanes(d_d[s, 0], xs - 2 - 2 * (blocks * (zs - 1) + b))
            if b < blocks - 1:
                ahead_y = z_lo[s, 0, rows(b, 1), :]
            else:
                ahead_y = jnp.where(last_row, d_g[s, 0, pl.ds(zs - 1, 1), :], turn_rows(u, -1))
            slopes = (
                jnp.where(last_lane, edge_x, turn_lanes(u, -1)) - up_x * u,
                ahead_y - up_y(b, u),
                bar[0, 0, r, :] - u,
            )
            p = shrink_p([zp[k, r, :] + SIGMA * (slopes[k] - z_lo[s, 1 + k, r, :]) for k in range(3)])
            for k in range(3):
                later.append((zp, (k, r), keep(below[2], p[k])))

            v = [z_hi[s, 1 + k, r, :] for k in range(3)]
            dx, dy, dz = [], [], []
            for k, (h, base) in enumerate(where):
                edge_x = turn_lanes(d_c[s, h], -base - 2 * b)
                dx.append(lo_x * v[k] - jnp.where(first_lane, edge_x, turn_lanes(v[k], 1)))
                if b > 0:
                    behind_y = z_hi[s, 1 + k, rows(b, -1), :]
                else:
                    behind_y = jnp.where(first_row, d_e[s, 1 + k, pl.ds(0, 1), :], turn_rows(v[k], 1))
                dy.append(lo_y(b, v[k]) - behind_y)
                dz.append(v[k] - bar[1 + k, zs - 1, r, :])
            q = shrink_q(grow_q([zq[k, r, :] for k in range(6)], dx, dy, dz))
            for k in range(6):
                later.append((zq, (k, r), keep(above[2], q[k])))
        flush(later)

    def pack_plane(packed, z):
        for b in range(blocks):
            pack_bar(packed, [bar[k, z, rows(b), :] for k in range(4)], z, b)

    halo = (
        cp,
        lambda z: yp[1, pl.ds(z, 1), :],
        lambda k, z: yq[k, pl.ds(z, 1), :],
        lambda r: zp[2, r, :],
        lambda k, r: zq[k, r, :],
    )

    def primal(z, only=None):
        later = []
        for b, r, pieces in primal_plane(z, below, above, u_out, v_out, p_out, q_out, gain, offset, halo, only):
            for k, (new, old) in enumerate(pieces):
                later.append((u_out, (z, r), new) if k == 0 else (v_out, (k - 1, z, r), new))
                ahead = 2.0 * new - old
                later.append((bar, (k, z, r), ahead))
                if b == 0:
                    later.append((face, (k, pl.ds(z, 1)), ahead[0:1, :]))
                if b == blocks - 1:
                    later.append((face, (6 + k, pl.ds(z, 1)), ahead[7:8, :]))
        flush(later)

    def pack_dual(packed, z):
        for b in range(blocks):
            for k in range(6):
                value = q_out[k, z, rows(b), :]
                if k < 3:
                    value = jnp.where(last_lane, p_out[k, z, rows(b), :], value)
                packed[k] = pack(packed[k], value, pairs, z * blocks + b)

    def prepare(z, carry):
        weight = TAU * gain[z]
        inverse = 1.0 / (1.0 + weight)
        gain[z] = inverse
        offset[z] = weight * offset[z] * inverse
        return carry

    ends, middle = (0, zs - 1), range(1, zs - 1)

    def primal_and_pack(lag=3):
        packed = [empty, empty]
        for z in middle:
            primal(z)
            if z > lag:
                pack_plane(packed, z - lag)
        for z in middle[-lag:]:
            pack_plane(packed, z)
        return packed

    with jax.named_scope("load_uv"):
        loaded(0)
    with jax.named_scope("barrier"):
        pl.semaphore_wait(barrier, peers)
    with jax.named_scope("send_z0"):
        start(exchanges[0][:2])
    with jax.named_scope("load_pq"):
        loaded(2, 3, 1)
        begin(4)
    with jax.named_scope("first_z"):
        packed = [empty, empty]
        for z in ends:
            pack_plane(packed, z)
        dual_first()
        xe[0] = packed[0]
        xe[1] = packed[1]
        start(exchanges[0][8:])
        start(duals[:2])
        start(duals[6:8])
        start(exchanges[0][4:6])
    with jax.named_scope("pack_uv"):
        loaded(5)
        for z in middle:
            pack_plane(packed, z)
        face[4] = packed[0]
        face[5] = packed[1]
        start(exchanges[0][6:8])
        start(exchanges[0][2:4])
        start(duals[2:4])
    with jax.named_scope("pack_pq"):
        loaded(6, 7)
        packed = [empty] * 6
        for z in range(zs):
            pack_dual(packed, z)
        for k in range(6):
            xs_own[k] = packed[k]
        start(duals[4:6])
    with jax.named_scope("inside0"):
        each(0, zs, dual_inside, ())
    with jax.named_scope("prepare"):
        loaded(4)
        lax.fori_loop(0, zs, prepare, 0)

    for s in range(ITERS):
        last = s == ITERS - 1
        moves = exchanges[s]
        if s > 0:
            with jax.named_scope(f"inside{s}"):
                each(0, zs, dual_inside, ())
        with jax.named_scope(f"wait_xy{s}"):
            got(moves[2:6])
            line_up(s)
        with jax.named_scope(f"dual_mid{s}"):
            for z in range(zs):
                dual(z, s)
            if s > 0:
                halo_x_inside(s)
                halo_y_inside(s)
        if s == 0:
            with jax.named_scope(f"wait_pq{s}"):
                got(duals[2:6])
                halo_x_inside(s)
                halo_y_inside(s)
        with jax.named_scope(f"wait_diag{s}"):
            got(moves[6:])
        with jax.named_scope(f"halo_xy{s}"):
            halo_x(s)
            halo_y(s)
        with jax.named_scope(f"wait_z{s}"):
            got(moves[:2])
            sent(moves)
        if s == 0:
            with jax.named_scope(f"wait_zpq{s}"):
                got(duals[:2])
            with jax.named_scope("early"):
                halo_z_first(range(blocks - 1))
                dual_ends(s, range(blocks - 1))
                for z in ends:
                    primal(z, range(blocks // 2))
                start(duals[8:])
            with jax.named_scope("middle"):
                packed = primal_and_pack()
            with jax.named_scope("wait_zpq_rest"):
                got(duals[6:8])
                sent(duals[:8])
        elif s == 1:
            with jax.named_scope("wait_early"):
                got(duals[8:])
                sent(duals[8:])
        with jax.named_scope(f"ends{s}"):
            of_ends = [empty, empty]
            if s == 0:
                halo_z_first([blocks - 1])
                dual_ends(s, [blocks - 1])
                for z in ends:
                    primal(z, range(blocks // 2, blocks))
            else:
                halo_z(s)
                dual_ends(s)
                if last:
                    edge_y[0] = yp[1]
                    edge_z[0] = zp[2]
                    for at, k in enumerate(Y_PARTS):
                        edge_y[1 + at] = yq[k]
                    for at, k in enumerate(Z_PARTS):
                        edge_z[1 + at] = zq[k]
                    continue
                for z in ends:
                    primal(z)
            for z in ends:
                pack_plane(of_ends, z)
            xe[0] = of_ends[0]
            xe[1] = of_ends[1]
            if s == 0:
                face[4] = packed[0] + of_ends[0]
                face[5] = packed[1] + of_ends[1]
        with jax.named_scope(f"send_z{s}"):
            start(exchanges[s + 1][8:])
            if s == 0:
                start(exchanges[s + 1][4:8])
                start(exchanges[s + 1][2:4])
            start(exchanges[s + 1][:2])
        if s > 0:
            with jax.named_scope(f"primal_mid{s}"):
                packed = primal_and_pack()
                face[4] = packed[0] + of_ends[0]
                face[5] = packed[1] + of_ends[1]
            with jax.named_scope(f"send{s}"):
                start(exchanges[s + 1][4:8])
                start(exchanges[s + 1][2:4])


def last_primal(*refs):
    pl.run_scoped(lambda sems: finish_kernel(sems, *refs), pltpu.SemaphoreType.DMA((4,)))


def finish_kernel(
    sems, u_in, v_in, p_in, q_in, gain, offset, cp, edge_y, edge_z,
    u_out, v_out, p_out, q_out,
    u_new, v_new,
):
    zs, ys, xs = u_in.shape
    place = [lax.axis_index(a) for a in AXES]
    count = [lax.axis_size(a) for a in AXES]
    below = [place[i] > 0 for i in range(3)]
    above = [place[i] < count[i] - 1 for i in range(3)]
    for k in range(6):
        pltpu.make_async_copy(q_in.at[k], q_out.at[k], sems.at[0]).start()
    for k in range(3):
        pltpu.make_async_copy(p_in.at[k], p_out.at[k], sems.at[1]).start()
    halo = (
        cp,
        lambda z: edge_y[0, pl.ds(z, 1), :],
        lambda k, z: edge_y[1 + Y_PARTS.index(k), pl.ds(z, 1), :],
        lambda r: edge_z[0, r, :],
        lambda k, r: edge_z[1 + Z_PARTS.index(k), r, :],
    )
    for z in range(zs):
        for _, r, pieces in primal_plane(z, below, above, u_in, v_in, p_in, q_in, gain, offset, halo):
            u_new[z, r, :] = pieces[0][0]
            for k in range(3):
                v_new[k, z, r, :] = pieces[1 + k][0]
        if z % 2 == 1:
            two = pl.ds(z - 1, 2)
            pltpu.make_async_copy(v_new.at[:, two], v_out.at[:, two], sems.at[2]).start()
            pltpu.make_async_copy(u_new.at[two], u_out.at[two], sems.at[3]).start()
    for k, (src, dst) in enumerate(((q_in, q_out), (p_in, p_out), (v_new, v_out), (u_new, u_out))):
        pltpu.make_async_copy(src, dst, sems.at[k]).wait()


def per_device(noisy_image, fidelity, primal_u, primal_v, dual_p, dual_q):
    zs, ys, xs = primal_u.shape
    blocks = ys // 8
    assert zs == 8 and ys % 8 == 0 and blocks & (blocks - 1) == 0 and 4 * zs * blocks == xs == 128
    f32 = jnp.float32

    def vmem(*shape):
        return pltpu.VMEM(shape, f32)

    shapes = [a.shape for a in (primal_u, primal_v, dual_p, dual_q)]
    kept = shapes + [(zs, ys, xs), (zs, ys, xs), (3, 8, xs), (4, 8, xs), (4, ys, xs)]
    results = pl.pallas_call(
        kernel,
        out_shape=tuple(vmem(*shape) for shape in kept),
        in_specs=[pl.BlockSpec(memory_space=pl.ANY)] * 6,
        out_specs=tuple([pl.BlockSpec(memory_space=pltpu.VMEM)] * len(kept)),
        scratch_shapes=[
            vmem(4, zs, ys, xs),
            vmem(10, 8, xs),
            vmem(ITERS, 4, ys, xs),
            vmem(ITERS, 4, ys, xs),
            vmem(ITERS, 2, 8, xs),
            vmem(ITERS, 2, 8, xs),
            vmem(ITERS, 4, 8, xs),
            vmem(ITERS, 4, 8, xs),
            vmem(ITERS, 2, 8, xs),
            vmem(ITERS, 2, 8, xs),
            vmem(ITERS, 2, 8, xs),
            vmem(ITERS, 2, 8, xs),
            vmem(ITERS, 4, 8, xs),
            vmem(ITERS, 4, 8, xs),
            vmem(3, ys, xs),
            vmem(6, ys, xs),
            vmem(3, 8, xs),
            vmem(6, 8, xs),
            vmem(6, 8, xs),
            vmem(6, 8, xs),
            vmem(6, 8, xs),
            vmem(3, 8, xs),
            vmem(2, 8, xs),
            vmem(3, ys, xs),
            vmem(6, ys, xs),
            vmem(3, ys, xs),
            vmem(6, ys, xs),
        ],
        compiler_params=pltpu.CompilerParams(collective_id=0, has_side_effects=True),
        name="tgv",
    )(noisy_image, fidelity, primal_u, primal_v, dual_p, dual_q)
    return pl.pallas_call(
        last_primal,
        out_shape=tuple(jax.ShapeDtypeStruct(shape, f32) for shape in shapes),
        in_specs=[pl.BlockSpec(memory_space=pltpu.VMEM)] * len(kept),
        out_specs=tuple([pl.BlockSpec(memory_space=pl.ANY)] * 4),
        scratch_shapes=[
            vmem(zs, ys, xs),
            vmem(3, zs, ys, xs),
        ],
        name="out",
    )(*[pltpu.with_memory_space_constraint(r, pltpu.VMEM) for r in results])


def solution(mesh):
    scalar, stack = P("gz", "gy", "gx"), P(None, "gz", "gy", "gx")
    return jax.shard_map(
        per_device,
        mesh=mesh,
        in_specs=(scalar, scalar, scalar, stack, stack, stack),
        out_specs=(scalar, stack, stack, stack),
        check_vma=False,
    )
```

```python
import jax
import jax.numpy as jnp
from jax import lax
from jax.experimental import pallas as pl
from jax.experimental.pallas import tpu as pltpu
from jax.sharding import PartitionSpec as P

ITERS = 3
AXES = ("gx", "gy", "gz")
ALPHA1, ALPHA0, SIGMA, TAU = 0.5, 1.0, 0.2, 0.2
XX, YY, ZZ, XY, XZ, YZ = range(6)
PARTS = ((XX, XY, XZ), (XY, YY, YZ), (XZ, YZ, ZZ))
Y_PARTS, Z_PARTS = (XY, YY, YZ), (XZ, YZ, ZZ)
MESH = pl.DeviceIdType.MESH
Z_UP, Z_DOWN, X_UP, X_DOWN, Y_UP, Y_DOWN, XY_A, XY_B, XZ_A, XZ_B, YZ_A, YZ_B = range(12)
WAYS = (
    (0, 0, 1), (0, 0, -1), (1, 0, 0), (-1, 0, 0), (0, 1, 0), (0, -1, 0),
    (1, -1, 0), (-1, 1, 0), (1, 0, -1), (-1, 0, 1), (0, 1, -1), (0, -1, 1),
)


def primal_plane(z, below, above, u_ref, v_ref, p_ref, q_ref, gain, offset, halo, only=None):
    zs, ys, xs = u_ref.shape
    blocks = ys // 8
    cp, row_p, row_q, plane_p, plane_q = halo
    lane = lax.broadcasted_iota(jnp.int32, (8, xs), 1)
    sub = lax.broadcasted_iota(jnp.int32, (8, xs), 0)
    first_lane, last_lane = lane == 0, lane == xs - 1
    first_row, last_row = sub == 0, sub == 7

    def factor(flag):
        return jnp.where(flag, jnp.float32(1), jnp.float32(0))

    up_x = jnp.where(last_lane, factor(above[0]), 1.0)
    lo_x = jnp.where(first_lane, factor(below[0]), 1.0)
    up_z = factor(above[2]) if z == zs - 1 else 1.0
    lo_z = factor(below[2]) if z == 0 else 1.0
    for b in range(blocks) if only is None else only:
        r = pl.ds(8 * b, 8)
        up_y = jnp.where(last_row, factor(above[1]), 1.0) if b == blocks - 1 else 1.0
        lo_y = jnp.where(first_row, factor(below[1]), 1.0) if b == 0 else 1.0
        by = xs // 2 - 2 * (z * blocks + b)
        from_x = [pltpu.roll(cp[k], by, 1) for k in range(3)]
        p = [p_ref[k, z, r, :] for k in range(3)]
        q = [q_ref[k, z, r, :] for k in range(6)]
        before_x = jnp.where(first_lane, from_x[0], pltpu.roll(p[0], 1, 1))
        if b > 0:
            before_y = p_ref[1, z, pl.ds(8 * b - 1, 8), :]
        else:
            before_y = jnp.where(first_row, row_p(z), pltpu.roll(p[1], 1, 0))
        before_z = plane_p(r) if z == 0 else p_ref[2, z - 1, r, :]
        div = (up_x * p[0] - before_x) + (up_y * p[1] - before_y) + (up_z * p[2] - before_z)
        old = u_ref[z, r, :]
        pieces = [((old + TAU * div) * gain[z, r, :] + offset[z, r, :], old)]
        for k, (ax, ay, az) in enumerate(PARTS):
            after_x = jnp.where(last_lane, from_x[k], pltpu.roll(q[ax], xs - 1, 1))
            if b < blocks - 1:
                after_y = q_ref[ay, z, pl.ds(8 * b + 1, 8), :]
            else:
                after_y = jnp.where(last_row, row_q(ay, z), pltpu.roll(q[ay], 7, 0))
            after_z = plane_q(az, r) if z == zs - 1 else q_ref[az, z + 1, r, :]
            div2 = (after_x - lo_x * q[ax]) + (after_y - lo_y * q[ay]) + (after_z - lo_z * q[az])
            old = v_ref[k, z, r, :]
            pieces.append((old + TAU * (p[k] + div2), old))
        yield b, r, pieces


def kernel(*refs):
    dma = pltpu.SemaphoreType.DMA
    pl.run_scoped(lambda *own: exchange_kernel(*own, *refs), dma((8,)), dma((12,)), dma((10,)), dma((2, 12)), dma((10,)))


def exchange_kernel(
    load_sem, send_sem, first_send, recv_sem, first_recv,
    noisy_in, fid_in, u_in, v_in, p_in, q_in,
    u_out, v_out, p_out, q_out, gain, offset, cp, edge_y, edge_z,
    bar, face,
    z_lo, z_hi, x_lo, x_hi, y_lo, y_hi, d_a, d_b, d_c, d_d, d_e, d_g,
    zp, zq, yp, yq, xs_own, xp, xq, cv, xe, part_p, part_q, tz_p, tz_q,
):
    zs, ys, xs = u_in.shape
    blocks = ys // 8
    pairs = zs * blocks
    half_lanes = 2 * pairs
    place = [lax.axis_index(a) for a in AXES]
    count = [lax.axis_size(a) for a in AXES]
    below = [place[i] > 0 for i in range(3)]
    above = [place[i] < count[i] - 1 for i in range(3)]


    def exists(way):
        there = None
        for i, by in enumerate(way):
            if by:
                one = above[i] if by > 0 else below[i]
                there = one if there is None else jnp.logical_and(there, one)
        return there

    def target(way):
        return {AXES[i]: place[i] + by for i, by in enumerate(way) if by}

    goes = [exists(way) for way in WAYS]
    comes = [exists(tuple(-by for by in way)) for way in WAYS]
    peers = sum(there.astype(jnp.int32) for there in goes)

    u_face, xf, top_face = pl.ds(0, 4), pl.ds(4, 2), pl.ds(6, 4)
    def load(group, *pairs):
        return [pltpu.make_async_copy(src, dst, load_sem.at[group]) for src, dst in pairs]

    inner = pl.ds(1, zs - 2)
    loads = (
        load(0, *[
            pair for z in (0, zs - 1)
            for pair in ((u_in.at[z], bar.at[0, z]), (v_in.at[:, z], bar.at[pl.ds(1, 3), z]))
        ]),
        load(
            1,
            (u_in.at[:, 0], face.at[0]), (v_in.at[:, :, 0], face.at[pl.ds(1, 3)]),
            (u_in.at[:, ys - 1], face.at[6]), (v_in.at[:, :, ys - 1], face.at[pl.ds(7, 3)]),
        ),
        load(2, (q_in.at[:, 0], q_out.at[:, 0])),
        load(3, (p_in.at[:, zs - 1], p_out.at[:, zs - 1])),
        load(4, (noisy_in, offset), (fid_in, gain), (u_in, u_out), (v_in, v_out)),
        load(5, (u_in.at[inner], bar.at[0, inner]), (v_in.at[:, inner], bar.at[pl.ds(1, 3), inner])),
        load(6, (q_in.at[:, pl.ds(1, zs - 1)], q_out.at[:, pl.ds(1, zs - 1)])),
        load(7, (p_in.at[:, pl.ds(0, zs - 1)], p_out.at[:, pl.ds(0, zs - 1)])),
    )
    whole = (
        bar.at[:, pl.ds(0, 2)], face.at[pl.ds(0, 8)], tz_q, tz_p, q_out,
        bar.at[:, inner], q_out.at[:, pl.ds(1, zs - 1)], p_out.at[:, pl.ds(0, zs - 1)],
    )

    def begin(*groups):
        for k in groups:
            for copy in loads[k]:
                copy.start()

    def loaded(*groups):
        for k in groups:
            pltpu.make_async_copy(whole[k], whole[k], load_sem.at[k]).wait()

    begin(0, 2, 3)

    barrier = pltpu.get_barrier_semaphore()
    for way, there in zip(WAYS, goes):
        @pl.when(there)
        def _():
            pl.semaphore_signal(barrier, inc=1, device_id=target(way), device_id_type=MESH)

    begin(1, 5, 6, 7)

    def clear(there, *refs):
        @pl.when(jnp.logical_not(there))
        def _():
            for ref in refs:
                ref[...] = jnp.zeros(ref.shape, jnp.float32)

    clear(below[0], x_lo, xp)
    clear(above[0], x_hi, xq)
    clear(below[1], y_lo, yp)
    clear(above[1], y_hi, yq)
    clear(below[2], z_lo, zp)
    clear(above[2], z_hi, zq)
    for way, ref in zip(WAYS[6:], (d_a, d_b, d_c, d_d, d_e, d_g)):
        clear(exists(tuple(-by for by in way)), ref)

    lane = lax.broadcasted_iota(jnp.int32, (8, xs), 1)
    sub = lax.broadcasted_iota(jnp.int32, (8, xs), 0)
    pair = lane >> 1
    odd = (lane & 1) == 1
    first_lane, last_lane = lane == 0, lane == xs - 1
    first_row, last_row = sub == 0, sub == 7
    p_pair, q_pair = (lane - half_lanes) >> 1, (lane + 1 - half_lanes) >> 1

    def factor(flag):
        return jnp.where(flag, jnp.float32(1), jnp.float32(0))

    up_x = jnp.where(last_lane, factor(above[0]), 1.0)
    lo_x = jnp.where(first_lane, factor(below[0]), 1.0)
    up_y_last = jnp.where(last_row, factor(above[1]), 1.0)
    lo_y_first = jnp.where(first_row, factor(below[1]), 1.0)

    def rows(b, by=0):
        return pl.ds(8 * b + by, 8)

    def turn_lanes(value, by):
        return value if isinstance(by, int) and by % xs == 0 else pltpu.roll(value, by % xs if isinstance(by, int) else by, 1)

    def turn_rows(value, by):
        return pltpu.roll(value, by % 8, 0)

    def flush(later):
        for ref, at, value in later:
            ref[at + (slice(None),)] = value
        later.clear()

    def up_z(z):
        return factor(jnp.logical_or(z < zs - 1, above[2]))

    def lo_z(z):
        return factor(jnp.logical_or(z > 0, below[2]))

    def up_y(b, value):
        return up_y_last * value if b == blocks - 1 else value

    def lo_y(b, value):
        return lo_y_first * value if b == 0 else value

    def next_x(value):
        return jnp.where(last_lane, 0.0, pltpu.roll(value, xs - 1, 1))

    def prev_x(value):
        return jnp.where(first_lane, 0.0, pltpu.roll(value, 1, 1))

    def next_y(ref, k, z, b, value):
        if b < blocks - 1:
            return ref[k, z, rows(b, 1), :]
        return jnp.where(last_row, 0.0, pltpu.roll(value, 7, 0))

    def prev_y(ref, k, z, b, value):
        if b > 0:
            return ref[k, z, rows(b, -1), :]
        return jnp.where(first_row, 0.0, pltpu.roll(value, 1, 0))

    def next_z(ref, k, z, b):
        if isinstance(z, int):
            return ref[k, z + 1, rows(b), :] if z < zs - 1 else jnp.zeros((8, xs), jnp.float32)
        return factor(z < zs - 1) * ref[k, jnp.minimum(z + 1, zs - 1), rows(b), :]

    def prev_z(ref, k, z, b):
        if isinstance(z, int):
            return ref[k, z - 1, rows(b), :] if z > 0 else jnp.zeros((8, xs), jnp.float32)
        return factor(z > 0) * ref[k, jnp.maximum(z - 1, 0), rows(b), :]

    def shrink_p(t):
        size = t[0] * t[0] + t[1] * t[1] + t[2] * t[2]
        scale = jnp.minimum(1.0, ALPHA1 * lax.rsqrt(size))
        return [scale * part for part in t]

    def shrink_q(s):
        size = (s[XX] * s[XX] + s[YY] * s[YY] + s[ZZ] * s[ZZ]) + 2.0 * (
            s[XY] * s[XY] + s[XZ] * s[XZ] + s[YZ] * s[YZ]
        )
        scale = jnp.minimum(1.0, ALPHA0 * lax.rsqrt(size))
        return [scale * part for part in s]

    half = 0.5 * SIGMA

    def grow_q(q, dx, dy, dz):
        return [
            q[XX] + SIGMA * dx[0], q[YY] + SIGMA * dy[1], q[ZZ] + SIGMA * dz[2],
            q[XY] + half * (dy[0] + dx[1]), q[XZ] + half * (dz[0] + dx[2]),
            q[YZ] + half * (dz[1] + dy[2]),
        ]

    def keep(flag, value):
        return jnp.where(flag, value, 0.0)

    def pack(packed, value, base, j):
        return jnp.where(pair == base + j, pltpu.roll(value, 2 * (base + j) + 1, 1), packed)

    def pack_bar(packed, values, z, b):
        j = z * blocks + b
        packed[0] = pack(packed[0], values[0], 0, j)
        packed[0] = pack(packed[0], values[1], pairs, j)
        packed[1] = pack(packed[1], values[2], 0, j)
        packed[1] = pack(packed[1], values[3], pairs, j)

    def message(src, dst, way, send, recv):
        return pltpu.make_async_remote_copy(
            src_ref=src, dst_ref=dst, send_sem=send, recv_sem=recv,
            device_id=target(WAYS[way]), device_id_type=MESH,
        )

    ahead_rows, early = ys - 8, 8 * (blocks // 2)
    exchanges = []
    for s in range(ITERS):
        z_up_part = pl.ds(1, 3) if s == 0 else pl.ds(0, 4)
        z_down_part = pl.ds(0, 1) if s == 0 else pl.ds(0, 4)
        z_rows = pl.ds(early, ys - early) if s == 1 else pl.ds(0, ys)
        ends = (
            (bar.at[z_up_part, zs - 1, z_rows], z_lo.at[s, z_up_part, z_rows]),
            (bar.at[z_down_part, 0, z_rows], z_hi.at[s, z_down_part, z_rows]),
            (face.at[xf], x_lo.at[s]),
            (face.at[xf], x_hi.at[s]),
            (face.at[top_face], y_lo.at[s]),
            (face.at[u_face], y_hi.at[s]),
            (face.at[xf, pl.ds(0, 1)], d_a.at[s, :, pl.ds(0, 1)]),
            (face.at[xf, pl.ds(7, 1)], d_b.at[s, :, pl.ds(7, 1)]),
            (xe, d_c.at[s]),
            (xe, d_d.at[s]),
            (face.at[top_face, pl.ds(0, 1)], d_e.at[s, :, pl.ds(0, 1)]),
            (face.at[u_face, pl.ds(zs - 1, 1)], d_g.at[s, :, pl.ds(zs - 1, 1)]),
        )
        exchanges.append([
            (message(src, dst, k, send_sem.at[k], recv_sem.at[s % 2, k]), goes[k], comes[k])
            for k, (src, dst) in enumerate(ends)
        ])
    duals = [
        (message(src, dst, way, first_send.at[k], first_recv.at[k]), goes[way], comes[way])
        for k, (src, dst, way) in enumerate((
            (tz_p.at[:, pl.ds(0, ahead_rows)], zp.at[:, pl.ds(0, ahead_rows)], Z_UP),
            (tz_q.at[:, pl.ds(0, ahead_rows)], zq.at[:, pl.ds(0, ahead_rows)], Z_DOWN),
            (p_in.at[:, :, ys - 1], yp, Y_UP),
            (q_in.at[:, :, 0], yq, Y_DOWN),
            (xs_own, xp, X_UP),
            (xs_own, xq, X_DOWN),
            (tz_p.at[:, pl.ds(ahead_rows, 8)], zp.at[:, pl.ds(ahead_rows, 8)], Z_UP),
            (tz_q.at[:, pl.ds(ahead_rows, 8)], zq.at[:, pl.ds(ahead_rows, 8)], Z_DOWN),
            (bar.at[:, zs - 1, pl.ds(0, early)], z_lo.at[1, :, pl.ds(0, early)], Z_UP),
            (bar.at[:, 0, pl.ds(0, early)], z_hi.at[1, :, pl.ds(0, early)], Z_DOWN),
        ))
    ]

    def start(moves, only=None):
        for copy, there, _ in moves:
            @pl.when(there if only is None else jnp.logical_and(there, only))
            def _():
                copy.start()

    def sent(moves):
        for copy, there, _ in moves:
            @pl.when(there)
            def _():
                copy.wait_send()

    def got(moves):
        for copy, _, there in moves:
            @pl.when(there)
            def _():
                copy.wait_recv()

    empty = jnp.zeros((8, xs), jnp.float32)

    def each(low, high, body, carry):
        def turn(j, carry):
            one = list(carry)
            body(low + 2 * j, one)
            body(low + 2 * j + 1, one)
            return tuple(one)

        return lax.fori_loop(0, (high - low) // 2, turn, tuple(carry))

    def dual_block(z, b, for_p=True, for_q=True):
        r = rows(b)
        v = [bar[1 + k, z, r, :] for k in range(3)]
        p = q = None
        if for_p:
            u = bar[0, z, r, :]
            slopes = (
                next_x(u) - up_x * u,
                next_y(bar, 0, z, b, u) - up_y(b, u),
                next_z(bar, 0, z, b) - up_z(z) * u,
            )
            p = [p_out[k, z, r, :] + SIGMA * (slopes[k] - v[k]) for k in range(3)]
        if for_q:
            dx = [lo_x * v[k] - prev_x(v[k]) for k in range(3)]
            dy = [lo_y(b, v[k]) - prev_y(bar, 1 + k, z, b, v[k]) for k in range(3)]
            dz = [lo_z(z) * v[k] - prev_z(bar, 1 + k, z, b) for k in range(3)]
            q = grow_q([q_out[k, z, r, :] for k in range(6)], dx, dy, dz)
        return p, q

    def dual_inside(z, _):
        later = []
        for b in range(blocks):
            p, q = dual_block(z, b)
            later += [(p_out, (k, z, rows(b)), new) for k, new in enumerate(p)]
            later += [(q_out, (k, z, rows(b)), new) for k, new in enumerate(q)]
        flush(later)

    def dual_first():
        later = []
        for b in range(blocks):
            p, q = dual_block(zs - 1, b, for_q=False)[0], dual_block(0, b, for_p=False)[1]
            later += [(tz_p, (k, rows(b)), new) for k, new in enumerate(p)]
            later += [(tz_q, (k, rows(b)), new) for k, new in enumerate(q)]
        flush(later)

    def line_up(s):
        cv[0] = SIGMA * jnp.where(odd, turn_lanes(x_hi[s, 0], half_lanes - 2), x_lo[s, 0])
        cv[1] = half * turn_lanes(x_lo[s, 1], half_lanes)
        cv[2] = half * x_lo[s, 1]

    def less_q(q, x=None, y=None, z=None):
        q = list(q)
        if x is not None:
            q[XX] = q[XX] - SIGMA * x[0]
            q[XY] = q[XY] - half * x[1]
            q[XZ] = q[XZ] - half * x[2]
        if y is not None:
            q[YY] = q[YY] - SIGMA * y[1]
            q[XY] = q[XY] - half * y[0]
            q[YZ] = q[YZ] - half * y[2]
        if z is not None:
            q[ZZ] = q[ZZ] - SIGMA * z[2]
            q[XZ] = q[XZ] - half * z[0]
            q[YZ] = q[YZ] - half * z[1]
        return q

    def dual(z, s):
        later = []
        for b in range(blocks):
            r = rows(b)
            by = half_lanes - 2 * (z * blocks + b)
            from_x = [turn_lanes(cv[k], by) for k in range(3)]
            t = [p_out[k, z, r, :] for k in range(3)]
            t[0] = t[0] + jnp.where(last_lane, from_x[0], 0.0)
            if b == blocks - 1:
                t[1] = t[1] + SIGMA * jnp.where(last_row, y_hi[s, 0, pl.ds(z, 1), :], 0.0)
            for k in range(3):
                if z == zs - 1:
                    later.append((part_p, (k, r), t[k]))
            if z < zs - 1:
                for k, new in enumerate(shrink_p(t)):
                    later.append((p_out, (k, z, r), new))
            hx = [jnp.where(first_lane, part, 0.0) for part in from_x]
            hy = None
            if b == 0:
                hy = [jnp.where(first_row, y_lo[s, 1 + k, pl.ds(z, 1), :], 0.0) for k in range(3)]
            q = less_q([q_out[k, z, r, :] for k in range(6)], y=hy)
            for k, part in zip((XX, XY, XZ), hx):
                q[k] = q[k] - part
            if z > 0:
                q = shrink_q(q)
            for k in range(6):
                later.append((part_q, (k, r), q[k]) if z == 0 else (q_out, (k, z, r), q[k]))
        flush(later)

    def dual_ends(s, only=range(blocks)):
        later = []
        for b in only:
            r = rows(b)
            t = [part_p[k, r, :] for k in range(3)]
            t[2] = t[2] + SIGMA * z_hi[s, 0, r, :]
            for k, new in enumerate(shrink_p(t)):
                later.append((p_out, (k, zs - 1, r), new))
            q = less_q([part_q[k, r, :] for k in range(6)], z=[z_lo[s, 1 + k, r, :] for k in range(3)])
            for k, new in enumerate(shrink_q(q)):
                later.append((q_out, (k, 0, r), new))
        flush(later)

    def spread(row):
        return jnp.broadcast_to(row, (8, xs))

    def column(row, lane_of_first):
        mine = lane == lane_of_first + 2 * blocks * sub
        return jnp.sum(jnp.where(mine, spread(row), 0.0), axis=1, keepdims=True)

    where = ((0, half_lanes), (1, 0), (1, half_lanes))

    def halo_x_inside(s):
        far = pairs - blocks
        up_yc = jnp.where(jnp.logical_and(last_row, (p_pair & (blocks - 1)) == blocks - 1), factor(above[1]), 1.0)
        lo_yc = jnp.where(jnp.logical_and(first_row, (q_pair & (blocks - 1)) == 0), factor(below[1]), 1.0)
        up_zc = jnp.where(p_pair >= far, factor(above[2]), 1.0)
        lo_zc = jnp.where(q_pair < blocks, factor(below[2]), 1.0)
        u = turn_lanes(x_lo[s, 0], half_lanes)
        v = [x_lo[s, 0], turn_lanes(x_lo[s, 1], half_lanes), x_lo[s, 1]]
        own = turn_lanes(face[4], half_lanes - 1)
        moved = turn_rows(u, -1)
        turned = jnp.where((p_pair & (blocks - 1)) == blocks - 1, 0.0, turn_lanes(moved, -2))
        ahead_y = jnp.where(last_row, turned, moved)
        ahead_z = jnp.where(p_pair >= far, 0.0, turn_lanes(u, -2 * blocks))
        slopes = (own - u, ahead_y - up_yc * u, ahead_z - up_zc * u)
        for k in range(3):
            xp[k] = xp[k] + SIGMA * (slopes[k] - v[k])

        v = [turn_lanes(x_hi[s, 0], -2), turn_lanes(x_hi[s, 1], half_lanes - 2), turn_lanes(x_hi[s, 1], -2)]
        mine = [turn_lanes(face[4], -1), turn_lanes(face[5], half_lanes - 1), turn_lanes(face[5], -1)]
        dx, dy, dz = [], [], []
        for k in range(3):
            dx.append(v[k] - mine[k])
            moved = turn_rows(v[k], 1)
            turned = jnp.where((q_pair & (blocks - 1)) == 0, 0.0, turn_lanes(moved, 2))
            dy.append(lo_yc * v[k] - jnp.where(first_row, turned, moved))
            dz.append(lo_zc * v[k] - jnp.where(q_pair < blocks, 0.0, turn_lanes(v[k], 2 * blocks)))
        q = [turn_lanes(xq[k], -2) if s == 0 else xq[k] for k in range(6)]
        for k, new in enumerate(grow_q(q, dx, dy, dz)):
            xq[k] = new

    def halo_x(s):
        far = pairs - blocks
        t = [xp[k] for k in range(3)]
        edge = turn_lanes(spread(d_a[s, 0, pl.ds(0, 1), :]), half_lanes + 2 * (blocks - 1))
        here = jnp.logical_and(last_row, (p_pair & (blocks - 1)) == blocks - 1)
        t[1] = t[1] + SIGMA * jnp.where(here, edge, 0.0)
        edge = turn_lanes(d_c[s, 0], half_lanes + 2 * far)
        t[2] = t[2] + SIGMA * jnp.where(p_pair >= far, edge, 0.0)
        p = [keep(below[0], part) for part in shrink_p(t)]
        here = jnp.logical_and(first_row, (q_pair & (blocks - 1)) == 0)
        edge_y, edge_z = [], []
        for h, base in where:
            edge = turn_lanes(spread(d_b[s, h, pl.ds(7, 1), :]), half_lanes - 2 * blocks - base)
            edge_y.append(jnp.where(here, edge, 0.0))
            edge = turn_lanes(d_d[s, h], half_lanes - 2 - 2 * far - base)
            edge_z.append(jnp.where(q_pair < blocks, edge, 0.0))
        q = shrink_q(less_q([xq[k] for k in range(6)], y=edge_y, z=edge_z))
        q = [keep(above[0], part) for part in q]
        for k in range(3):
            xp[k] = p[k]
        for k in range(6):
            xq[k] = q[k]
        cp[0] = jnp.where(odd, q[XX], p[0])
        cp[1] = q[XY]
        cp[2] = q[XZ]

    def halo_y_inside(s):
        up_zr = jnp.where(last_row, factor(above[2]), 1.0)
        lo_zr = jnp.where(first_row, factor(below[2]), 1.0)
        u = y_lo[s, 0]
        slopes = (
            next_x(u) - up_x * u,
            face[0] - u,
            jnp.where(last_row, 0.0, turn_rows(u, -1)) - up_zr * u,
        )
        for k in range(3):
            yp[k] = yp[k] + SIGMA * (slopes[k] - y_lo[s, 1 + k])
        v = [y_hi[s, 1 + k] for k in range(3)]
        dx = [lo_x * v[k] - prev_x(v[k]) for k in range(3)]
        dy = [v[k] - face[7 + k] for k in range(3)]
        dz = [lo_zr * v[k] - jnp.where(first_row, 0.0, turn_rows(v[k], 1)) for k in range(3)]
        for k, new in enumerate(grow_q([yq[k] for k in range(6)], dx, dy, dz)):
            yq[k] = new

    def halo_y(s):
        t = [yp[k] for k in range(3)]
        edge = column(d_b[s, 0, pl.ds(7, 1), :], 2 * blocks - 1)
        t[0] = t[0] + SIGMA * jnp.where(last_lane, edge, 0.0)
        t[2] = t[2] + SIGMA * jnp.where(last_row, d_e[s, 0, pl.ds(0, 1), :], 0.0)
        p = shrink_p(t)
        edge_x = [
            jnp.where(first_lane, column(d_a[s, h, pl.ds(0, 1), :], base), 0.0) for h, base in where
        ]
        edge_z = [jnp.where(first_row, d_g[s, 1 + k, pl.ds(zs - 1, 1), :], 0.0) for k in range(3)]
        q = shrink_q(less_q([yq[k] for k in range(6)], x=edge_x, z=edge_z))
        for k in range(3):
            yp[k] = keep(below[1], p[k])
        for k in range(6):
            yq[k] = keep(above[1], q[k])

    def halo_z_first(only):
        later = []
        for b in only:
            r = rows(b)
            t = [zp[k, r, :] for k in range(3)]
            edge_x = turn_lanes(d_d[0, 0], xs - 2 - 2 * (blocks * (zs - 1) + b))
            t[0] = t[0] + SIGMA * jnp.where(last_lane, edge_x, 0.0)
            if b == blocks - 1:
                t[1] = t[1] + SIGMA * jnp.where(last_row, d_g[0, 0, pl.ds(zs - 1, 1), :], 0.0)
            t[2] = t[2] + SIGMA * bar[0, 0, r, :]
            for k, new in enumerate(shrink_p(t)):
                later.append((zp, (k, r), keep(below[2], new)))

            hx = [
                jnp.where(first_lane, turn_lanes(d_c[0, h], -base - 2 * b), 0.0) for h, base in where
            ]
            hz = [bar[1 + k, zs - 1, r, :] for k in range(3)]
            hy = None
            if b == 0:
                hy = [jnp.where(first_row, d_e[0, 1 + k, pl.ds(0, 1), :], 0.0) for k in range(3)]
            q = less_q([zq[k, r, :] for k in range(6)], hx, hy, hz)
            for k, new in enumerate(shrink_q(q)):
                later.append((zq, (k, r), keep(above[2], new)))
        flush(later)

    def halo_z(s):
        later = []
        for b in range(blocks):
            r = rows(b)
            u = z_lo[s, 0, r, :]
            edge_x = turn_lanes(d_d[s, 0], xs - 2 - 2 * (blocks * (zs - 1) + b))
            if b < blocks - 1:
                ahead_y = z_lo[s, 0, rows(b, 1), :]
            else:
                ahead_y = jnp.where(last_row, d_g[s, 0, pl.ds(zs - 1, 1), :], turn_rows(u, -1))
            slopes = (
                jnp.where(last_lane, edge_x, turn_lanes(u, -1)) - up_x * u,
                ahead_y - up_y(b, u),
                bar[0, 0, r, :] - u,
            )
            p = shrink_p([zp[k, r, :] + SIGMA * (slopes[k] - z_lo[s, 1 + k, r, :]) for k in range(3)])
            for k in range(3):
                later.append((zp, (k, r), keep(below[2], p[k])))

            v = [z_hi[s, 1 + k, r, :] for k in range(3)]
            dx, dy, dz = [], [], []
            for k, (h, base) in enumerate(where):
                edge_x = turn_lanes(d_c[s, h], -base - 2 * b)
                dx.append(lo_x * v[k] - jnp.where(first_lane, edge_x, turn_lanes(v[k], 1)))
                if b > 0:
                    behind_y = z_hi[s, 1 + k, rows(b, -1), :]
                else:
                    behind_y = jnp.where(first_row, d_e[s, 1 + k, pl.ds(0, 1), :], turn_rows(v[k], 1))
                dy.append(lo_y(b, v[k]) - behind_y)
                dz.append(v[k] - bar[1 + k, zs - 1, r, :])
            q = shrink_q(grow_q([zq[k, r, :] for k in range(6)], dx, dy, dz))
            for k in range(6):
                later.append((zq, (k, r), keep(above[2], q[k])))
        flush(later)

    def pack_plane(packed, z):
        for b in range(blocks):
            pack_bar(packed, [bar[k, z, rows(b), :] for k in range(4)], z, b)

    halo = (
        cp,
        lambda z: yp[1, pl.ds(z, 1), :],
        lambda k, z: yq[k, pl.ds(z, 1), :],
        lambda r: zp[2, r, :],
        lambda k, r: zq[k, r, :],
    )

    def primal(z, only=None):
        later = []
        for b, r, pieces in primal_plane(z, below, above, u_out, v_out, p_out, q_out, gain, offset, halo, only):
            for k, (new, old) in enumerate(pieces):
                later.append((u_out, (z, r), new) if k == 0 else (v_out, (k - 1, z, r), new))
                ahead = 2.0 * new - old
                later.append((bar, (k, z, r), ahead))
                if b == 0:
                    later.append((face, (k, pl.ds(z, 1)), ahead[0:1, :]))
                if b == blocks - 1:
                    later.append((face, (6 + k, pl.ds(z, 1)), ahead[7:8, :]))
        flush(later)

    def pack_dual(packed, z):
        for b in range(blocks):
            for k in range(6):
                value = q_out[k, z, rows(b), :]
                if k < 3:
                    value = jnp.where(last_lane, p_out[k, z, rows(b), :], value)
                packed[k] = pack(packed[k], value, pairs, z * blocks + b)

    def prepare(z, carry):
        weight = TAU * gain[z]
        inverse = 1.0 / (1.0 + weight)
        gain[z] = inverse
        offset[z] = weight * offset[z] * inverse
        return carry

    ends, middle = (0, zs - 1), range(1, zs - 1)

    def primal_and_pack(lag=3):
        packed = [empty, empty]
        for z in middle:
            primal(z)
            if z > lag:
                pack_plane(packed, z - lag)
        for z in middle[-lag:]:
            pack_plane(packed, z)
        return packed

    with jax.named_scope("load_uv"):
        loaded(0)
    with jax.named_scope("load_pq"):
        loaded(2, 3, 1)
    with jax.named_scope("first_z"):
        packed = [empty, empty]
        for z in ends:
            pack_plane(packed, z)
        dual_first()
        xe[0] = packed[0]
        xe[1] = packed[1]
    with jax.named_scope("barrier"):
        pl.semaphore_wait(barrier, peers)
    with jax.named_scope("send_z0"):
        start(exchanges[0][8:])
        start(exchanges[0][:2])
        start(duals[:2])
        start(duals[6:8])
        start(exchanges[0][4:6])
        begin(4)
    with jax.named_scope("pack_uv"):
        loaded(5)
        for z in middle:
            pack_plane(packed, z)
        face[4] = packed[0]
        face[5] = packed[1]
        start(exchanges[0][6:8])
        start(exchanges[0][2:4])
        start(duals[2:4])
    with jax.named_scope("pack_pq"):
        loaded(6, 7)
        packed = [empty] * 6
        for z in range(zs):
            pack_dual(packed, z)
        for k in range(6):
            xs_own[k] = packed[k]
        start(duals[4:6])
    with jax.named_scope("inside0"):
        each(0, zs, dual_inside, ())
    with jax.named_scope("prepare"):
        loaded(4)
        lax.fori_loop(0, zs, prepare, 0)

    for s in range(ITERS):
        last = s == ITERS - 1
        moves = exchanges[s]
        if s > 0:
            with jax.named_scope(f"inside{s}"):
                each(0, zs, dual_inside, ())
        with jax.named_scope(f"wait_xy{s}"):
            got(moves[2:6])
            line_up(s)
        with jax.named_scope(f"dual_mid{s}"):
            for z in range(zs):
                dual(z, s)
            if s > 0:
                halo_x_inside(s)
                halo_y_inside(s)
        if s == 0:
            with jax.named_scope(f"wait_pq{s}"):
                got(duals[2:6])
                halo_x_inside(s)
                halo_y_inside(s)
        with jax.named_scope(f"wait_diag{s}"):
            got(moves[6:])
        with jax.named_scope(f"halo_xy{s}"):
            halo_x(s)
            halo_y(s)
        with jax.named_scope(f"wait_z{s}"):
            got(moves[:2])
            sent(moves)
        if s == 0:
            with jax.named_scope(f"wait_zpq{s}"):
                got(duals[:2])
            with jax.named_scope("early"):
                halo_z_first(range(blocks - 1))
                dual_ends(s, range(blocks - 1))
                for z in ends:
                    primal(z, range(blocks // 2))
                start(duals[8:])
            with jax.named_scope("middle"):
                packed = primal_and_pack()
            with jax.named_scope("wait_zpq_rest"):
                got(duals[6:8])
                sent(duals[:8])
        elif s == 1:
            with jax.named_scope("wait_early"):
                got(duals[8:])
                sent(duals[8:])
        with jax.named_scope(f"ends{s}"):
            of_ends = [empty, empty]
            if s == 0:
                halo_z_first([blocks - 1])
                dual_ends(s, [blocks - 1])
                for z in ends:
                    primal(z, range(blocks // 2, blocks))
            else:
                halo_z(s)
                dual_ends(s)
                if last:
                    edge_y[0] = yp[1]
                    edge_z[0] = zp[2]
                    for at, k in enumerate(Y_PARTS):
                        edge_y[1 + at] = yq[k]
                    for at, k in enumerate(Z_PARTS):
                        edge_z[1 + at] = zq[k]
                    continue
                for z in ends:
                    primal(z)
            for z in ends:
                pack_plane(of_ends, z)
            xe[0] = of_ends[0]
            xe[1] = of_ends[1]
            if s == 0:
                face[4] = packed[0] + of_ends[0]
                face[5] = packed[1] + of_ends[1]
        with jax.named_scope(f"send_z{s}"):
            start(exchanges[s + 1][8:])
            if s == 0:
                start(exchanges[s + 1][4:8])
                start(exchanges[s + 1][2:4])
            start(exchanges[s + 1][:2])
        if s > 0:
            with jax.named_scope(f"primal_mid{s}"):
                packed = primal_and_pack()
                face[4] = packed[0] + of_ends[0]
                face[5] = packed[1] + of_ends[1]
            with jax.named_scope(f"send{s}"):
                start(exchanges[s + 1][4:8])
                start(exchanges[s + 1][2:4])


def last_primal(*refs):
    pl.run_scoped(lambda sems: finish_kernel(sems, *refs), pltpu.SemaphoreType.DMA((4,)))


def finish_kernel(
    sems, u_in, v_in, p_in, q_in, gain, offset, cp, edge_y, edge_z,
    u_out, v_out, p_out, q_out,
    u_new, v_new,
):
    zs, ys, xs = u_in.shape
    place = [lax.axis_index(a) for a in AXES]
    count = [lax.axis_size(a) for a in AXES]
    below = [place[i] > 0 for i in range(3)]
    above = [place[i] < count[i] - 1 for i in range(3)]
    for k in range(6):
        pltpu.make_async_copy(q_in.at[k], q_out.at[k], sems.at[0]).start()
    for k in range(3):
        pltpu.make_async_copy(p_in.at[k], p_out.at[k], sems.at[1]).start()
    halo = (
        cp,
        lambda z: edge_y[0, pl.ds(z, 1), :],
        lambda k, z: edge_y[1 + Y_PARTS.index(k), pl.ds(z, 1), :],
        lambda r: edge_z[0, r, :],
        lambda k, r: edge_z[1 + Z_PARTS.index(k), r, :],
    )
    for z in range(zs):
        for _, r, pieces in primal_plane(z, below, above, u_in, v_in, p_in, q_in, gain, offset, halo):
            u_new[z, r, :] = pieces[0][0]
            for k in range(3):
                v_new[k, z, r, :] = pieces[1 + k][0]
        if z % 2 == 1:
            two = pl.ds(z - 1, 2)
            pltpu.make_async_copy(v_new.at[:, two], v_out.at[:, two], sems.at[2]).start()
            pltpu.make_async_copy(u_new.at[two], u_out.at[two], sems.at[3]).start()
    for k, (src, dst) in enumerate(((q_in, q_out), (p_in, p_out), (v_new, v_out), (u_new, u_out))):
        pltpu.make_async_copy(src, dst, sems.at[k]).wait()


def per_device(noisy_image, fidelity, primal_u, primal_v, dual_p, dual_q):
    zs, ys, xs = primal_u.shape
    blocks = ys // 8
    assert zs == 8 and ys % 8 == 0 and blocks & (blocks - 1) == 0 and 4 * zs * blocks == xs == 128
    f32 = jnp.float32

    def vmem(*shape):
        return pltpu.VMEM(shape, f32)

    shapes = [a.shape for a in (primal_u, primal_v, dual_p, dual_q)]
    kept = shapes + [(zs, ys, xs), (zs, ys, xs), (3, 8, xs), (4, 8, xs), (4, ys, xs)]
    results = pl.pallas_call(
        kernel,
        out_shape=tuple(vmem(*shape) for shape in kept),
        in_specs=[pl.BlockSpec(memory_space=pl.ANY)] * 6,
        out_specs=tuple([pl.BlockSpec(memory_space=pltpu.VMEM)] * len(kept)),
        scratch_shapes=[
            vmem(4, zs, ys, xs),
            vmem(10, 8, xs),
            vmem(ITERS, 4, ys, xs),
            vmem(ITERS, 4, ys, xs),
            vmem(ITERS, 2, 8, xs),
            vmem(ITERS, 2, 8, xs),
            vmem(ITERS, 4, 8, xs),
            vmem(ITERS, 4, 8, xs),
            vmem(ITERS, 2, 8, xs),
            vmem(ITERS, 2, 8, xs),
            vmem(ITERS, 2, 8, xs),
            vmem(ITERS, 2, 8, xs),
            vmem(ITERS, 4, 8, xs),
            vmem(ITERS, 4, 8, xs),
            vmem(3, ys, xs),
            vmem(6, ys, xs),
            vmem(3, 8, xs),
            vmem(6, 8, xs),
            vmem(6, 8, xs),
            vmem(6, 8, xs),
            vmem(6, 8, xs),
            vmem(3, 8, xs),
            vmem(2, 8, xs),
            vmem(3, ys, xs),
            vmem(6, ys, xs),
            vmem(3, ys, xs),
            vmem(6, ys, xs),
        ],
        compiler_params=pltpu.CompilerParams(collective_id=0, has_side_effects=True),
        name="tgv",
    )(noisy_image, fidelity, primal_u, primal_v, dual_p, dual_q)
    return pl.pallas_call(
        last_primal,
        out_shape=tuple(jax.ShapeDtypeStruct(shape, f32) for shape in shapes),
        in_specs=[pl.BlockSpec(memory_space=pltpu.VMEM)] * len(kept),
        out_specs=tuple([pl.BlockSpec(memory_space=pl.ANY)] * 4),
        scratch_shapes=[
            vmem(zs, ys, xs),
            vmem(3, zs, ys, xs),
        ],
        name="out",
    )(*[pltpu.with_memory_space_constraint(r, pltpu.VMEM) for r in results])


def solution(mesh):
    scalar, stack = P("gz", "gy", "gx"), P(None, "gz", "gy", "gx")
    return jax.shard_map(
        per_device,
        mesh=mesh,
        in_specs=(scalar, scalar, scalar, stack, stack, stack),
        out_specs=(scalar, stack, stack, stack),
        check_vma=False,
    )
```
